128 devices in a mesh: gx: 8 (over z, x_lo), gy: 16 (over y, x_hi, core).
Axes of the slice: x: 4 (x_hi: 2, x_lo: 2; x = x_hi * 2 + x_lo), y: 4, z: 4, core: 2. Of those that a mesh axis runs over, the one named last changes fastest.
Arguments:
- forcing: float32 [4, 2048, 4096], P(None, ('gx', 'gy')), may hold values from -6 to 6
- ice_state: float32 [2, 2048, 4096], P(None, ('gx', 'gy')), may hold values from 0.3 to 3, as said below
- velocity: float32 [2, 2048, 4096], P(None, ('gx', 'gy')), may hold values from -4 to 4
- stress: float32 [3, 2048, 4096], P(None, ('gx', 'gy')), may hold values from -4 to 4
- ice_mask: int32 [2048, 4096], P(('gx', 'gy')), may hold values from 0 to 2, as said below
Outputs:
- ice_velocity: float32 [2, 2048, 4096], P(None, ('gx', 'gy'))
- ice_stress: float32 [3, 2048, 4096], P(None, ('gx', 'gy'))
- ocean_stress: float32 [2, 2048, 4096], P(None, ('gx', 'gy'))
The draws below stay inside these ranges and needn't reach their ends.
Inputs may be any that keep to these rules, and one draw needn't show every extreme that they name: `ice_state`: row 0 lies in 0.7 to 1, row 1 in 0.3 to 3. `ice_mask`: 0 marks land, 1 open water, 2 ice-covered cells.
All inputs are finite; a program needn't handle non-finite values.
Results may differ from the reference program's by a relative error of at most 0.00002.
Values sent between devices are 32-bit elements; how exact they have to be, the bound alone decides.
No kernel may reach another device: no remote copies, remote signals or barrier semaphores. Data moves between devices by JAX's collectives and lax.ppermute only.
A program may use at most 128 MiB of HBM per device.

```python
import math
import jax
import jax.numpy as jnp
from jax import lax

ITERS = 4
NX = 2048
NY = 4096


def draw_ice_state(key, part):
    key_conc, key_thick = jax.random.split(key)
    concentration = jax.random.uniform(key_conc, (NX, NY), jnp.float32, 0.7, 1.0)
    log_thick = jax.random.uniform(key_thick, (NX, NY), jnp.float32, jnp.log(0.3), jnp.log(3.0))
    return jnp.stack([concentration, jnp.exp(log_thick)]).astype(jnp.float32)


def draw_ice_mask(key, part):
    noise = jax.random.randint(key, (NX, NY), 0, 100)
    row_index = lax.broadcasted_iota(jnp.int32, (NX, NY), 1)
    polar_band = jnp.abs(2 * row_index - NY + 1) * 100 // NY
    return jnp.where(noise >= 95, 0, jnp.where(noise < 50 + polar_band // 3, 2, 1)).astype(jnp.int32)


def block_scale(key, dims, shards, low, high):
    def one(dim, parts):
        heights = jax.random.uniform(jax.random.fold_in(jax.random.fold_in(key, 6), dim), (parts,), jnp.float32, low / len(shards), high / len(shards))
        return jnp.repeat(jnp.exp(heights), dims[dim] // parts).reshape((-1,) + (1,) * (len(dims) - dim - 1))

    gain = one(*shards[0])
    for cut in shards[1:]:
        gain = gain * one(*cut)
    return gain


def bell_draw(key, shape, width, limit, cuts=(), kind=jnp.bfloat16):
    values = width * jax.random.normal(key, shape, jnp.float32)
    if cuts:
        values = values * block_scale(key, shape, cuts, -0.22, 0.18)
    return jnp.clip(values, -limit, limit).astype(kind)


def setup_inputs(seed: int = 0) -> dict:
    seeds = jax.random.split(jax.random.key(seed), 6)
    forcing = bell_draw(seeds[0], (4, NX, NY), 1.0, 6.0, ((1, 128),), jnp.float32)
    ice_state = draw_ice_state(jax.random.fold_in(seeds[5], 71), 0)
    velocity = bell_draw(seeds[2], (2, NX, NY), 0.5, 4.0, ((1, 128),), jnp.float32)
    stress = bell_draw(seeds[3], (3, NX, NY), 0.5, 4.0, ((1, 128),), jnp.float32)
    ice_mask = draw_ice_mask(jax.random.fold_in(seeds[5], 71), 0)
    return dict(forcing=forcing, ice_state=ice_state, velocity=velocity, stress=stress, ice_mask=ice_mask)


P_STAR = 1.0
C_STAR = 20.0
ECC_SQ = 4.0
DELTA_MIN = 0.05
ALPHA_EVP = 30.0
BETA_EVP = 30.0
DRAG_COEF = 0.5
SPEED_FLOOR = 0.05
CORIOLIS_MAX = 0.5

def extend_global(fields, sign_flip):
    top_row = fields[:, ::-1, -1:] * sign_flip[:, None, None]
    tall = jnp.concatenate([jnp.zeros_like(top_row), fields, top_row], axis=2)
    return jnp.concatenate([tall[:, -1:, :], tall, tall[:, :1, :]], axis=1)

def update_stress(vel_ext, state, pressure, ice_cover):
    u_field = vel_ext[0]
    v_field = vel_ext[1]
    diff_u = u_field[1:, 1:] - u_field[:-1, 1:]
    diff_v = v_field[1:, 1:] - v_field[1:, :-1]
    divergence = diff_u + diff_v
    tension = diff_u - diff_v
    shear_all = u_field[:-1, 1:] - u_field[:-1, :-1] + v_field[1:, :-1] - v_field[:-1, :-1]
    shear_cell = 0.25 * (shear_all[1:, 1:] + shear_all[:-1, 1:] + shear_all[1:, :-1] + shear_all[:-1, :-1])
    div_cell = divergence[:-1, :-1]
    ten_cell = tension[:-1, :-1]
    delta_cell = jnp.sqrt(div_cell * div_cell + (ten_cell * ten_cell + shear_cell * shear_cell) / ECC_SQ)
    capped = delta_cell + DELTA_MIN
    target_one = pressure * (div_cell - delta_cell) / capped
    target_two = pressure * ten_cell / (ECC_SQ * capped)
    div_corner = 0.25 * (divergence[:-1, :-1] + divergence[1:, :-1] + divergence[:-1, 1:] + divergence[1:, 1:])
    ten_corner = 0.25 * (tension[:-1, :-1] + tension[1:, :-1] + tension[:-1, 1:] + tension[1:, 1:])
    shear_corner = shear_all[1:, 1:]
    delta_corner = jnp.sqrt(div_corner * div_corner + (ten_corner * ten_corner + shear_corner * shear_corner) / ECC_SQ)
    capped_corner = delta_corner + DELTA_MIN
    target_three = pressure * shear_corner / (2.0 * ECC_SQ * capped_corner)
    targets = jnp.stack([target_one, target_two, target_three])
    return ice_cover[None] * (state + (targets - state) / ALPHA_EVP)

def update_velocity(vel_ext, stress_ext, start_vel, currents, wind_stress, ice_mass, coriolis, ice_cover, open_water):
    sigma_one = stress_ext[0]
    sigma_two = stress_ext[1]
    sigma_shear = stress_ext[2]
    normal_xx = 0.5 * (sigma_one + sigma_two)
    normal_yy = 0.5 * (sigma_one - sigma_two)
    force_u = normal_xx[2:, 1:-1] - normal_xx[1:-1, 1:-1] + sigma_shear[1:-1, 1:-1] - sigma_shear[1:-1, :-2]
    force_v = normal_yy[1:-1, 2:] - normal_yy[1:-1, 1:-1] + sigma_shear[1:-1, 1:-1] - sigma_shear[:-2, 1:-1]
    u_field = vel_ext[0]
    v_field = vel_ext[1]
    u_now = u_field[1:-1, 1:-1]
    v_now = v_field[1:-1, 1:-1]
    v_at_u = 0.25 * (v_field[1:-1, 1:-1] + v_field[2:, 1:-1] + v_field[1:-1, :-2] + v_field[2:, :-2])
    u_at_v = 0.25 * (u_field[1:-1, 1:-1] + u_field[:-2, 1:-1] + u_field[1:-1, 2:] + u_field[:-2, 2:])
    drag_u = DRAG_COEF * jnp.sqrt((currents[0] - u_now) ** 2 + SPEED_FLOOR ** 2)
    drag_v = DRAG_COEF * jnp.sqrt((currents[1] - v_now) ** 2 + SPEED_FLOOR ** 2)
    u_new = (BETA_EVP * u_now + start_vel[0] + (force_u + wind_stress[0] + drag_u * currents[0]) / ice_mass + coriolis * v_at_u) / (BETA_EVP + 1.0 + drag_u / ice_mass)
    v_new = (BETA_EVP * v_now + start_vel[1] + (force_v + wind_stress[1] + drag_v * currents[1]) / ice_mass - coriolis * u_at_v) / (BETA_EVP + 1.0 + drag_v / ice_mass)
    fresh = jnp.stack([u_new, v_new])
    return ice_cover[None] * fresh + open_water[None] * currents

def coriolis_field(first_row, row_count, total_rows):
    row_index = (first_row + jnp.arange(row_count, dtype=jnp.int32)).astype(jnp.float32)
    latitude = math.pi * ((row_index + 0.5) / total_rows - 0.5)
    return CORIOLIS_MAX * jnp.sin(latitude)[None, :]

def run_window(forcing, ice_state, velocity, stress, ice_mask, extend, first_row, total_rows):
    concentration = ice_state[0]
    thickness = ice_state[1]
    pressure = P_STAR * thickness * jnp.exp(-C_STAR * (1.0 - concentration))
    ice_mass = concentration * thickness
    ice_cover = (ice_mask == 2).astype(jnp.float32)
    open_water = (ice_mask == 1).astype(jnp.float32)
    currents = forcing[0:2]
    wind_stress = forcing[2:4]
    coriolis = coriolis_field(first_row, ice_mask.shape[1], total_rows)
    vel_flip = jnp.array([-1.0, -1.0], jnp.float32)
    stress_flip = jnp.array([1.0, 1.0, 1.0], jnp.float32)
    current_vel = velocity
    state = stress
    for turn_index in range(ITERS):
        vel_ext = extend(current_vel, vel_flip)
        state = update_stress(vel_ext, state, pressure, ice_cover)
        stress_ext = extend(state, stress_flip)
        current_vel = update_velocity(vel_ext, stress_ext, velocity, currents, wind_stress, ice_mass, coriolis, ice_cover, open_water)
    drag_final = DRAG_COEF * jnp.sqrt((currents - current_vel) ** 2 + SPEED_FLOOR ** 2)
    ocean = drag_final * (current_vel - currents)
    return (current_vel, state, ocean)

def reference(forcing, ice_state, velocity, stress, ice_mask):
    return run_window(forcing, ice_state, velocity, stress, ice_mask, extend_global, 0, NY)
```

```python
import math

import jax
import jax.numpy as jnp
import numpy as np
from jax import lax
from jax.experimental import pallas as pl
from jax.experimental.pallas import tpu as pltpu
from jax.sharding import PartitionSpec as P

F32 = jnp.float32
AXES = ("gx", "gy")
C = 16
R = 32
H = 3
NC = C + 2 * H
FIELDS = ("uo", "vo", "tx", "ty", "a", "h", "u", "v", "s1", "s2", "s12", "mask")
WHERE = {n: k for k, n in enumerate(FIELDS)}
STATE = ("u", "v", "s1", "s2", "s12")
FIRST = [(n, m) for m in range(2) for n in FIELDS] + [("u", 2), ("v", 2)]
SECOND = [(n, m) for m in range(2) for n in STATE] + [("u", 2), ("v", 2)]
U, V, S1, S2, S12 = range(5)
PR, MI, UO, CU, VO, CV, MK, OU, OV = range(9)
T, D2, W, DV2, E1, UP = range(6)
K29 = 29.0 / 30.0
STAGE = (2, 8 * 40, 128)
TOP = len(FIELDS)


def view(x):
    c = x.shape[0]
    return x.reshape(c, 2, 8, 8, 4, 128).transpose(0, 1, 3, 4, 2, 5).reshape(c, 2, 8, 32, 128)


def unview(y):
    c = y.shape[0]
    return y.reshape(c, 2, 8, 4, 8, 128).transpose(0, 1, 4, 2, 3, 5).reshape(c, C, 4096)


def iotas(shape):
    return lax.broadcasted_iota(jnp.int32, shape, 0), lax.broadcasted_iota(jnp.int32, shape, 1)


def root(x):
    return x * lax.rsqrt(jnp.maximum(x, 1e-30))


def below(x, masks):
    lane0, _, sub0, _ = masks
    r = pltpu.roll(x, 1, 1)
    q = jnp.where(sub0, 0.0, pltpu.roll(r[24:32], 1, 0))
    return jnp.where(lane0, jnp.concatenate([q, r[0:24]], 0), r)


def above(x, masks):
    _, lane127, _, _ = masks
    r = pltpu.roll(x, 127, 1)
    q = pltpu.roll(r[0:8], 7, 0)
    return jnp.where(lane127, jnp.concatenate([r[8:32], q], 0), r)


def make_masks():
    _, lane = iotas((R, 128))
    sub, _ = iotas((8, 128))
    return lane == 0, lane == 127, sub == 0, sub == 7


def rows(c):
    return pl.ds(pl.multiple_of((c + H) * R, R), R)


def each_column(lo, hi, chunk, body):
    def step(t, carry):
        for q in range(chunk):
            body(lo + t * chunk + q)
        return carry

    lax.fori_loop(0, (hi - lo) // chunk, step, 0)


def stress_terms(x1, e1, sc4, x, y, s, p):
    d = x1 + e1
    e = x1 - e1
    delta = root(d * d + 0.25 * (e * e) + (1.0 / 64.0) * (sc4 * sc4))
    r = p / (delta + 0.05)
    dk = x + y
    ek = x - y
    dk2 = root((1.0 / 16.0) * (dk * dk) + (1.0 / 64.0) * (ek * ek) + 0.25 * (s * s))
    rk = p / (dk2 + 0.05)
    return r * (d - delta), r * (0.25 * e), rk * (0.125 * s)


def momentum(w, o, c, mi, force, cor, ice, open_o):
    g = 0.5 * root((o - w) * (o - w) + 0.0025) * mi
    new = (30.0 * w + c + force * mi + g * o + cor) / (31.0 + g)
    return jnp.where(ice, new, open_o)


def subcycle(st, sc, tmp, f4, masks, vel, stress, mom):
    def shift(c):
        u, v = st[U, rows(c), :], st[V, rows(c), :]
        up, um = above(u, masks), below(u, masks)
        vp, vm = above(v, masks), below(v, masks)
        tmp[T, rows(c), :] = u + up
        tmp[D2, rows(c), :] = up - um
        tmp[UP, rows(c), :] = up - u
        tmp[W, rows(c), :] = v + vm
        tmp[E1, rows(c), :] = v - vm
        tmp[DV2, rows(c), :] = vp - vm

    each_column(*vel, shift)

    def strain(c):
        ld = lambda k, d=0: tmp[k, rows(c + d), :]
        us = lambda d: st[U, rows(c + d), :]
        vs = lambda d: st[V, rows(c + d), :]
        a1, a2, a12 = stress_terms(
            us(0) - us(-1),
            ld(E1),
            (ld(D2) + ld(D2, -1)) + (ld(W, 1) - ld(W, -1)),
            ld(T, 1) - ld(T, -1),
            ld(DV2) + ld(DV2, 1),
            ld(UP) + (vs(1) - vs(0)),
            sc[PR, rows(c), :],
        )
        st[S1, rows(c), :] = K29 * st[S1, rows(c), :] + a1
        st[S2, rows(c), :] = K29 * st[S2, rows(c), :] + a2
        st[S12, rows(c), :] = K29 * st[S12, rows(c), :] + a12

    each_column(*stress, strain)

    def move(c):
        ss = lambda k, d=0: st[k, rows(c + d), :]
        q1 = ss(S1) + ss(S2)
        q1n = ss(S1, 1) + ss(S2, 1)
        q2 = ss(S1) - ss(S2)
        s12 = ss(S12)
        fu = 0.5 * (q1n - q1) + (s12 - below(s12, masks))
        fv = 0.5 * (above(q2, masks) - q2) + (s12 - ss(S12, -1))
        cu = f4 * (tmp[W, rows(c), :] + tmp[W, rows(c + 1), :])
        cv = f4 * (tmp[T, rows(c), :] + tmp[T, rows(c - 1), :])
        k = lambda n: sc[n, rows(c), :]
        ice = k(MK) == 2.0
        mi = k(MI)
        st[U, rows(c), :] = momentum(ss(U), k(UO), k(CU), mi, fu, cu, ice, k(OU))
        st[V, rows(c), :] = momentum(ss(V), k(VO), k(CV), mi, fv, -cv, ice, k(OV))

    each_column(*mom, move)


def two_subcycles(st, sc, tmp, f4):
    masks = make_masks()
    subcycle(st, sc, tmp, f4, masks, (-3, 19, 11), (-2, 18, 5), (-2, 18, 5))
    subcycle(st, sc, tmp, f4, masks, (-2, 18, 5), (-1, 17, 6), (0, 16, 4))


def statics(raw):
    a, h, mask = raw["a"], raw["h"], raw["mask"]
    ice = mask == 2.0
    opened = mask == 1.0
    mi = 1.0 / (a * h)
    out = {
        PR: jnp.where(ice, h * jnp.exp(-20.0 * (1.0 - a)) * (1.0 / 30.0), 0.0),
        MI: mi,
        UO: raw["uo"],
        CU: raw["u"] + raw["tx"] * mi,
        VO: raw["vo"],
        CV: raw["v"] + raw["ty"] * mi,
        MK: mask,
        OU: jnp.where(opened, raw["uo"], 0.0),
        OV: jnp.where(opened, raw["vo"], 0.0),
    }
    return out, ice


def put_column(st, sc, at, raw):
    out, ice = statics(raw)
    for k, x in out.items():
        sc[k, at, :] = x
    st[U, at, :] = raw["u"]
    st[V, at, :] = raw["v"]
    st[S1, at, :] = jnp.where(ice, raw["s1"], 0.0)
    st[S2, at, :] = jnp.where(ice, raw["s2"], 0.0)
    st[S12, at, :] = jnp.where(ice, raw["s12"], 0.0)


def stage_in(srcs, stage, mstage, sems):
    copies = []
    at = 0
    for k, src in enumerate(srcs):
        n = src.shape[0]
        if k < 4:
            dst = stage.reshape(11, 2, 8, 40, 128).at[pl.ds(at, n), :, :, pl.ds(0, 32), :]
        else:
            dst = mstage.reshape(1, 2, 8, 40, 128).at[:, :, :, pl.ds(0, 32), :]
        copies.append(pltpu.make_async_copy(src, dst, sems.at[k]))
        at += n
    for c in copies:
        c.start()
    for c in copies:
        c.wait()


def staged_column(stage, mstage, name, c):
    ref, f = (mstage, 0) if name == "mask" else (stage, WHERE[name])
    parts = [ref[f, c // 8, pl.ds(8 * k + c % 8, 8, stride=40), :] for k in range(4)]
    return jnp.concatenate(parts, 0).astype(F32)


def parity():
    return lax.rem(lax.axis_index("gy"), 2)


def pack_kernel(f_ref, i_ref, v_ref, s_ref, m_ref, b_out, a_out, m_out, stage, mstage, sems):
    stage_in((f_ref, i_ref, v_ref, s_ref, m_ref), stage, mstage, sems)
    even = parity() == 0
    for n, (name, m) in enumerate(FIRST):
        left = staged_column(stage, mstage, name, m)
        right = staged_column(stage, mstage, name, C - 1 - m)
        b_out[pl.ds(n * R, R), :] = jnp.where(even, left, right)
        a_out[pl.ds(n * R, R), :] = jnp.where(even, right, left)
    for k in range(TOP):
        for ih in range(2):
            ref, f = (mstage, 0) if k == TOP - 1 else (stage, k)
            m_out[pl.ds(k * C + 8 * ih, 8), :] = ref[f, ih, pl.ds(7 * 40 + 24, 8), :].astype(F32)


def halo_rows(even, m):
    left, right = (H - 1 - m) * R, (H + C + m) * R
    via_b = pl.ds(pl.multiple_of(jnp.where(even, left, right), R), R)
    via_a = pl.ds(pl.multiple_of(jnp.where(even, right, left), R), R)
    return via_b, via_a


def first_kernel(
    f_ref, i_ref, v_ref, s_ref, m_ref, rb, ra, rm, cor, st, sc, strip, b_out, a_out,
    tmp, stage, mstage, sems,
):
    stage_in((f_ref, i_ref, v_ref, s_ref, m_ref), stage, mstage, sems)
    even = parity() == 0
    zero = jnp.zeros((R, 128), F32)
    for k in (S1, S2, S12):
        st[k, rows(-3), :] = zero
        st[k, rows(18), :] = zero
    for m in range(H):
        via = halo_rows(even, m)
        for at, src in zip(via, (rb, ra)):
            raw = {
                name: src[pl.ds(n * R, R), :] for n, (name, d) in enumerate(FIRST) if d == m
            }
            if m < 2:
                put_column(st, sc, at, raw)
            else:
                st[U, at, :] = raw["u"]
                st[V, at, :] = raw["v"]
    for c in range(C):
        put_column(
            st, sc, rows(c), {name: staged_column(stage, mstage, name, c) for name in FIELDS}
        )
    for k in range(TOP):
        for ih in range(2):
            ref, f = (mstage, 0) if k == TOP - 1 else (stage, k)
            strip[k, pl.ds(8 + 8 * ih, 8), :] = ref[f, ih, pl.ds(7 * 40 + 24, 8), :].astype(F32)
        for c in range(C):
            strip[TOP + k, pl.ds(8 + c, 1), :] = rm[pl.ds(k * C + (C - 1 - c), 1), :]
    two_subcycles(st, sc, tmp, 0.25 * cor[...])
    for n, (name, m) in enumerate(SECOND):
        left = st[STATE.index(name), rows(m), :]
        right = st[STATE.index(name), rows(C - 1 - m), :]
        b_out[pl.ds(n * R, R), :] = jnp.where(even, left, right)
        a_out[pl.ds(n * R, R), :] = jnp.where(even, right, left)
    base = len(SECOND) * R
    for k in range(2 * TOP):
        left = strip[k, pl.ds(8, 8), :]
        right = strip[k, pl.ds(16, 8), :]
        b_out[pl.ds(base + 8 * k, 8), :] = jnp.where(even, left, right)
        a_out[pl.ds(base + 8 * k, 8), :] = jnp.where(even, right, left)


def run_strips(strip, work, cor):
    _, lane = iotas((R, 128))
    last = lane == 127
    f4 = jnp.broadcast_to(0.25 * cor[pl.ds(31, 1), :], (R, 128))
    fixed = []
    for side in range(2):
        raw = {name: strip[side * TOP + k] for k, name in enumerate(FIELDS)}
        out, ice = statics(raw)
        fixed.append(out)
        work[5 * side + U] = raw["u"]
        work[5 * side + V] = raw["v"]
        for k, name in ((S1, "s1"), (S2, "s2"), (S12, "s12")):
            work[5 * side + k] = jnp.where(ice, raw[name], 0.0)
        for k in range(9):
            work[10 + 9 * side + k] = out[k]

    def step(t, carry):
        x = [[work[5 * side + k] for k in range(5)] for side in range(2)]
        east = [lambda y: pltpu.roll(y, R - 1, 0), lambda y: pltpu.roll(y, 1, 0)]
        west = [east[1], east[0]]
        down = lambda y: pltpu.roll(y, 1, 1)
        up = lambda y, other, sign: jnp.where(last, sign * other, pltpu.roll(y, 127, 1))
        terms = []
        for side in range(2):
            e, w = east[side], west[side]
            u, v = x[side][U], x[side][V]
            ou, ov = x[1 - side][U], x[1 - side][V]
            upu, um, vp, vm = up(u, ou, -1.0), down(u), up(v, ov, -1.0), down(v)
            tt, d2, ww, dv2 = u + upu, upu - um, v + vm, vp - vm
            terms.append((tt, ww))
            k = lambda n: work[10 + 9 * side + n]
            a1, a2, a12 = stress_terms(
                u - w(u),
                v - vm,
                (d2 + w(d2)) + (e(ww) - w(ww)),
                e(tt) - w(tt),
                dv2 + e(dv2),
                (upu - u) + (e(v) - v),
                k(PR),
            )
            x[side][S1] = K29 * x[side][S1] + a1
            x[side][S2] = K29 * x[side][S2] + a2
            x[side][S12] = K29 * x[side][S12] + a12
        new = []
        for side in range(2):
            e, w = east[side], west[side]
            u, v, s1, s2, s12 = x[side]
            q1, q2 = s1 + s2, s1 - s2
            other = x[1 - side][S1] - x[1 - side][S2]
            fu = 0.5 * (e(q1) - q1) + (s12 - down(s12))
            fv = 0.5 * (up(q2, other, 1.0) - q2) + (s12 - w(s12))
            tt, ww = terms[side]
            k = lambda n: work[10 + 9 * side + n]
            ice = k(MK) == 2.0
            nu = momentum(u, k(UO), k(CU), k(MI), fu, f4 * (ww + e(ww)), ice, k(OU))
            nv = momentum(v, k(VO), k(CV), k(MI), fv, -f4 * (tt + w(tt)), ice, k(OV))
            new.append((nu, nv, s1, s2, s12))
        for side in range(2):
            for k in range(5):
                work[5 * side + k] = new[side][k]
        return carry

    lax.fori_loop(0, 4, step, 0)


def second_kernel(
    st_in, sc, strip_in, rb, ra, cor, vel_o, str_o, oce_o, st, tmp, strip, work, stage, sems
):
    even = parity() == 0
    for k in range(5):
        st[k] = st_in[k]
    for m in range(H):
        via = halo_rows(even, m)
        for at, src in zip(via, (rb, ra)):
            for n, (name, d) in enumerate(SECOND):
                if d == m:
                    st[STATE.index(name), at, :] = src[pl.ds(n * R, R), :]
    base = len(SECOND) * R
    for k in range(2 * TOP):
        strip[k, pl.ds(8, 16), :] = strip_in[k, pl.ds(8, 16), :]
        xb = rb[pl.ds(base + 8 * k, 8), :]
        xa = ra[pl.ds(base + 8 * k, 8), :]
        strip[k, pl.ds(0, 8), :] = jnp.where(even, xb, xa)
        strip[k, pl.ds(24, 8), :] = jnp.where(even, xa, xb)
    run_strips(strip, work, cor)
    two_subcycles(st, sc, tmp, 0.25 * cor[...])
    row, lane = iotas((R, 128))
    top = (row == R - 1) & (lane >= 120)

    for c in range(C):
        x = [
            jnp.where(top, work[k, pl.ds(8 + c, 1), :], st[k, rows(c), :]) for k in range(5)
        ]
        for w, o in ((U, UO), (V, VO)):
            d = x[w] - sc[o, rows(c), :]
            x.append(0.5 * root(d * d + 0.0025) * d)
        for f, y in enumerate(x):
            for k in range(4):
                stage[f, c // 8, pl.ds(8 * k + c % 8, 8, stride=40), :] = y[8 * k : 8 * k + 8]
    whole = stage.reshape(7, 2, 8, 40, 128)
    copies = []
    for n, (dst, at) in enumerate(((vel_o, 0), (str_o, 2), (oce_o, 5))):
        src = whole.at[pl.ds(at, dst.shape[0]), :, :, pl.ds(0, 32), :]
        copies.append(pltpu.make_async_copy(src, dst, sems.at[n]))
    for c in copies:
        c.start()
    for c in copies:
        c.wait()


ANY = pl.BlockSpec(memory_space=pl.ANY)
VM = pl.BlockSpec(memory_space=pltpu.VMEM)


def shape(*dims):
    return jax.ShapeDtypeStruct(dims, F32)


def swap(b, a):
    n = 128
    cross = [(d, (d + 1) % n if d % 2 else (d - 1) % n) for d in range(n)]
    chip = [(d, d ^ 1) for d in range(n)]
    return lax.ppermute(b, AXES, cross), lax.ppermute(a, AXES, chip)


def coriolis():
    b = 4 * np.arange(8)[None, :] + np.arange(4)[:, None]
    j = b.reshape(32, 1) * 128 + np.arange(128)[None, :]
    return (0.5 * np.sin(math.pi * ((j + 0.5) / 4096 - 0.5))).astype(np.float32)


def staging():
    return [
        pltpu.VMEM((11, *STAGE), F32),
        pltpu.VMEM((1, *STAGE), jnp.int32),
        pltpu.SemaphoreType.DMA((5,)),
    ]


def on_device(forcing, ice_state, velocity, stress, ice_mask):
    raw = [view(x) for x in (forcing, ice_state, velocity, stress, ice_mask[None])]
    n1, n2 = len(FIRST) * R, len(SECOND) * R + 2 * TOP * 8
    b, a, m = pl.pallas_call(
        pack_kernel,
        out_shape=[shape(n1, 128), shape(n1, 128), shape(TOP * C, 128)],
        in_specs=[ANY] * 5,
        out_specs=[VM] * 3,
        scratch_shapes=staging(),
        compiler_params=pltpu.CompilerParams(vmem_limit_bytes=24 << 20),
        name="pack",
    )(*raw)
    rb, ra = swap(b, a)
    rm = lax.ppermute(m, AXES, [(d, 127 - d) for d in range(128)])
    cor = jnp.asarray(coriolis())
    st, sc, strip, b, a = pl.pallas_call(
        first_kernel,
        out_shape=[
            shape(5, NC * R, 128),
            shape(9, NC * R, 128),
            shape(2 * TOP, R, 128),
            shape(n2, 128),
            shape(n2, 128),
        ],
        in_specs=[ANY] * 5 + [VM] * 4,
        out_specs=[VM] * 5,
        scratch_shapes=[pltpu.VMEM((6, NC * R, 128), F32), *staging()],
        compiler_params=pltpu.CompilerParams(vmem_limit_bytes=32 << 20),
        name="first",
    )(*raw, rb, ra, rm, cor)
    rb, ra = swap(b, a)
    vel, strs, ocean = pl.pallas_call(
        second_kernel,
        out_shape=[shape(n, 2, 8, 32, 128) for n in (2, 3, 2)],
        in_specs=[VM] * 6,
        out_specs=[ANY] * 3,
        scratch_shapes=[
            pltpu.VMEM((5, NC * R, 128), F32),
            pltpu.VMEM((6, NC * R, 128), F32),
            pltpu.VMEM((2 * TOP, R, 128), F32),
            pltpu.VMEM((28, R, 128), F32),
            pltpu.VMEM((7, *STAGE), F32),
            pltpu.SemaphoreType.DMA((3,)),
        ],
        compiler_params=pltpu.CompilerParams(vmem_limit_bytes=32 << 20),
        name="second",
    )(st, sc, strip, rb, ra, cor)
    return unview(vel), unview(strs), unview(ocean)


def solution(mesh):
    slab = P(None, AXES, None)
    return jax.shard_map(
        on_device,
        mesh=mesh,
        in_specs=(slab, slab, slab, slab, P(AXES, None)),
        out_specs=(slab, slab, slab),
        check_vma=False,
    )
```

```python
import math

import jax
import jax.numpy as jnp
import numpy as np
from jax import lax
from jax.experimental import pallas as pl
from jax.experimental.pallas import tpu as pltpu
from jax.sharding import PartitionSpec as P

F32 = jnp.float32
AXES = ("gx", "gy")
C = 16
R = 32
H = 3
NC = C + 2 * H
FIELDS = ("uo", "vo", "tx", "ty", "a", "h", "u", "v", "s1", "s2", "s12", "mask")
WHERE = {n: k for k, n in enumerate(FIELDS)}
STATE = ("u", "v", "s1", "s2", "s12")
NEAR = [(n, 1) for n in ("a", "h", "u", "v", "s1", "s2", "s12", "mask", "o", "t")]
FIRST = [(n, 0) for n in FIELDS] + NEAR + [("u", 2), ("v", 2)]
SECOND = [(n, m) for m in range(2) for n in STATE] + [("u", 2), ("v", 2)]
U, V, S1, S2, S12 = range(5)
PR, MI, UO, CU, VO, CV, MK, OU, OV = range(9)
T, D2, W, DV2, E1, UP = range(6)
K29 = 29.0 / 30.0
STAGE = (2, 8 * 40, 128)
TOP = len(FIELDS)


def view(x):
    c = x.shape[0]
    return x.reshape(c, 2, 8, 8, 4, 128).transpose(0, 1, 3, 4, 2, 5).reshape(c, 2, 8, 32, 128)


def unview(y):
    c = y.shape[0]
    return y.reshape(c, 2, 8, 4, 8, 128).transpose(0, 1, 4, 2, 3, 5).reshape(c, C, 4096)


def iotas(shape):
    return lax.broadcasted_iota(jnp.int32, shape, 0), lax.broadcasted_iota(jnp.int32, shape, 1)


def root(x):
    return x * lax.rsqrt(jnp.maximum(x, 1e-30))


def below(x, masks):
    lane0, _, sub0, _ = masks
    r = pltpu.roll(x, 1, 1)
    q = jnp.where(sub0, 0.0, pltpu.roll(r[24:32], 1, 0))
    return jnp.where(lane0, jnp.concatenate([q, r[0:24]], 0), r)


def above(x, masks):
    _, lane127, _, _ = masks
    r = pltpu.roll(x, 127, 1)
    q = pltpu.roll(r[0:8], 7, 0)
    return jnp.where(lane127, jnp.concatenate([r[8:32], q], 0), r)


def make_masks():
    _, lane = iotas((R, 128))
    sub, _ = iotas((8, 128))
    return lane == 0, lane == 127, sub == 0, sub == 7


def rows(c):
    return pl.ds(pl.multiple_of((c + H) * R, R), R)


def each_column(span, body):
    if isinstance(span, tuple):
        lo, hi, chunk = span

        def step(t, carry):
            for q in range(chunk):
                body(lo + t * chunk + q)
            return carry

        lax.fori_loop(0, (hi - lo) // chunk, step, 0)
    else:
        for c in span:
            body(c)


def stress_terms(x1, e1, sc4, x, y, s, p):
    d = x1 + e1
    e = x1 - e1
    delta = root(d * d + 0.25 * (e * e) + (1.0 / 64.0) * (sc4 * sc4))
    r = p / (delta + 0.05)
    dk = x + y
    ek = x - y
    dk2 = root((1.0 / 16.0) * (dk * dk) + (1.0 / 64.0) * (ek * ek) + 0.25 * (s * s))
    rk = p / (dk2 + 0.05)
    return r * (d - delta), r * (0.25 * e), rk * (0.125 * s)


def momentum(w, o, c, mi, force, cor, ice, open_o):
    g = 0.5 * root((o - w) * (o - w) + 0.0025) * mi
    new = (30.0 * w + c + force * mi + g * o + cor) / (31.0 + g)
    return jnp.where(ice, new, open_o)


def subcycle(st, sc, tmp, f4, masks, vel, stress, mom):
    def shift(c):
        u, v = st[U, rows(c), :], st[V, rows(c), :]
        up, um = above(u, masks), below(u, masks)
        vp, vm = above(v, masks), below(v, masks)
        tmp[T, rows(c), :] = u + up
        tmp[D2, rows(c), :] = up - um
        tmp[UP, rows(c), :] = up - u
        tmp[W, rows(c), :] = v + vm
        tmp[E1, rows(c), :] = v - vm
        tmp[DV2, rows(c), :] = vp - vm

    each_column(vel, shift)

    def strain(c):
        ld = lambda k, d=0: tmp[k, rows(c + d), :]
        us = lambda d: st[U, rows(c + d), :]
        vs = lambda d: st[V, rows(c + d), :]
        a1, a2, a12 = stress_terms(
            us(0) - us(-1),
            ld(E1),
            (ld(D2) + ld(D2, -1)) + (ld(W, 1) - ld(W, -1)),
            ld(T, 1) - ld(T, -1),
            ld(DV2) + ld(DV2, 1),
            ld(UP) + (vs(1) - vs(0)),
            sc[PR, rows(c), :],
        )
        st[S1, rows(c), :] = K29 * st[S1, rows(c), :] + a1
        st[S2, rows(c), :] = K29 * st[S2, rows(c), :] + a2
        st[S12, rows(c), :] = K29 * st[S12, rows(c), :] + a12

    each_column(stress, strain)

    def move(c):
        ss = lambda k, d=0: st[k, rows(c + d), :]
        q1 = ss(S1) + ss(S2)
        q1n = ss(S1, 1) + ss(S2, 1)
        q2 = ss(S1) - ss(S2)
        s12 = ss(S12)
        fu = 0.5 * (q1n - q1) + (s12 - below(s12, masks))
        fv = 0.5 * (above(q2, masks) - q2) + (s12 - ss(S12, -1))
        cu = f4 * (tmp[W, rows(c), :] + tmp[W, rows(c + 1), :])
        cv = f4 * (tmp[T, rows(c), :] + tmp[T, rows(c - 1), :])
        k = lambda n: sc[n, rows(c), :]
        ice = k(MK) == 2.0
        mi = k(MI)
        st[U, rows(c), :] = momentum(ss(U), k(UO), k(CU), mi, fu, cu, ice, k(OU))
        st[V, rows(c), :] = momentum(ss(V), k(VO), k(CV), mi, fv, -cv, ice, k(OV))

    each_column(mom, move)


def both(a, b, c, d):
    return [*range(a, b), *range(c, d)]


def interior(st, sc, tmp1, tmp2, f4):
    masks = make_masks()
    subcycle(st, sc, tmp1, f4, masks, (0, 16, 8), (1, 15, 7), (2, 14, 6))
    subcycle(st, sc, tmp2, f4, masks, (2, 14, 6), (3, 13, 5), (4, 12, 4))


def edges(st, sc, tmp1, tmp2, f4):
    masks = make_masks()
    subcycle(
        st, sc, tmp1, f4, masks, both(-3, 0, 16, 19), both(-2, 1, 15, 18), both(-2, 2, 14, 18)
    )
    subcycle(
        st, sc, tmp2, f4, masks, both(-2, 2, 14, 18), both(-1, 3, 13, 17), both(0, 4, 12, 16)
    )


def statics(raw):
    a, h, mask = raw["a"], raw["h"], raw["mask"]
    ice = mask == 2.0
    opened = mask == 1.0
    mi = 1.0 / (a * h)
    out = {
        PR: jnp.where(ice, h * jnp.exp(-20.0 * (1.0 - a)) * (1.0 / 30.0), 0.0),
        MI: mi,
        UO: raw["uo"],
        CU: raw["u"] + raw["tx"] * mi,
        VO: raw["vo"],
        CV: raw["v"] + raw["ty"] * mi,
        MK: mask,
        OU: jnp.where(opened, raw["uo"], 0.0),
        OV: jnp.where(opened, raw["vo"], 0.0),
    }
    return out, ice


def put_column(st, sc, at, raw):
    out, ice = statics(raw)
    for k, x in out.items():
        sc[k, at, :] = x
    st[U, at, :] = raw["u"]
    st[V, at, :] = raw["v"]
    st[S1, at, :] = jnp.where(ice, raw["s1"], 0.0)
    st[S2, at, :] = jnp.where(ice, raw["s2"], 0.0)
    st[S12, at, :] = jnp.where(ice, raw["s12"], 0.0)


def stage_in(srcs, stage, mstage, sems):
    copies = []
    at = 0
    for k, src in enumerate(srcs):
        n = src.shape[0]
        if k < 4:
            dst = stage.reshape(11, 2, 8, 40, 128).at[pl.ds(at, n), :, :, pl.ds(0, 32), :]
        else:
            dst = mstage.reshape(1, 2, 8, 40, 128).at[:, :, :, pl.ds(0, 32), :]
        copies.append(pltpu.make_async_copy(src, dst, sems.at[k]))
        at += n
    for c in copies:
        c.start()
    for c in copies:
        c.wait()


def staged_column(stage, mstage, name, c):
    ref, f = (mstage, 0) if name == "mask" else (stage, WHERE[name])
    parts = [ref[f, c // 8, pl.ds(8 * k + c % 8, 8, stride=40), :] for k in range(4)]
    return jnp.concatenate(parts, 0).astype(F32)


def parity():
    return lax.rem(lax.axis_index("gy"), 2)


def squeeze(tiles):
    _, lane = iotas((8, 128))
    out = []
    for t in range(0, len(tiles), 8):
        x = tiles[t + 7]
        for g in range(7):
            x = jnp.where(lane // 16 == g, pltpu.roll(tiles[t + g], 16 * (g + 1), 1), x)
        out.append(x)
    return out


def spread(packed, n):
    x = packed[n // 8]
    g = n % 8
    return x if g == 7 else pltpu.roll(x, 128 - 16 * (g + 1), 1)


def top_tile(stage, mstage, k, ih):
    ref, f = (mstage, 0) if k == TOP - 1 else (stage, k)
    return ref[f, ih, pl.ds(7 * 40 + 24, 8), :].astype(F32)


def pack_kernel(f_ref, i_ref, v_ref, s_ref, m_ref, b_out, a_out, m_out, stage, mstage, sems):
    stage_in((f_ref, i_ref, v_ref, s_ref, m_ref), stage, mstage, sems)
    even = parity() == 0
    for n, (name, m) in enumerate(FIRST):
        far = {"o": ("vo", "uo"), "t": ("ty", "tx")}.get(name, (name, name))
        left = staged_column(stage, mstage, far[0], m)
        right = staged_column(stage, mstage, far[1], C - 1 - m)
        b_out[pl.ds(n * R, R), :] = jnp.where(even, left, right)
        a_out[pl.ds(n * R, R), :] = jnp.where(even, right, left)
    tops = squeeze([top_tile(stage, mstage, k, ih) for k in range(TOP) for ih in range(2)])
    for n, x in enumerate(tops):
        m_out[pl.ds(8 * n, 8), :] = x


def halo_rows(even, m):
    left, right = (H - 1 - m) * R, (H + C + m) * R
    via_b = pl.ds(pl.multiple_of(jnp.where(even, left, right), R), R)
    via_a = pl.ds(pl.multiple_of(jnp.where(even, right, left), R), R)
    return via_b, via_a


def first_interior(
    f_ref, i_ref, v_ref, s_ref, m_ref, cor, st, sc, tmp1, tmp2, strip, f4, stage, mstage, sems
):
    stage_in((f_ref, i_ref, v_ref, s_ref, m_ref), stage, mstage, sems)
    zero = jnp.zeros((R, 128), F32)
    for k in (S1, S2, S12):
        st[k, rows(-3), :] = zero
        st[k, rows(18), :] = zero
    f4[...] = 0.25 * cor[...]
    for c in range(C):
        put_column(
            st, sc, rows(c), {name: staged_column(stage, mstage, name, c) for name in FIELDS}
        )
    for k in range(TOP):
        for ih in range(2):
            strip[k, pl.ds(8 + 8 * ih, 8), :] = top_tile(stage, mstage, k, ih)
    interior(st, sc, tmp1, tmp2, f4[...])


def first_edges(*refs):
    rb, ra, rm, f4 = refs[:4]
    st, sc, tmp1, tmp2, strip, b_out, a_out = refs[9:]
    even = parity() == 0
    for m in range(H):
        via = halo_rows(even, m)
        for at, src in zip(via, (rb, ra)):
            raw = {
                name: src[pl.ds(n * R, R), :] for n, (name, d) in enumerate(FIRST) if d == m
            }
            if m == 1:
                raw["uo"] = raw["vo"] = raw["o"]
                raw["tx"] = raw["ty"] = raw["t"]
            if m < 2:
                put_column(st, sc, at, raw)
            else:
                st[U, at, :] = raw["u"]
                st[V, at, :] = raw["v"]
    flip = 7 - iotas((8, 128))[0]
    packed = [rm[pl.ds(8 * n, 8), :] for n in range(3)]
    for k in range(TOP):
        for ih in range(2):
            x = spread(packed, 2 * k + ih)
            strip[TOP + k, pl.ds(16 - 8 * ih, 8), :] = jnp.take_along_axis(x, flip, axis=0)
    edges(st, sc, tmp1, tmp2, f4[...])
    for n, (name, m) in enumerate(SECOND):
        left = st[STATE.index(name), rows(m), :]
        right = st[STATE.index(name), rows(C - 1 - m), :]
        b_out[pl.ds(n * R, R), :] = jnp.where(even, left, right)
        a_out[pl.ds(n * R, R), :] = jnp.where(even, right, left)
    base = len(SECOND) * R
    left = squeeze([strip[k, pl.ds(8, 8), :] for k in range(2 * TOP)])
    right = squeeze([strip[k, pl.ds(16, 8), :] for k in range(2 * TOP)])
    for n in range(3):
        b_out[pl.ds(base + 8 * n, 8), :] = jnp.where(even, left[n], right[n])
        a_out[pl.ds(base + 8 * n, 8), :] = jnp.where(even, right[n], left[n])


def second_interior(*refs):
    f4, (st, sc, tmp1, tmp2) = refs[0], refs[5:]
    interior(st, sc, tmp1, tmp2, f4[...])


def run_strips(strip, work, cor4):
    _, lane = iotas((R, 128))
    last = lane == 127
    f4 = jnp.broadcast_to(cor4[pl.ds(31, 1), :], (R, 128))
    for side in range(2):
        raw = {name: strip[side * TOP + k] for k, name in enumerate(FIELDS)}
        out, ice = statics(raw)
        work[5 * side + U] = raw["u"]
        work[5 * side + V] = raw["v"]
        for k, name in ((S1, "s1"), (S2, "s2"), (S12, "s12")):
            work[5 * side + k] = jnp.where(ice, raw[name], 0.0)
        for k in range(9):
            work[10 + 9 * side + k] = out[k]

    def step():
        x = [[work[5 * side + k] for k in range(5)] for side in range(2)]
        east = [lambda y: pltpu.roll(y, R - 1, 0), lambda y: pltpu.roll(y, 1, 0)]
        west = [east[1], east[0]]
        down = lambda y: pltpu.roll(y, 1, 1)
        up = lambda y, other, sign: jnp.where(last, sign * other, pltpu.roll(y, 127, 1))
        terms = []
        for side in range(2):
            e, w = east[side], west[side]
            u, v = x[side][U], x[side][V]
            ou, ov = x[1 - side][U], x[1 - side][V]
            upu, um, vp, vm = up(u, ou, -1.0), down(u), up(v, ov, -1.0), down(v)
            tt, d2, ww, dv2 = u + upu, upu - um, v + vm, vp - vm
            terms.append((tt, ww))
            k = lambda n: work[10 + 9 * side + n]
            a1, a2, a12 = stress_terms(
                u - w(u),
                v - vm,
                (d2 + w(d2)) + (e(ww) - w(ww)),
                e(tt) - w(tt),
                dv2 + e(dv2),
                (upu - u) + (e(v) - v),
                k(PR),
            )
            x[side][S1] = K29 * x[side][S1] + a1
            x[side][S2] = K29 * x[side][S2] + a2
            x[side][S12] = K29 * x[side][S12] + a12
        new = []
        for side in range(2):
            e, w = east[side], west[side]
            u, v, s1, s2, s12 = x[side]
            q1, q2 = s1 + s2, s1 - s2
            other = x[1 - side][S1] - x[1 - side][S2]
            fu = 0.5 * (e(q1) - q1) + (s12 - down(s12))
            fv = 0.5 * (up(q2, other, 1.0) - q2) + (s12 - w(s12))
            tt, ww = terms[side]
            k = lambda n: work[10 + 9 * side + n]
            ice = k(MK) == 2.0
            nu = momentum(u, k(UO), k(CU), k(MI), fu, f4 * (ww + e(ww)), ice, k(OU))
            nv = momentum(v, k(VO), k(CV), k(MI), fv, -f4 * (tt + w(tt)), ice, k(OV))
            new.append((nu, nv, s1, s2, s12))
        for side in range(2):
            for k in range(5):
                work[5 * side + k] = new[side][k]

    return step


def second_edges(*refs):
    rb, ra, f4 = refs[:3]
    vel_o, str_o, oce_o, st, sc, tmp1, tmp2, strip, work, stage, sems = refs[8:]
    even = parity() == 0
    for m in range(H):
        via = halo_rows(even, m)
        for at, src in zip(via, (rb, ra)):
            for n, (name, d) in enumerate(SECOND):
                if d == m:
                    st[STATE.index(name), at, :] = src[pl.ds(n * R, R), :]
    base = len(SECOND) * R
    pb = [rb[pl.ds(base + 8 * n, 8), :] for n in range(3)]
    pa = [ra[pl.ds(base + 8 * n, 8), :] for n in range(3)]
    low = [jnp.where(even, b, a) for b, a in zip(pb, pa)]
    high = [jnp.where(even, a, b) for b, a in zip(pb, pa)]
    for k in range(2 * TOP):
        strip[k, pl.ds(0, 8), :] = spread(low, k)
        strip[k, pl.ds(24, 8), :] = spread(high, k)
    step = run_strips(strip, work, f4)
    for _ in range(4):
        step()
    edges(st, sc, tmp1, tmp2, f4[...])
    row, lane = iotas((R, 128))
    top = (row == R - 1) & (lane >= 120)

    for c in range(C):
        x = [
            jnp.where(top, work[k, pl.ds(8 + c, 1), :], st[k, rows(c), :]) for k in range(5)
        ]
        for w, o in ((U, UO), (V, VO)):
            d = x[w] - sc[o, rows(c), :]
            x.append(0.5 * root(d * d + 0.0025) * d)
        for f, y in enumerate(x):
            for k in range(4):
                stage[f, c // 8, pl.ds(8 * k + c % 8, 8, stride=40), :] = y[8 * k : 8 * k + 8]
    whole = stage.reshape(7, 2, 8, 40, 128)
    copies = []
    for n, (dst, at) in enumerate(((vel_o, 0), (str_o, 2), (oce_o, 5))):
        src = whole.at[pl.ds(at, dst.shape[0]), :, :, pl.ds(0, 32), :]
        copies.append(pltpu.make_async_copy(src, dst, sems.at[n]))
    for c in copies:
        c.start()
    for c in copies:
        c.wait()


HBM = pl.BlockSpec(memory_space=pltpu.HBM)
VM = pl.BlockSpec(memory_space=pltpu.VMEM)


def shape(*dims):
    return jax.ShapeDtypeStruct(dims, F32)


def swap(b, a):
    n = 128
    cross = [(d, (d + 1) % n if d % 2 else (d - 1) % n) for d in range(n)]
    chip = [(d, d ^ 1) for d in range(n)]
    return lax.ppermute(b, AXES, cross), lax.ppermute(a, AXES, chip)


def coriolis():
    b = 4 * np.arange(8)[None, :] + np.arange(4)[:, None]
    j = b.reshape(32, 1) * 128 + np.arange(128)[None, :]
    return (0.5 * np.sin(math.pi * ((j + 0.5) / 4096 - 0.5))).astype(np.float32)


def staging():
    return [
        pltpu.VMEM((11, *STAGE), F32),
        pltpu.VMEM((1, *STAGE), jnp.int32),
        pltpu.SemaphoreType.DMA((5,)),
    ]


def call(kernel, name, out, ins, specs, scratch, alias=None, outs=None, cost=None):
    return pl.pallas_call(
        kernel,
        out_shape=out,
        in_specs=specs,
        out_specs=outs or [VM] * len(out),
        scratch_shapes=scratch,
        input_output_aliases=alias or {},
        compiler_params=pltpu.CompilerParams(vmem_limit_bytes=20 << 20),
        cost_estimate=cost,
        name=name,
    )(*ins)


def on_device(forcing, ice_state, velocity, stress, ice_mask):
    raw = [
        pltpu.with_memory_space_constraint(view(x), pltpu.HBM)
        for x in (forcing, ice_state, velocity, stress, ice_mask[None])
    ]
    n1, n2 = len(FIRST) * R, len(SECOND) * R + 24
    b, a, m = call(
        pack_kernel,
        "pack",
        [shape(n1, 128), shape(n1, 128), shape(24, 128)],
        raw,
        [HBM] * 5,
        staging(),
    )
    rb, ra = swap(b, a)
    rm = lax.ppermute(m, AXES, [(d, 127 - d) for d in range(128)])
    cor = jnp.asarray(coriolis())
    cost = pl.CostEstimate(flops=20_000_000, bytes_accessed=4_000_000, transcendentals=500_000)
    main = [shape(5, NC * R, 128), shape(9, NC * R, 128), *[shape(6, NC * R, 128)] * 2]
    strips = shape(2 * TOP, R, 128)
    *state, strip, f4 = call(
        first_interior,
        "interior1",
        [*main, strips, shape(R, 128)],
        [*raw, cor],
        [HBM] * 5 + [VM],
        staging(),
        cost=cost,
    )
    *state, strip, b, a = call(
        first_edges,
        "edges1",
        [*main, strips, shape(n2, 128), shape(n2, 128)],
        [rb, ra, rm, f4, *state, strip],
        [VM] * 9,
        [],
        alias={4 + k: k for k in range(5)},
    )
    rb, ra = swap(b, a)
    state = call(
        second_interior,
        "interior2",
        main,
        [f4, *state],
        [VM] * 5,
        [],
        alias={1 + k: k for k in range(4)},
        cost=cost,
    )
    vel, strs, ocean, *_ = call(
        second_edges,
        "edges2",
        [*[shape(n, 2, 8, 32, 128) for n in (2, 3, 2)], *main, strips],
        [rb, ra, f4, *state, strip],
        [VM] * 8,
        [
            pltpu.VMEM((28, R, 128), F32),
            pltpu.VMEM((7, *STAGE), F32),
            pltpu.SemaphoreType.DMA((3,)),
        ],
        alias={3 + k: 3 + k for k in range(5)},
        outs=[HBM] * 3 + [VM] * 5,
    )
    return unview(vel), unview(strs), unview(ocean)


def solution(mesh):
    slab = P(None, AXES, None)
    return jax.shard_map(
        on_device,
        mesh=mesh,
        in_specs=(slab, slab, slab, slab, P(AXES, None)),
        out_specs=(slab, slab, slab),
        check_vma=False,
    )
```

```python
import math

import jax
import jax.numpy as jnp
import numpy as np
from jax import lax
from jax.experimental import pallas as pl
from jax.experimental.pallas import tpu as pltpu
from jax.sharding import PartitionSpec as P

F32 = jnp.float32
AXES = ("gx", "gy")
C = 16
R = 32
H = 3
NC = C + 2 * H
FIELDS = ("uo", "vo", "tx", "ty", "a", "h", "u", "v", "s1", "s2", "s12", "mask")
WHERE = {n: k for k, n in enumerate(FIELDS)}
STATE = ("u", "v", "s1", "s2", "s12")
NEXT = ("u", "v", "z", "alpha", "beta")
U, V, S1, S2, S12 = range(5)
PR, MI, UO, CU, VO, CV, MK, OU, OV = range(9)
T, D2, W, DV2, E1, UP = range(6)
K29 = 29.0 / 30.0
STAGE = (2, 8 * 40, 128)
TOP = len(FIELDS)


def view(x):
    c = x.shape[0]
    return x.reshape(c, 2, 8, 8, 4, 128).transpose(0, 1, 3, 4, 2, 5).reshape(c, 2, 8, 32, 128)


def unview(y):
    c = y.shape[0]
    return y.reshape(c, 2, 8, 4, 8, 128).transpose(0, 1, 4, 2, 3, 5).reshape(c, C, 4096)


def iotas(shape):
    return lax.broadcasted_iota(jnp.int32, shape, 0), lax.broadcasted_iota(jnp.int32, shape, 1)


def root(x):
    return x * lax.rsqrt(jnp.maximum(x, 1e-30))


def below(x, masks):
    lane0, _, sub0, _ = masks
    r = pltpu.roll(x, 1, 1)
    q = jnp.where(sub0, 0.0, pltpu.roll(r[24:32], 1, 0))
    return jnp.where(lane0, jnp.concatenate([q, r[0:24]], 0), r)


def above(x, masks):
    _, lane127, _, _ = masks
    r = pltpu.roll(x, 127, 1)
    q = pltpu.roll(r[0:8], 7, 0)
    return jnp.where(lane127, jnp.concatenate([r[8:32], q], 0), r)


def make_masks():
    _, lane = iotas((R, 128))
    sub, _ = iotas((8, 128))
    return lane == 0, lane == 127, sub == 0, sub == 7


def rows(c):
    return pl.ds(pl.multiple_of((c + H) * R, R), R)


def each_column(span, body):
    if isinstance(span, tuple):
        lo, hi, chunk = span

        def step(t, carry):
            for q in range(chunk):
                body(lo + t * chunk + q)
            return carry

        lax.fori_loop(0, (hi - lo) // chunk, step, 0)
    else:
        for c in span:
            body(c)


def stress_terms(x1, e1, sc4, x, y, s, p):
    d = x1 + e1
    e = x1 - e1
    delta = root(d * d + 0.25 * (e * e) + (1.0 / 64.0) * (sc4 * sc4))
    r = p / (delta + 0.05)
    dk = x + y
    ek = x - y
    dk2 = root((1.0 / 16.0) * (dk * dk) + (1.0 / 64.0) * (ek * ek) + 0.25 * (s * s))
    rk = p / (dk2 + 0.05)
    return r * (d - delta), r * (0.25 * e), rk * (0.125 * s)


def momentum(w, o, c, mi, force, cor, ice, open_o):
    g = 0.5 * root((o - w) * (o - w) + 0.0025) * mi
    new = (30.0 * w + c + force * mi + g * o + cor) / (31.0 + g)
    return jnp.where(ice, new, open_o)


def subcycle(st, sc, tmp, f4, masks, vel, stress, mom):
    def shift(c):
        u, v = st[U, rows(c), :], st[V, rows(c), :]
        up, um = above(u, masks), below(u, masks)
        vp, vm = above(v, masks), below(v, masks)
        tmp[T, rows(c), :] = u + up
        tmp[D2, rows(c), :] = up - um
        tmp[UP, rows(c), :] = up - u
        tmp[W, rows(c), :] = v + vm
        tmp[E1, rows(c), :] = v - vm
        tmp[DV2, rows(c), :] = vp - vm

    each_column(vel, shift)

    def strain(c):
        ld = lambda k, d=0: tmp[k, rows(c + d), :]
        us = lambda d: st[U, rows(c + d), :]
        vs = lambda d: st[V, rows(c + d), :]
        a1, a2, a12 = stress_terms(
            us(0) - us(-1),
            ld(E1),
            (ld(D2) + ld(D2, -1)) + (ld(W, 1) - ld(W, -1)),
            ld(T, 1) - ld(T, -1),
            ld(DV2) + ld(DV2, 1),
            ld(UP) + (vs(1) - vs(0)),
            sc[PR, rows(c), :],
        )
        st[S1, rows(c), :] = K29 * st[S1, rows(c), :] + a1
        st[S2, rows(c), :] = K29 * st[S2, rows(c), :] + a2
        st[S12, rows(c), :] = K29 * st[S12, rows(c), :] + a12

    each_column(stress, strain)

    def move(c):
        ss = lambda k, d=0: st[k, rows(c + d), :]
        q1 = ss(S1) + ss(S2)
        q1n = ss(S1, 1) + ss(S2, 1)
        q2 = ss(S1) - ss(S2)
        s12 = ss(S12)
        fu = 0.5 * (q1n - q1) + (s12 - below(s12, masks))
        fv = 0.5 * (above(q2, masks) - q2) + (s12 - ss(S12, -1))
        cu = f4 * (tmp[W, rows(c), :] + tmp[W, rows(c + 1), :])
        cv = f4 * (tmp[T, rows(c), :] + tmp[T, rows(c - 1), :])
        k = lambda n: sc[n, rows(c), :]
        ice = k(MK) == 2.0
        mi = k(MI)
        st[U, rows(c), :] = momentum(ss(U), k(UO), k(CU), mi, fu, cu, ice, k(OU))
        st[V, rows(c), :] = momentum(ss(V), k(VO), k(CV), mi, fv, -cv, ice, k(OV))

    each_column(mom, move)


def both(a, b, c, d):
    return [*range(a, b), *range(c, d)]


def interior(st, sc, tmp1, tmp2, f4):
    masks = make_masks()
    subcycle(st, sc, tmp1, f4, masks, (0, 16, 8), (1, 15, 7), (2, 14, 6))
    subcycle(st, sc, tmp2, f4, masks, (2, 14, 6), (3, 13, 5), (4, 12, 4))


def edges(st, sc, tmp1, tmp2, f4, left, right):
    masks = make_masks()
    st[U, rows(-2), :], st[V, rows(-2), :] = left["u"], left["v"]
    st[U, rows(17), :], st[V, rows(17), :] = right["u"], right["v"]
    st[S12, rows(-2), :] = left["z"]
    st[S1, rows(17), :] = right["z"]
    st[S2, rows(17), :] = jnp.zeros((R, 128), F32)
    subcycle(
        st, sc, tmp1, f4, masks, both(-2, 0, 16, 18), both(-1, 1, 15, 17), both(-1, 2, 14, 17)
    )
    n11 = 0.5 * (st[S1, rows(-1), :] + st[S2, rows(-1), :])
    st[U, rows(-2), :] = left["alpha"] + left["beta"] * n11
    st[V, rows(17), :] = right["alpha"] - right["beta"] * st[S12, rows(16), :]
    subcycle(
        st, sc, tmp2, f4, masks, both(-2, 2, 14, 18), both(-1, 3, 13, 17), both(0, 4, 12, 16)
    )


def outgoing(st, sc, f4):
    masks = make_masks()

    def around(c):
        s = lambda k, d=0: st[k, rows(c + d), :]
        f = lambda k: sc[k, rows(c), :]
        t, d2, w, dv2 = [], [], [], []
        for d in (-1, 0, 1):
            u, v = s(U, d), s(V, d)
            up, um, vp, vm = above(u, masks), below(u, masks), above(v, masks), below(v, masks)
            t.append(u + up)
            d2.append(up - um)
            w.append(v + vm)
            dv2.append(vp - vm)
            if d == 0:
                e1, rise = v - vm, up - u
        a1, a2, a12 = stress_terms(
            s(U) - s(U, -1),
            e1,
            (d2[1] + d2[0]) + (w[2] - w[0]),
            t[2] - t[0],
            dv2[1] + dv2[2],
            rise + (s(V, 1) - s(V)),
            f(PR),
        )
        s1, s2, s12 = K29 * s(S1) + a1, K29 * s(S2) + a2, K29 * s(S12) + a12
        return s, f, t, w, s1 + s2, s1 - s2, s12

    def numbers(x, o, c, mi, force, cor, ice, open_o):
        g = 0.5 * root((o - x) * (o - x) + 0.0025) * mi
        b = 1.0 / (31.0 + g)
        a = (30.0 * x + c + force * mi + g * o + cor) * b
        return jnp.where(ice, a, open_o), jnp.where(ice, mi * b, 0.0)

    s, f, t, w, q1, q2, s12 = around(1)
    force = 0.5 * (above(q2, masks) - q2) + s12
    ab = numbers(
        s(V), f(VO), f(CV), f(MI), force, -f4 * (t[1] + t[0]), f(MK) == 2.0, f(OV)
    )
    left = (s(U), s(V), q1, *ab)
    s, f, t, w, q1, q2, s12 = around(C - 2)
    force = (s12 - below(s12, masks)) - 0.5 * q1
    ab = numbers(s(U), f(UO), f(CU), f(MI), force, f4 * (w[1] + w[2]), f(MK) == 2.0, f(OU))
    return left, (s(U), s(V), s12, *ab)


def send(b_out, a_out, n, left, right, even):
    b_out[pl.ds(n * R, R), :] = jnp.where(even, left, right)
    a_out[pl.ds(n * R, R), :] = jnp.where(even, right, left)


def receive(rb, ra, names, even):
    left, right = {}, {}
    for n, name in enumerate(names):
        b, a = rb[pl.ds(n * R, R), :], ra[pl.ds(n * R, R), :]
        left[name], right[name] = jnp.where(even, b, a), jnp.where(even, a, b)
    return left, right


def statics(raw):
    a, h, mask = raw["a"], raw["h"], raw["mask"]
    ice = mask == 2.0
    opened = mask == 1.0
    mi = 1.0 / (a * h)
    out = {
        PR: jnp.where(ice, h * jnp.exp(-20.0 * (1.0 - a)) * (1.0 / 30.0), 0.0),
        MI: mi,
        UO: raw["uo"],
        CU: raw["u"] + raw["tx"] * mi,
        VO: raw["vo"],
        CV: raw["v"] + raw["ty"] * mi,
        MK: mask,
        OU: jnp.where(opened, raw["uo"], 0.0),
        OV: jnp.where(opened, raw["vo"], 0.0),
    }
    return out, ice


def put_column(st, sc, at, raw):
    out, ice = statics(raw)
    for k, x in out.items():
        sc[k, at, :] = x
    st[U, at, :] = raw["u"]
    st[V, at, :] = raw["v"]
    st[S1, at, :] = jnp.where(ice, raw["s1"], 0.0)
    st[S2, at, :] = jnp.where(ice, raw["s2"], 0.0)
    st[S12, at, :] = jnp.where(ice, raw["s12"], 0.0)


def stage_in(srcs, stage, mstage, sems):
    copies = []
    at = 0
    for k, src in enumerate(srcs):
        n = src.shape[0]
        if k < 4:
            dst = stage.reshape(11, 2, 8, 40, 128).at[pl.ds(at, n), :, :, pl.ds(0, 32), :]
        else:
            dst = mstage.reshape(1, 2, 8, 40, 128).at[:, :, :, pl.ds(0, 32), :]
        copies.append(pltpu.make_async_copy(src, dst, sems.at[k]))
        at += n
    for c in copies:
        c.start()
    for c in copies:
        c.wait()


def staged_column(stage, mstage, name, c):
    ref, f = (mstage, 0) if name == "mask" else (stage, WHERE[name])
    parts = [ref[f, c // 8, pl.ds(8 * k + c % 8, 8, stride=40), :] for k in range(4)]
    return jnp.concatenate(parts, 0).astype(F32)


def parity():
    return lax.rem(lax.axis_index("gy"), 2)


def squeeze(tiles):
    _, lane = iotas((8, 128))
    out = []
    for t in range(0, len(tiles), 8):
        x = tiles[t + 7]
        for g in range(7):
            x = jnp.where(lane // 16 == g, pltpu.roll(tiles[t + g], 16 * (g + 1), 1), x)
        out.append(x)
    return out


def spread(packed, n):
    x = packed[n // 8]
    g = n % 8
    return x if g == 7 else pltpu.roll(x, 128 - 16 * (g + 1), 1)


def top_tile(stage, mstage, k, ih):
    ref, f = (mstage, 0) if k == TOP - 1 else (stage, k)
    return ref[f, ih, pl.ds(7 * 40 + 24, 8), :].astype(F32)


def pack_kernel(
    f_ref, i_ref, v_ref, s_ref, m_ref, cor, b_out, a_out, m_out, f4, st, sc, stage, mstage, sems
):
    cor_in = pltpu.make_async_copy(cor, f4, sems.at[5])
    cor_in.start()
    stage_in((f_ref, i_ref, v_ref, s_ref, m_ref), stage, mstage, sems)
    cor_in.wait()
    even = parity() == 0
    for c in (1, C - 2):
        put_column(
            st, sc, rows(c), {name: staged_column(stage, mstage, name, c) for name in FIELDS}
        )
    for c in (0, 2, C - 3, C - 1):
        for k, name in ((U, "u"), (V, "v")):
            st[k, rows(c), :] = staged_column(stage, mstage, name, c)
    for n, name in enumerate(FIELDS):
        left = staged_column(stage, mstage, name, 0)
        right = staged_column(stage, mstage, name, C - 1)
        send(b_out, a_out, n, left, right, even)
    for n, pair in enumerate(zip(*outgoing(st, sc, f4[...]))):
        send(b_out, a_out, TOP + n, *pair, even)
    tops = squeeze([top_tile(stage, mstage, k, ih) for k in range(TOP) for ih in range(2)])
    for n, x in enumerate(tops):
        m_out[pl.ds(8 * n, 8), :] = x


def first_interior(
    f_ref, i_ref, v_ref, s_ref, m_ref, f4, st, sc, tmp1, tmp2, strip, stage, mstage, sems
):
    stage_in((f_ref, i_ref, v_ref, s_ref, m_ref), stage, mstage, sems)
    for c in range(C):
        put_column(
            st, sc, rows(c), {name: staged_column(stage, mstage, name, c) for name in FIELDS}
        )
    for k in range(TOP):
        for ih in range(2):
            strip[k, pl.ds(8 + 8 * ih, 8), :] = top_tile(stage, mstage, k, ih)
    interior(st, sc, tmp1, tmp2, f4[...])


def first_edges(*refs):
    rb, ra, rm, f4 = refs[:4]
    st, sc, tmp1, tmp2, strip, b_out, a_out = refs[9:]
    even = parity() == 0
    left, right = receive(rb, ra, (*FIELDS, *[n + "1" for n in NEXT]), even)
    put_column(st, sc, rows(-1), left)
    put_column(st, sc, rows(C), right)
    flip = 7 - iotas((8, 128))[0]
    packed = [rm[pl.ds(8 * n, 8), :] for n in range(3)]
    for k in range(TOP):
        for ih in range(2):
            x = spread(packed, 2 * k + ih)
            strip[TOP + k, pl.ds(16 - 8 * ih, 8), :] = jnp.take_along_axis(x, flip, axis=0)
    near = [{n: x[n + "1"] for n in NEXT} for x in (left, right)]
    edges(st, sc, tmp1, tmp2, f4[...], *near)
    for k in range(5):
        send(b_out, a_out, k, st[k, rows(0), :], st[k, rows(C - 1), :], even)
    for n, pair in enumerate(zip(*outgoing(st, sc, f4[...]))):
        send(b_out, a_out, 5 + n, *pair, even)
    base = (5 + len(NEXT)) * R
    left = squeeze([strip[k, pl.ds(8, 8), :] for k in range(2 * TOP)])
    right = squeeze([strip[k, pl.ds(16, 8), :] for k in range(2 * TOP)])
    for n in range(3):
        b_out[pl.ds(base + 8 * n, 8), :] = jnp.where(even, left[n], right[n])
        a_out[pl.ds(base + 8 * n, 8), :] = jnp.where(even, right[n], left[n])


def second_interior(*refs):
    f4, (st, sc, tmp1, tmp2) = refs[0], refs[5:]
    interior(st, sc, tmp1, tmp2, f4[...])


def run_strips(strip, work, cor4):
    _, lane = iotas((R, 128))
    last = lane == 127
    f4 = jnp.broadcast_to(cor4[pl.ds(31, 1), :], (R, 128))
    for side in range(2):
        raw = {name: strip[side * TOP + k] for k, name in enumerate(FIELDS)}
        out, ice = statics(raw)
        work[5 * side + U] = raw["u"]
        work[5 * side + V] = raw["v"]
        for k, name in ((S1, "s1"), (S2, "s2"), (S12, "s12")):
            work[5 * side + k] = jnp.where(ice, raw[name], 0.0)
        for k in range(9):
            work[10 + 9 * side + k] = out[k]

    def step():
        x = [[work[5 * side + k] for k in range(5)] for side in range(2)]
        east = [lambda y: pltpu.roll(y, R - 1, 0), lambda y: pltpu.roll(y, 1, 0)]
        west = [east[1], east[0]]
        down = lambda y: pltpu.roll(y, 1, 1)
        up = lambda y, other, sign: jnp.where(last, sign * other, pltpu.roll(y, 127, 1))
        terms = []
        for side in range(2):
            e, w = east[side], west[side]
            u, v = x[side][U], x[side][V]
            ou, ov = x[1 - side][U], x[1 - side][V]
            upu, um, vp, vm = up(u, ou, -1.0), down(u), up(v, ov, -1.0), down(v)
            tt, d2, ww, dv2 = u + upu, upu - um, v + vm, vp - vm
            terms.append((tt, ww))
            k = lambda n: work[10 + 9 * side + n]
            a1, a2, a12 = stress_terms(
                u - w(u),
                v - vm,
                (d2 + w(d2)) + (e(ww) - w(ww)),
                e(tt) - w(tt),
                dv2 + e(dv2),
                (upu - u) + (e(v) - v),
                k(PR),
            )
            x[side][S1] = K29 * x[side][S1] + a1
            x[side][S2] = K29 * x[side][S2] + a2
            x[side][S12] = K29 * x[side][S12] + a12
        new = []
        for side in range(2):
            e, w = east[side], west[side]
            u, v, s1, s2, s12 = x[side]
            q1, q2 = s1 + s2, s1 - s2
            other = x[1 - side][S1] - x[1 - side][S2]
            fu = 0.5 * (e(q1) - q1) + (s12 - down(s12))
            fv = 0.5 * (up(q2, other, 1.0) - q2) + (s12 - w(s12))
            tt, ww = terms[side]
            k = lambda n: work[10 + 9 * side + n]
            ice = k(MK) == 2.0
            nu = momentum(u, k(UO), k(CU), k(MI), fu, f4 * (ww + e(ww)), ice, k(OU))
            nv = momentum(v, k(VO), k(CV), k(MI), fv, -f4 * (tt + w(tt)), ice, k(OV))
            new.append((nu, nv, s1, s2, s12))
        for side in range(2):
            for k in range(5):
                work[5 * side + k] = new[side][k]

    return step


def second_edges(*refs):
    rb, ra, f4 = refs[:3]
    vel_o, str_o, oce_o, st, sc, tmp1, tmp2, strip, work, stage, sems = refs[8:]
    even = parity() == 0
    left, right = receive(rb, ra, (*STATE, *[n + "1" for n in NEXT]), even)
    for k, name in enumerate(STATE):
        st[k, rows(-1), :], st[k, rows(C), :] = left[name], right[name]
    near = [{n: x[n + "1"] for n in NEXT} for x in (left, right)]
    base = (5 + len(NEXT)) * R
    pb = [rb[pl.ds(base + 8 * n, 8), :] for n in range(3)]
    pa = [ra[pl.ds(base + 8 * n, 8), :] for n in range(3)]
    low = [jnp.where(even, b, a) for b, a in zip(pb, pa)]
    high = [jnp.where(even, a, b) for b, a in zip(pb, pa)]
    for k in range(2 * TOP):
        strip[k, pl.ds(0, 8), :] = spread(low, k)
        strip[k, pl.ds(24, 8), :] = spread(high, k)
    step = run_strips(strip, work, f4)
    for _ in range(4):
        step()
    edges(st, sc, tmp1, tmp2, f4[...], *near)
    row, lane = iotas((R, 128))
    top = (row == R - 1) & (lane >= 120)

    for c in range(C):
        x = [
            jnp.where(top, work[k, pl.ds(8 + c, 1), :], st[k, rows(c), :]) for k in range(5)
        ]
        for w, o in ((U, UO), (V, VO)):
            d = x[w] - sc[o, rows(c), :]
            x.append(0.5 * root(d * d + 0.0025) * d)
        for f, y in enumerate(x):
            for k in range(4):
                stage[f, c // 8, pl.ds(8 * k + c % 8, 8, stride=40), :] = y[8 * k : 8 * k + 8]
    whole = stage.reshape(7, 2, 8, 40, 128)
    copies = []
    for n, (dst, at) in enumerate(((vel_o, 0), (str_o, 2), (oce_o, 5))):
        src = whole.at[pl.ds(at, dst.shape[0]), :, :, pl.ds(0, 32), :]
        copies.append(pltpu.make_async_copy(src, dst, sems.at[n]))
    for c in copies:
        c.start()
    for c in copies:
        c.wait()


HBM = pl.BlockSpec(memory_space=pltpu.HBM)
VM = pl.BlockSpec(memory_space=pltpu.VMEM)


def shape(*dims):
    return jax.ShapeDtypeStruct(dims, F32)


def swap(b, a):
    n = 128
    cross = [(d, (d + 1) % n if d % 2 else (d - 1) % n) for d in range(n)]
    chip = [(d, d ^ 1) for d in range(n)]
    return lax.ppermute(b, AXES, cross), lax.ppermute(a, AXES, chip)


def coriolis():
    b = 4 * np.arange(8)[None, :] + np.arange(4)[:, None]
    j = b.reshape(32, 1) * 128 + np.arange(128)[None, :]
    return (0.125 * np.sin(math.pi * ((j + 0.5) / 4096 - 0.5))).astype(np.float32)


def staging():
    return [
        pltpu.VMEM((11, *STAGE), F32),
        pltpu.VMEM((1, *STAGE), jnp.int32),
        pltpu.SemaphoreType.DMA((6,)),
    ]


def call(kernel, name, out, ins, specs, scratch, alias=None, outs=None, cost=None):
    return pl.pallas_call(
        kernel,
        out_shape=out,
        in_specs=specs,
        out_specs=outs or [VM] * len(out),
        scratch_shapes=scratch,
        input_output_aliases=alias or {},
        compiler_params=pltpu.CompilerParams(vmem_limit_bytes=20 << 20),
        cost_estimate=cost,
        name=name,
    )(*ins)


def on_device(forcing, ice_state, velocity, stress, ice_mask):
    raw = [
        pltpu.with_memory_space_constraint(view(x), pltpu.HBM)
        for x in (forcing, ice_state, velocity, stress, ice_mask[None])
    ]
    n1, n2 = (TOP + len(NEXT)) * R, (5 + len(NEXT)) * R + 24
    cor = pltpu.with_memory_space_constraint(jnp.asarray(coriolis()), pltpu.HBM)
    b, a, m, f4 = call(
        pack_kernel,
        "pack",
        [shape(n1, 128), shape(n1, 128), shape(24, 128), shape(R, 128)],
        [*raw, cor],
        [HBM] * 6,
        [pltpu.VMEM((5, NC * R, 128), F32), pltpu.VMEM((9, NC * R, 128), F32), *staging()],
    )
    rb, ra = swap(b, a)
    rm = lax.ppermute(m, AXES, [(d, 127 - d) for d in range(128)])
    cost = pl.CostEstimate(flops=20_000_000, bytes_accessed=4_000_000, transcendentals=500_000)
    main = [shape(5, NC * R, 128), shape(9, NC * R, 128), *[shape(6, NC * R, 128)] * 2]
    strips = shape(2 * TOP, R, 128)
    *state, strip = call(
        first_interior,
        "interior1",
        [*main, strips],
        [*raw, f4],
        [HBM] * 5 + [VM],
        staging(),
        cost=cost,
    )
    *state, strip, b, a = call(
        first_edges,
        "edges1",
        [*main, strips, shape(n2, 128), shape(n2, 128)],
        [rb, ra, rm, f4, *state, strip],
        [VM] * 9,
        [],
        alias={4 + k: k for k in range(5)},
    )
    rb, ra = swap(b, a)
    state = call(
        second_interior,
        "interior2",
        main,
        [f4, *state],
        [VM] * 5,
        [],
        alias={1 + k: k for k in range(4)},
        cost=cost,
    )
    vel, strs, ocean, *_ = call(
        second_edges,
        "edges2",
        [*[shape(n, 2, 8, 32, 128) for n in (2, 3, 2)], *main, strips],
        [rb, ra, f4, *state, strip],
        [VM] * 8,
        [
            pltpu.VMEM((28, R, 128), F32),
            pltpu.VMEM((7, *STAGE), F32),
            pltpu.SemaphoreType.DMA((3,)),
        ],
        alias={3 + k: 3 + k for k in range(5)},
        outs=[HBM] * 3 + [VM] * 5,
    )
    return unview(vel), unview(strs), unview(ocean)


def solution(mesh):
    slab = P(None, AXES, None)
    return jax.shard_map(
        on_device,
        mesh=mesh,
        in_specs=(slab, slab, slab, slab, P(AXES, None)),
        out_specs=(slab, slab, slab),
        check_vma=False,
    )
```

```python
import math

import jax
import jax.numpy as jnp
import numpy as np
from jax import lax
from jax.experimental import pallas as pl
from jax.experimental.pallas import tpu as pltpu
from jax.sharding import PartitionSpec as P


F32 = jnp.float32
AXES = ("gx", "gy")
C = 16
R = 32
H = 3
NC = C + 2 * H
FIELDS = ("uo", "vo", "tx", "ty", "a", "h", "u", "v", "s1", "s2", "s12", "mask")
WHERE = {n: k for k, n in enumerate(FIELDS)}
STATE = ("u", "v", "s1", "s2", "s12")
NEXT = ("u", "v", "z", "alpha", "beta")
U, V, S1, S2, S12 = range(5)
PR, MI, UO, CU, VO, CV, MK, OU, OV = range(9)
T, D2, W, DV2, E1, UP = range(6)
K29 = 29.0 / 30.0
STAGE = (2, 8 * 40, 128)
TOP = len(FIELDS)


def view(x):
    c = x.shape[0]
    return x.reshape(c, 2, 8, 8, 4, 128).transpose(0, 1, 3, 4, 2, 5).reshape(c, 2, 8, 32, 128)


def unview(y):
    c = y.shape[0]
    return y.reshape(c, 2, 8, 4, 8, 128).transpose(0, 1, 4, 2, 3, 5).reshape(c, C, 4096)


def iotas(shape):
    return lax.broadcasted_iota(jnp.int32, shape, 0), lax.broadcasted_iota(jnp.int32, shape, 1)


def root(x):
    return x * lax.rsqrt(jnp.maximum(x, 1e-30))


def below(x, masks):
    lane0, _, sub0, _ = masks
    r = pltpu.roll(x, 1, 1)
    q = jnp.where(sub0, 0.0, pltpu.roll(r[24:32], 1, 0))
    return jnp.where(lane0, jnp.concatenate([q, r[0:24]], 0), r)


def above(x, masks):
    _, lane127, _, _ = masks
    r = pltpu.roll(x, 127, 1)
    q = pltpu.roll(r[0:8], 7, 0)
    return jnp.where(lane127, jnp.concatenate([r[8:32], q], 0), r)


def make_masks():
    _, lane = iotas((R, 128))
    sub, _ = iotas((8, 128))
    return lane == 0, lane == 127, sub == 0, sub == 7


def rows(c):
    return pl.ds(pl.multiple_of((c + H) * R, R), R)


def each_column(span, body):
    if isinstance(span, tuple):
        lo, hi, chunk = span

        def step(t, carry):
            for q in range(chunk):
                body(lo + t * chunk + q)
            return carry

        lax.fori_loop(0, (hi - lo) // chunk, step, 0)
    else:
        for c in span:
            body(c)


def stress_terms(x1, e1, sc4, x, y, s, p):
    d = x1 + e1
    e = x1 - e1
    delta = root(d * d + 0.25 * (e * e) + (1.0 / 64.0) * (sc4 * sc4))
    r = p / (delta + 0.05)
    dk = x + y
    ek = x - y
    dk2 = root((1.0 / 16.0) * (dk * dk) + (1.0 / 64.0) * (ek * ek) + 0.25 * (s * s))
    rk = p / (dk2 + 0.05)
    return r * (d - delta), r * (0.25 * e), rk * (0.125 * s)


def momentum(w, o, c, mi, force, cor, ice, open_o):
    g = 0.5 * root((o - w) * (o - w) + 0.0025) * mi
    new = (30.0 * w + c + force * mi + g * o + cor) / (31.0 + g)
    return jnp.where(ice, new, open_o)


def subcycle(st, sc, tmp, f4, masks, vel, stress, mom):
    def shift(c):
        u, v = st[U, rows(c), :], st[V, rows(c), :]
        up, um = above(u, masks), below(u, masks)
        vp, vm = above(v, masks), below(v, masks)
        tmp[T, rows(c), :] = u + up
        tmp[D2, rows(c), :] = up - um
        tmp[UP, rows(c), :] = up - u
        tmp[W, rows(c), :] = v + vm
        tmp[E1, rows(c), :] = v - vm
        tmp[DV2, rows(c), :] = vp - vm

    each_column(vel, shift)

    def strain(c):
        ld = lambda k, d=0: tmp[k, rows(c + d), :]
        us = lambda d: st[U, rows(c + d), :]
        vs = lambda d: st[V, rows(c + d), :]
        a1, a2, a12 = stress_terms(
            us(0) - us(-1),
            ld(E1),
            (ld(D2) + ld(D2, -1)) + (ld(W, 1) - ld(W, -1)),
            ld(T, 1) - ld(T, -1),
            ld(DV2) + ld(DV2, 1),
            ld(UP) + (vs(1) - vs(0)),
            sc[PR, rows(c), :],
        )
        st[S1, rows(c), :] = K29 * st[S1, rows(c), :] + a1
        st[S2, rows(c), :] = K29 * st[S2, rows(c), :] + a2
        st[S12, rows(c), :] = K29 * st[S12, rows(c), :] + a12

    each_column(stress, strain)

    def move(c):
        ss = lambda k, d=0: st[k, rows(c + d), :]
        q1 = ss(S1) + ss(S2)
        q1n = ss(S1, 1) + ss(S2, 1)
        q2 = ss(S1) - ss(S2)
        s12 = ss(S12)
        fu = 0.5 * (q1n - q1) + (s12 - below(s12, masks))
        fv = 0.5 * (above(q2, masks) - q2) + (s12 - ss(S12, -1))
        cu = f4 * (tmp[W, rows(c), :] + tmp[W, rows(c + 1), :])
        cv = f4 * (tmp[T, rows(c), :] + tmp[T, rows(c - 1), :])
        k = lambda n: sc[n, rows(c), :]
        ice = k(MK) == 2.0
        mi = k(MI)
        st[U, rows(c), :] = momentum(ss(U), k(UO), k(CU), mi, fu, cu, ice, k(OU))
        st[V, rows(c), :] = momentum(ss(V), k(VO), k(CV), mi, fv, -cv, ice, k(OV))

    each_column(mom, move)


def interior(st, sc, tmp1, tmp2, f4):
    masks = make_masks()
    subcycle(st, sc, tmp1, f4, masks, (0, 16, 8), (1, 15, 7), (2, 14, 6))
    subcycle(st, sc, tmp2, f4, masks, (2, 14, 6), (3, 13, 5), (4, 12, 4))


def edges(st, sc, tmp1, tmp2, f4, left=None, right=None):
    masks = make_masks()

    def near(a, b, c, d):
        return [*(range(a, b) if left else ()), *(range(c, d) if right else ())]

    if left:
        st[U, rows(-2), :], st[V, rows(-2), :] = left["u"], left["v"]
        st[S12, rows(-2), :] = left["z"]
    if right:
        st[U, rows(17), :], st[V, rows(17), :] = right["u"], right["v"]
        st[S1, rows(17), :] = right["z"]
        st[S2, rows(17), :] = jnp.zeros((R, 128), F32)
    subcycle(
        st, sc, tmp1, f4, masks, near(-2, 0, 16, 18), near(-1, 1, 15, 17), near(-1, 2, 14, 17)
    )
    if left:
        n11 = 0.5 * (st[S1, rows(-1), :] + st[S2, rows(-1), :])
        st[U, rows(-2), :] = left["alpha"] + left["beta"] * n11
    if right:
        st[V, rows(17), :] = right["alpha"] - right["beta"] * st[S12, rows(16), :]
    subcycle(
        st, sc, tmp2, f4, masks, near(-2, 2, 14, 18), near(-1, 3, 13, 17), near(0, 4, 12, 16)
    )


def outgoing(st, sc, f4, side):
    masks = make_masks()

    def around(c):
        s = lambda k, d=0: st[k, rows(c + d), :]
        f = lambda k: sc[k, rows(c), :]
        t, d2, w, dv2 = [], [], [], []
        for d in (-1, 0, 1):
            u, v = s(U, d), s(V, d)
            up, um, vp, vm = above(u, masks), below(u, masks), above(v, masks), below(v, masks)
            t.append(u + up)
            d2.append(up - um)
            w.append(v + vm)
            dv2.append(vp - vm)
            if d == 0:
                e1, rise = v - vm, up - u
        a1, a2, a12 = stress_terms(
            s(U) - s(U, -1),
            e1,
            (d2[1] + d2[0]) + (w[2] - w[0]),
            t[2] - t[0],
            dv2[1] + dv2[2],
            rise + (s(V, 1) - s(V)),
            f(PR),
        )
        s1, s2, s12 = K29 * s(S1) + a1, K29 * s(S2) + a2, K29 * s(S12) + a12
        return s, f, t, w, s1 + s2, s1 - s2, s12

    def numbers(x, o, c, mi, force, cor, ice, open_o):
        g = 0.5 * root((o - x) * (o - x) + 0.0025) * mi
        b = 1.0 / (31.0 + g)
        a = (30.0 * x + c + force * mi + g * o + cor) * b
        return jnp.where(ice, a, open_o), jnp.where(ice, mi * b, 0.0)

    if side == 0:
        s, f, t, w, q1, q2, s12 = around(1)
        force = 0.5 * (above(q2, masks) - q2) + s12
        cor = -f4 * (t[1] + t[0])
        ice = f(MK) == 2.0
        return s(U), s(V), q1, *numbers(s(V), f(VO), f(CV), f(MI), force, cor, ice, f(OV))
    s, f, t, w, q1, q2, s12 = around(C - 2)
    force = (s12 - below(s12, masks)) - 0.5 * q1
    cor = f4 * (w[1] + w[2])
    ice = f(MK) == 2.0
    return s(U), s(V), s12, *numbers(s(U), f(UO), f(CU), f(MI), force, cor, ice, f(OU))


def put(out, xs, n=0):
    for x in xs:
        out[pl.ds(n * R, R), :] = x
        n += 1


def take(ref, names):
    return {name: ref[pl.ds(n * R, R), :] for n, name in enumerate(names)}


def receive(rb, ra, names, even):
    b, a = take(rb, names), take(ra, names)
    left = {n: jnp.where(even, b[n], a[n]) for n in names}
    right = {n: jnp.where(even, a[n], b[n]) for n in names}
    return left, right


def next_names(x):
    return {n: x[n + "1"] for n in NEXT}


FIRST = (*FIELDS, *[n + "1" for n in NEXT])
SECOND = (*STATE, *[n + "1" for n in NEXT])


def statics(raw):
    a, h, mask = raw["a"], raw["h"], raw["mask"]
    ice = mask == 2.0
    opened = mask == 1.0
    mi = 1.0 / (a * h)
    out = {
        PR: jnp.where(ice, h * jnp.exp(-20.0 * (1.0 - a)) * (1.0 / 30.0), 0.0),
        MI: mi,
        UO: raw["uo"],
        CU: raw["u"] + raw["tx"] * mi,
        VO: raw["vo"],
        CV: raw["v"] + raw["ty"] * mi,
        MK: mask,
        OU: jnp.where(opened, raw["uo"], 0.0),
        OV: jnp.where(opened, raw["vo"], 0.0),
    }
    return out, ice


def put_column(st, sc, at, raw):
    out, ice = statics(raw)
    for k, x in out.items():
        sc[k, at, :] = x
    st[U, at, :] = raw["u"]
    st[V, at, :] = raw["v"]
    st[S1, at, :] = jnp.where(ice, raw["s1"], 0.0)
    st[S2, at, :] = jnp.where(ice, raw["s2"], 0.0)
    st[S12, at, :] = jnp.where(ice, raw["s12"], 0.0)


def stage_in(srcs, stage, mstage, sems):
    copies = []
    at = 0
    for k, src in enumerate(srcs):
        n = src.shape[0]
        if k < 4:
            dst = stage.reshape(11, 2, 8, 40, 128).at[pl.ds(at, n), :, :, pl.ds(0, 32), :]
        else:
            dst = mstage.reshape(1, 2, 8, 40, 128).at[:, :, :, pl.ds(0, 32), :]
        copies.append(pltpu.make_async_copy(src, dst, sems.at[k]))
        at += n
    for c in copies:
        c.start()
    for c in copies:
        c.wait()


def staged_column(stage, mstage, name, c):
    ref, f = (mstage, 0) if name == "mask" else (stage, WHERE[name])
    parts = [ref[f, c // 8, pl.ds(8 * k + c % 8, 8, stride=40), :] for k in range(4)]
    return jnp.concatenate(parts, 0).astype(F32)


def parity():
    return lax.rem(lax.axis_index("gy"), 2)


def squeeze(tiles):
    _, lane = iotas((8, 128))
    out = []
    for t in range(0, len(tiles), 8):
        x = tiles[t + 7]
        for g in range(7):
            x = jnp.where(lane // 16 == g, pltpu.roll(tiles[t + g], 16 * (g + 1), 1), x)
        out.append(x)
    return out


def spread(packed, n):
    x = packed[n // 8]
    g = n % 8
    return x if g == 7 else pltpu.roll(x, 128 - 16 * (g + 1), 1)


def top_tile(stage, mstage, k, ih):
    ref, f = (mstage, 0) if k == TOP - 1 else (stage, k)
    return ref[f, ih, pl.ds(7 * 40 + 24, 8), :].astype(F32)


def by_side(cross, body):
    even = parity() == 0
    here = even if cross else jnp.logical_not(even)

    @pl.when(here)
    def _():
        body(0)

    @pl.when(jnp.logical_not(here))
    def _():
        body(1)


def pack_side(out, f4, st, sc, stage, mstage, side, half):
    def column(name, m):
        ref, f = (mstage, 0) if name == "mask" else (stage, WHERE[name])
        il = 7 - m if side else m
        parts = [ref[f, half, pl.ds(8 * k + il, 8, stride=40), :] for k in range(4)]
        return jnp.concatenate(parts, 0).astype(F32)

    at = lambda m: rows(C - 1 - m if side else m)
    put_column(st, sc, at(1), {name: column(name, 1) for name in FIELDS})
    for m in (0, 2):
        st[U, at(m), :], st[V, at(m), :] = column("u", m), column("v", m)
    put(out, [column(name, 0) for name in FIELDS])
    put(out, outgoing(st, sc, f4[...], side), TOP)


def pack_cross(
    f_ref, i_ref, v_ref, s_ref, m_ref, cor, b_out, m_out, f4, st, sc, stage, mstage, top, mtop, sems
):
    srcs = (f_ref, i_ref, v_ref, s_ref, m_ref)

    def body(side):
        main = [pltpu.make_async_copy(cor, f4, sems.at[5])]
        tops = []
        at = 0
        for k, src in enumerate(srcs):
            n = src.shape[0]
            if k < 4:
                dst = stage.reshape(11, 1, 8, 40, 128).at[pl.ds(at, n), 0, :, pl.ds(0, 32), :]
            else:
                dst = mstage.reshape(1, 1, 8, 40, 128).at[:, 0, :, pl.ds(0, 32), :]
            main.append(pltpu.make_async_copy(src.at[:, side], dst, sems.at[k]))
            dst = top.at[pl.ds(at, n)] if k < 4 else mtop
            tile = src.at[:, :, 7, pl.ds(24, 8), :]
            tops.append(pltpu.make_async_copy(tile, dst, sems.at[6 + k]))
            at += n
        for c in main + tops:
            c.start()
        for c in main:
            c.wait()
        pack_side(b_out, f4, st, sc, stage, mstage, side, 0)
        for c in tops:
            c.wait()
        tiles = [
            mtop[0, ih].astype(F32) if k == TOP - 1 else top[k, ih]
            for k in range(TOP)
            for ih in range(2)
        ]
        for n, x in enumerate(squeeze(tiles)):
            m_out[pl.ds(8 * n, 8), :] = x

    by_side(True, body)


def pack_chip(f_ref, i_ref, v_ref, s_ref, m_ref, f4, a_out, stage, mstage, st, sc, sems):
    stage_in((f_ref, i_ref, v_ref, s_ref, m_ref), stage, mstage, sems)
    by_side(False, lambda side: pack_side(a_out, f4, st, sc, stage, mstage, side, side))


def first_interior(stage, mstage, f4, st, sc, tmp1, tmp2, strip):
    for c in range(C):
        put_column(
            st, sc, rows(c), {name: staged_column(stage, mstage, name, c) for name in FIELDS}
        )
    for k in range(TOP):
        for ih in range(2):
            strip[k, pl.ds(8 + 8 * ih, 8), :] = top_tile(stage, mstage, k, ih)
    interior(st, sc, tmp1, tmp2, f4[...])


def edge_side(r, out, st, sc, tmp1, tmp2, strip, f4, cross):
    def body(side):
        got = take(r, FIRST)
        put_column(st, sc, rows(C if side else -1), got)
        edges(st, sc, tmp1, tmp2, f4[...], **{("left", "right")[side]: next_names(got)})
        put(out, [st[k, rows(C - 1 if side else 0), :] for k in range(5)])
        put(out, outgoing(st, sc, f4[...], side), 5)
        tiles = squeeze([strip[k, pl.ds(16 if side else 8, 8), :] for k in range(2 * TOP)])
        for n, x in enumerate(tiles):
            out[pl.ds(len(SECOND) * R + 8 * n, 8), :] = x

    by_side(cross, body)


def cross_edges(*refs):
    rb, rm, f4 = refs[:3]
    st, sc, tmp1, tmp2, strip, out = refs[8:]
    flip = 7 - iotas((8, 128))[0]
    packed = [rm[pl.ds(8 * n, 8), :] for n in range(3)]
    for k in range(TOP):
        for ih in range(2):
            x = spread(packed, 2 * k + ih)
            strip[TOP + k, pl.ds(16 - 8 * ih, 8), :] = jnp.take_along_axis(x, flip, axis=0)
    edge_side(rb, out, st, sc, tmp1, tmp2, strip, f4, True)


def chip_edges(*refs):
    ra, f4 = refs[:2]
    st, sc, tmp1, tmp2, strip, out = refs[7:]
    edge_side(ra, out, st, sc, tmp1, tmp2, strip, f4, False)


def second_interior(*refs):
    f4, (st, sc, tmp1, tmp2) = refs[0], refs[5:]
    interior(st, sc, tmp1, tmp2, f4[...])


def run_strips(strip, work, cor4):
    _, lane = iotas((R, 128))
    last = lane == 127
    f4 = jnp.broadcast_to(cor4[pl.ds(31, 1), :], (R, 128))
    for side in range(2):
        raw = {name: strip[side * TOP + k] for k, name in enumerate(FIELDS)}
        out, ice = statics(raw)
        work[5 * side + U] = raw["u"]
        work[5 * side + V] = raw["v"]
        for k, name in ((S1, "s1"), (S2, "s2"), (S12, "s12")):
            work[5 * side + k] = jnp.where(ice, raw[name], 0.0)
        for k in range(9):
            work[10 + 9 * side + k] = out[k]

    def step():
        x = [[work[5 * side + k] for k in range(5)] for side in range(2)]
        east = [lambda y: pltpu.roll(y, R - 1, 0), lambda y: pltpu.roll(y, 1, 0)]
        west = [east[1], east[0]]
        down = lambda y: pltpu.roll(y, 1, 1)
        up = lambda y, other, sign: jnp.where(last, sign * other, pltpu.roll(y, 127, 1))
        terms = []
        for side in range(2):
            e, w = east[side], west[side]
            u, v = x[side][U], x[side][V]
            ou, ov = x[1 - side][U], x[1 - side][V]
            upu, um, vp, vm = up(u, ou, -1.0), down(u), up(v, ov, -1.0), down(v)
            tt, d2, ww, dv2 = u + upu, upu - um, v + vm, vp - vm
            terms.append((tt, ww))
            k = lambda n: work[10 + 9 * side + n]
            a1, a2, a12 = stress_terms(
                u - w(u),
                v - vm,
                (d2 + w(d2)) + (e(ww) - w(ww)),
                e(tt) - w(tt),
                dv2 + e(dv2),
                (upu - u) + (e(v) - v),
                k(PR),
            )
            x[side][S1] = K29 * x[side][S1] + a1
            x[side][S2] = K29 * x[side][S2] + a2
            x[side][S12] = K29 * x[side][S12] + a12
        new = []
        for side in range(2):
            e, w = east[side], west[side]
            u, v, s1, s2, s12 = x[side]
            q1, q2 = s1 + s2, s1 - s2
            other = x[1 - side][S1] - x[1 - side][S2]
            fu = 0.5 * (e(q1) - q1) + (s12 - down(s12))
            fv = 0.5 * (up(q2, other, 1.0) - q2) + (s12 - w(s12))
            tt, ww = terms[side]
            k = lambda n: work[10 + 9 * side + n]
            ice = k(MK) == 2.0
            nu = momentum(u, k(UO), k(CU), k(MI), fu, f4 * (ww + e(ww)), ice, k(OU))
            nv = momentum(v, k(VO), k(CV), k(MI), fv, -f4 * (tt + w(tt)), ice, k(OV))
            new.append((nu, nv, s1, s2, s12))
        for side in range(2):
            for k in range(5):
                work[5 * side + k] = new[side][k]

    return step


def second_edges(*refs):
    rb, ra, f4 = refs[:3]
    vel_o, str_o, oce_o, st, sc, tmp1, tmp2, strip, work, stage, sems = refs[8:]
    even = parity() == 0
    left, right = receive(rb, ra, SECOND, even)
    for k, name in enumerate(STATE):
        st[k, rows(-1), :], st[k, rows(C), :] = left[name], right[name]
    base = len(SECOND) * R
    pb = [rb[pl.ds(base + 8 * n, 8), :] for n in range(3)]
    pa = [ra[pl.ds(base + 8 * n, 8), :] for n in range(3)]
    low = [jnp.where(even, b, a) for b, a in zip(pb, pa)]
    high = [jnp.where(even, a, b) for b, a in zip(pb, pa)]
    for k in range(2 * TOP):
        strip[k, pl.ds(0, 8), :] = spread(low, k)
        strip[k, pl.ds(24, 8), :] = spread(high, k)
    step = run_strips(strip, work, f4)
    for _ in range(4):
        step()
    edges(st, sc, tmp1, tmp2, f4[...], next_names(left), next_names(right))
    row, lane = iotas((R, 128))
    top = (row == R - 1) & (lane >= 120)

    whole = stage.reshape(7, 2, 8, 40, 128)
    copies = []
    for ih in range(2):
        for c in range(8 * ih, 8 * ih + 8):
            x = [
                jnp.where(top, work[k, pl.ds(8 + c, 1), :], st[k, rows(c), :]) for k in range(5)
            ]
            for w, o in ((U, UO), (V, VO)):
                d = x[w] - sc[o, rows(c), :]
                x.append(0.5 * root(d * d + 0.0025) * d)
            for f, y in enumerate(x):
                for k in range(4):
                    stage[f, ih, pl.ds(8 * k + c % 8, 8, stride=40), :] = y[8 * k : 8 * k + 8]
        for n, (dst, at) in enumerate(((vel_o, 0), (str_o, 2), (oce_o, 5))):
            src = whole.at[pl.ds(at, dst.shape[0]), ih, :, pl.ds(0, 32), :]
            copies.append(pltpu.make_async_copy(src, dst.at[:, ih], sems.at[3 * ih + n]))
            copies[-1].start()
    for c in copies:
        c.wait()


HBM = pl.BlockSpec(memory_space=pltpu.HBM)
VM = pl.BlockSpec(memory_space=pltpu.VMEM)


def shape(*dims):
    return jax.ShapeDtypeStruct(dims, F32)


def permuted(x, pairs):
    return lax.ppermute(x, AXES, pairs)


N = 128
CROSS = [(d, (d + 1) % N if d % 2 else (d - 1) % N) for d in range(N)]
CHIP = [(d, d ^ 1) for d in range(N)]
MIRROR = [(d, N - 1 - d) for d in range(N)]


def coriolis():
    b = 4 * np.arange(8)[None, :] + np.arange(4)[:, None]
    j = b.reshape(32, 1) * 128 + np.arange(128)[None, :]
    return (0.125 * np.sin(math.pi * ((j + 0.5) / 4096 - 0.5))).astype(np.float32)


def edge_scratch():
    return [pltpu.VMEM((5, NC * R, 128), F32), pltpu.VMEM((9, NC * R, 128), F32)]


def call(kernel, out, ins, specs, scratch, alias=None, outs=None, cost=None):
    return pl.pallas_call(
        kernel,
        out_shape=out,
        in_specs=specs,
        out_specs=outs or [VM] * len(out),
        scratch_shapes=scratch,
        input_output_aliases=alias or {},
        compiler_params=pltpu.CompilerParams(vmem_limit_bytes=20 << 20),
        cost_estimate=cost,
    )(*ins)


def on_device(forcing, ice_state, velocity, stress, ice_mask):
    raw = [
        pltpu.with_memory_space_constraint(view(x), pltpu.HBM)
        for x in (forcing, ice_state, velocity, stress, ice_mask[None])
    ]
    vel, strs, ocean = window(raw)
    return unview(vel), unview(strs), unview(ocean)


def window(raw):
    n1, n2 = len(FIRST) * R, len(SECOND) * R + 24
    cor = pltpu.with_memory_space_constraint(jnp.asarray(coriolis()), pltpu.HBM)
    cost = pl.CostEstimate(flops=20_000_000, bytes_accessed=4_000_000, transcendentals=500_000)
    b, m, f4 = call(
        pack_cross,
        [shape(n1, 128), shape(24, 128), shape(R, 128)],
        [*raw, cor],
        [HBM] * 6,
        [
            *edge_scratch(),
            pltpu.VMEM((11, 1, *STAGE[1:]), F32),
            pltpu.VMEM((1, 1, *STAGE[1:]), jnp.int32),
            pltpu.VMEM((11, 2, 8, 128), F32),
            pltpu.VMEM((1, 2, 8, 128), jnp.int32),
            pltpu.SemaphoreType.DMA((11,)),
        ],
    )
    rb = permuted(b, CROSS)
    rm = permuted(m, MIRROR)
    a, stage, mstage = call(
        pack_chip,
        [
            shape(n1, 128),
            shape(11, *STAGE),
            jax.ShapeDtypeStruct((1, *STAGE), jnp.int32),
        ],
        [*raw, f4],
        [HBM] * 5 + [VM],
        [*edge_scratch(), pltpu.SemaphoreType.DMA((5,))],
        cost=cost,
    )
    ra = permuted(a, CHIP)
    main = [shape(5, NC * R, 128), shape(9, NC * R, 128), *[shape(6, NC * R, 128)] * 2]
    strips = shape(2 * TOP, R, 128)
    *state, strip = call(
        first_interior, [*main, strips], [stage, mstage, f4], [VM] * 3, [], cost=cost
    )
    *state, strip, b = call(
        cross_edges,
        [*main, strips, shape(n2, 128)],
        [rb, rm, f4, *state, strip],
        [VM] * 8,
        [],
        alias={3 + k: k for k in range(5)},
    )
    rb = permuted(b, CROSS)
    *state, strip, a = call(
        chip_edges,
        [*main, strips, shape(n2, 128)],
        [ra, f4, *state, strip],
        [VM] * 7,
        [],
        alias={2 + k: k for k in range(5)},
        cost=cost,
    )
    ra = permuted(a, CHIP)
    state = call(
        second_interior,
        main,
        [f4, *state],
        [VM] * 5,
        [],
        alias={1 + k: k for k in range(4)},
        cost=cost,
    )
    vel, strs, ocean, *_ = call(
        second_edges,
        [*[shape(n, 2, 8, 32, 128) for n in (2, 3, 2)], *main, strips],
        [rb, ra, f4, *state, strip],
        [VM] * 8,
        [
            pltpu.VMEM((28, R, 128), F32),
            pltpu.VMEM((7, *STAGE), F32),
            pltpu.SemaphoreType.DMA((6,)),
        ],
        alias={3 + k: 3 + k for k in range(5)},
        outs=[HBM] * 3 + [VM] * 5,
    )
    return vel, strs, ocean


def solution(mesh):
    slab = P(None, AXES, None)
    return jax.shard_map(
        on_device,
        mesh=mesh,
        in_specs=(slab, slab, slab, slab, P(AXES, None)),
        out_specs=(slab, slab, slab),
        check_vma=False,
    )
```

```python
import math

import jax
import jax.numpy as jnp
import numpy as np
from jax import lax
from jax.experimental import pallas as pl
from jax.experimental.pallas import tpu as pltpu
from jax.sharding import PartitionSpec as P


F32 = jnp.float32
AXES = ("gx", "gy")
C = 16
R = 32
H = 3
NC = C + 2 * H
FIELDS = ("uo", "vo", "tx", "ty", "a", "h", "u", "v", "s1", "s2", "s12", "mask")
WHERE = {n: k for k, n in enumerate(FIELDS)}
STATE = ("u", "v", "s1", "s2", "s12")
NEXT = ("u", "v", "z", "alpha", "beta")
U, V, S1, S2, S12 = range(5)
PR, MI, UO, CU, VO, CV, MK, OU, OV = range(9)
T, D2, W, DV2, E1, UP = range(6)
K29 = 29.0 / 30.0
STAGE = (2, 8 * 40, 128)
TOP = len(FIELDS)


def view(x):
    c = x.shape[0]
    return x.reshape(c, 2, 8, 8, 4, 128).transpose(0, 1, 3, 4, 2, 5).reshape(c, 2, 8, 32, 128)


def unview(y):
    c = y.shape[0]
    return y.reshape(c, 2, 8, 4, 8, 128).transpose(0, 1, 4, 2, 3, 5).reshape(c, C, 4096)


def iotas(shape):
    return lax.broadcasted_iota(jnp.int32, shape, 0), lax.broadcasted_iota(jnp.int32, shape, 1)


def root(x):
    return x * lax.rsqrt(jnp.maximum(x, 1e-30))


def below(x, masks):
    lane0, _, sub0, _ = masks
    r = pltpu.roll(x, 1, 1)
    q = jnp.where(sub0, 0.0, pltpu.roll(r[24:32], 1, 0))
    return jnp.where(lane0, jnp.concatenate([q, r[0:24]], 0), r)


def above(x, masks):
    _, lane127, _, _ = masks
    r = pltpu.roll(x, 127, 1)
    q = pltpu.roll(r[0:8], 7, 0)
    return jnp.where(lane127, jnp.concatenate([r[8:32], q], 0), r)


def make_masks():
    _, lane = iotas((R, 128))
    sub, _ = iotas((8, 128))
    return lane == 0, lane == 127, sub == 0, sub == 7


def rows(c):
    return pl.ds(pl.multiple_of((c + H) * R, R), R)


def each_column(span, body):
    if isinstance(span, tuple):
        lo, hi, chunk = span

        def step(t, carry):
            for q in range(chunk):
                body(lo + t * chunk + q)
            return carry

        lax.fori_loop(0, (hi - lo) // chunk, step, 0)
    else:
        for c in span:
            body(c)


def stress_terms(x1, e1, sc4, x, y, s, p):
    d = x1 + e1
    e = x1 - e1
    delta = root(d * d + 0.25 * (e * e) + (1.0 / 64.0) * (sc4 * sc4))
    r = p / (delta + 0.05)
    dk = x + y
    ek = x - y
    dk2 = root((1.0 / 16.0) * (dk * dk) + (1.0 / 64.0) * (ek * ek) + 0.25 * (s * s))
    rk = p / (dk2 + 0.05)
    return r * (d - delta), r * (0.25 * e), rk * (0.125 * s)


def momentum(w, o, c, mi, force, cor, ice, open_o):
    g = 0.5 * root((o - w) * (o - w) + 0.0025) * mi
    new = (30.0 * w + c + force * mi + g * o + cor) / (31.0 + g)
    return jnp.where(ice, new, open_o)


def subcycle(st, sc, tmp, f4, masks, vel, stress, mom):
    def shift(c):
        u, v = st[U, rows(c), :], st[V, rows(c), :]
        up, um = above(u, masks), below(u, masks)
        vp, vm = above(v, masks), below(v, masks)
        tmp[T, rows(c), :] = u + up
        tmp[D2, rows(c), :] = up - um
        tmp[UP, rows(c), :] = up - u
        tmp[W, rows(c), :] = v + vm
        tmp[E1, rows(c), :] = v - vm
        tmp[DV2, rows(c), :] = vp - vm

    each_column(vel, shift)

    def strain(c):
        ld = lambda k, d=0: tmp[k, rows(c + d), :]
        us = lambda d: st[U, rows(c + d), :]
        vs = lambda d: st[V, rows(c + d), :]
        a1, a2, a12 = stress_terms(
            us(0) - us(-1),
            ld(E1),
            (ld(D2) + ld(D2, -1)) + (ld(W, 1) - ld(W, -1)),
            ld(T, 1) - ld(T, -1),
            ld(DV2) + ld(DV2, 1),
            ld(UP) + (vs(1) - vs(0)),
            sc[PR, rows(c), :],
        )
        st[S1, rows(c), :] = K29 * st[S1, rows(c), :] + a1
        st[S2, rows(c), :] = K29 * st[S2, rows(c), :] + a2
        st[S12, rows(c), :] = K29 * st[S12, rows(c), :] + a12

    each_column(stress, strain)

    def move(c):
        ss = lambda k, d=0: st[k, rows(c + d), :]
        q1 = ss(S1) + ss(S2)
        q1n = ss(S1, 1) + ss(S2, 1)
        q2 = ss(S1) - ss(S2)
        s12 = ss(S12)
        fu = 0.5 * (q1n - q1) + (s12 - below(s12, masks))
        fv = 0.5 * (above(q2, masks) - q2) + (s12 - ss(S12, -1))
        cu = f4 * (tmp[W, rows(c), :] + tmp[W, rows(c + 1), :])
        cv = f4 * (tmp[T, rows(c), :] + tmp[T, rows(c - 1), :])
        k = lambda n: sc[n, rows(c), :]
        ice = k(MK) == 2.0
        mi = k(MI)
        st[U, rows(c), :] = momentum(ss(U), k(UO), k(CU), mi, fu, cu, ice, k(OU))
        st[V, rows(c), :] = momentum(ss(V), k(VO), k(CV), mi, fv, -cv, ice, k(OV))

    each_column(mom, move)


def interior(st, sc, tmp1, tmp2, f4):
    masks = make_masks()
    subcycle(st, sc, tmp1, f4, masks, (0, 16, 8), (1, 15, 7), (2, 14, 6))
    subcycle(st, sc, tmp2, f4, masks, (2, 14, 6), (3, 13, 5), (4, 12, 4))


def edges(st, sc, tmp1, tmp2, f4, left=None, right=None):
    masks = make_masks()

    def near(a, b, c, d):
        return [*(range(a, b) if left else ()), *(range(c, d) if right else ())]

    if left:
        st[U, rows(-2), :], st[V, rows(-2), :] = left["u"], left["v"]
        st[S12, rows(-2), :] = left["z"]
    if right:
        st[U, rows(17), :], st[V, rows(17), :] = right["u"], right["v"]
        st[S1, rows(17), :] = right["z"]
        st[S2, rows(17), :] = jnp.zeros((R, 128), F32)
    subcycle(
        st, sc, tmp1, f4, masks, near(-2, 0, 16, 18), near(-1, 1, 15, 17), near(-1, 2, 14, 17)
    )
    if left:
        n11 = 0.5 * (st[S1, rows(-1), :] + st[S2, rows(-1), :])
        st[U, rows(-2), :] = left["alpha"] + left["beta"] * n11
    if right:
        st[V, rows(17), :] = right["alpha"] - right["beta"] * st[S12, rows(16), :]
    subcycle(
        st, sc, tmp2, f4, masks, near(-2, 2, 14, 18), near(-1, 3, 13, 17), near(0, 4, 12, 16)
    )


def outgoing(st, sc, f4, side):
    masks = make_masks()

    def around(c):
        s = lambda k, d=0: st[k, rows(c + d), :]
        f = lambda k: sc[k, rows(c), :]
        t, d2, w, dv2 = [], [], [], []
        for d in (-1, 0, 1):
            u, v = s(U, d), s(V, d)
            up, um, vp, vm = above(u, masks), below(u, masks), above(v, masks), below(v, masks)
            t.append(u + up)
            d2.append(up - um)
            w.append(v + vm)
            dv2.append(vp - vm)
            if d == 0:
                e1, rise = v - vm, up - u
        a1, a2, a12 = stress_terms(
            s(U) - s(U, -1),
            e1,
            (d2[1] + d2[0]) + (w[2] - w[0]),
            t[2] - t[0],
            dv2[1] + dv2[2],
            rise + (s(V, 1) - s(V)),
            f(PR),
        )
        s1, s2, s12 = K29 * s(S1) + a1, K29 * s(S2) + a2, K29 * s(S12) + a12
        return s, f, t, w, s1 + s2, s1 - s2, s12

    def numbers(x, o, c, mi, force, cor, ice, open_o):
        g = 0.5 * root((o - x) * (o - x) + 0.0025) * mi
        b = 1.0 / (31.0 + g)
        a = (30.0 * x + c + force * mi + g * o + cor) * b
        return jnp.where(ice, a, open_o), jnp.where(ice, mi * b, 0.0)

    if side == 0:
        s, f, t, w, q1, q2, s12 = around(1)
        force = 0.5 * (above(q2, masks) - q2) + s12
        cor = -f4 * (t[1] + t[0])
        ice = f(MK) == 2.0
        return s(U), s(V), q1, *numbers(s(V), f(VO), f(CV), f(MI), force, cor, ice, f(OV))
    s, f, t, w, q1, q2, s12 = around(C - 2)
    force = (s12 - below(s12, masks)) - 0.5 * q1
    cor = f4 * (w[1] + w[2])
    ice = f(MK) == 2.0
    return s(U), s(V), s12, *numbers(s(U), f(UO), f(CU), f(MI), force, cor, ice, f(OU))


def put(out, xs, n=0):
    for x in xs:
        out[pl.ds(n * R, R), :] = x
        n += 1


def take(ref, names):
    return {name: ref[pl.ds(n * R, R), :] for n, name in enumerate(names)}


def receive(rb, ra, names, even):
    b, a = take(rb, names), take(ra, names)
    left = {n: jnp.where(even, b[n], a[n]) for n in names}
    right = {n: jnp.where(even, a[n], b[n]) for n in names}
    return left, right


def next_names(x):
    return {n: x[n + "1"] for n in NEXT}


FIRST = (*FIELDS, *[n + "1" for n in NEXT])
SECOND = (*STATE, *[n + "1" for n in NEXT])


def statics(raw):
    a, h, mask = raw["a"], raw["h"], raw["mask"]
    ice = mask == 2.0
    opened = mask == 1.0
    mi = 1.0 / (a * h)
    out = {
        PR: jnp.where(ice, h * jnp.exp(-20.0 * (1.0 - a)) * (1.0 / 30.0), 0.0),
        MI: mi,
        UO: raw["uo"],
        CU: raw["u"] + raw["tx"] * mi,
        VO: raw["vo"],
        CV: raw["v"] + raw["ty"] * mi,
        MK: mask,
        OU: jnp.where(opened, raw["uo"], 0.0),
        OV: jnp.where(opened, raw["vo"], 0.0),
    }
    return out, ice


def put_column(st, sc, at, raw):
    out, ice = statics(raw)
    for k, x in out.items():
        sc[k, at, :] = x
    st[U, at, :] = raw["u"]
    st[V, at, :] = raw["v"]
    st[S1, at, :] = jnp.where(ice, raw["s1"], 0.0)
    st[S2, at, :] = jnp.where(ice, raw["s2"], 0.0)
    st[S12, at, :] = jnp.where(ice, raw["s12"], 0.0)


def stage_in(srcs, stage, mstage, sems):
    copies = []
    at = 0
    for k, src in enumerate(srcs):
        n = src.shape[0]
        if k < 4:
            dst = stage.reshape(11, 2, 8, 40, 128).at[pl.ds(at, n), :, :, pl.ds(0, 32), :]
        else:
            dst = mstage.reshape(1, 2, 8, 40, 128).at[:, :, :, pl.ds(0, 32), :]
        copies.append(pltpu.make_async_copy(src, dst, sems.at[k]))
        at += n
    for c in copies:
        c.start()
    for c in copies:
        c.wait()


def staged_column(stage, mstage, name, c):
    ref, f = (mstage, 0) if name == "mask" else (stage, WHERE[name])
    parts = [ref[f, c // 8, pl.ds(8 * k + c % 8, 8, stride=40), :] for k in range(4)]
    return jnp.concatenate(parts, 0).astype(F32)


def parity():
    return lax.rem(lax.axis_index("gy"), 2)


def squeeze(tiles):
    _, lane = iotas((8, 128))
    out = []
    for t in range(0, len(tiles), 8):
        x = tiles[t + 7]
        for g in range(7):
            x = jnp.where(lane // 16 == g, pltpu.roll(tiles[t + g], 16 * (g + 1), 1), x)
        out.append(x)
    return out


def spread(packed, n):
    x = packed[n // 8]
    g = n % 8
    return x if g == 7 else pltpu.roll(x, 128 - 16 * (g + 1), 1)


def top_tile(stage, mstage, k, ih):
    ref, f = (mstage, 0) if k == TOP - 1 else (stage, k)
    return ref[f, ih, pl.ds(7 * 40 + 24, 8), :].astype(F32)


def by_side(cross, body):
    even = parity() == 0
    here = even if cross else jnp.logical_not(even)

    @pl.when(here)
    def _():
        body(0)

    @pl.when(jnp.logical_not(here))
    def _():
        body(1)


def pack_side(out, f4, st, sc, stage, mstage, side, half):
    def column(name, m):
        ref, f = (mstage, 0) if name == "mask" else (stage, WHERE[name])
        il = 7 - m if side else m
        parts = [ref[f, half, pl.ds(8 * k + il, 8, stride=40), :] for k in range(4)]
        return jnp.concatenate(parts, 0).astype(F32)

    at = lambda m: rows(C - 1 - m if side else m)
    put_column(st, sc, at(1), {name: column(name, 1) for name in FIELDS})
    for m in (0, 2):
        st[U, at(m), :], st[V, at(m), :] = column("u", m), column("v", m)
    put(out, [column(name, 0) for name in FIELDS])
    put(out, outgoing(st, sc, f4[...], side), TOP)


def pack_cross(
    f_ref, i_ref, v_ref, s_ref, m_ref, cor, b_out, m_out, f4, st, sc, stage, mstage, top, mtop, sems
):
    srcs = (f_ref, i_ref, v_ref, s_ref, m_ref)

    def body(side):
        main = [pltpu.make_async_copy(cor, f4, sems.at[5])]
        tops = []
        at = 0
        for k, src in enumerate(srcs):
            n = src.shape[0]
            if k < 4:
                dst = stage.reshape(11, 1, 8, 40, 128).at[pl.ds(at, n), 0, :, pl.ds(0, 32), :]
            else:
                dst = mstage.reshape(1, 1, 8, 40, 128).at[:, 0, :, pl.ds(0, 32), :]
            main.append(pltpu.make_async_copy(src.at[:, side], dst, sems.at[k]))
            dst = top.at[pl.ds(at, n)] if k < 4 else mtop
            tile = src.at[:, :, 7, pl.ds(24, 8), :]
            tops.append(pltpu.make_async_copy(tile, dst, sems.at[6 + k]))
            at += n
        for c in main + tops:
            c.start()
        for c in main:
            c.wait()
        pack_side(b_out, f4, st, sc, stage, mstage, side, 0)
        for c in tops:
            c.wait()
        tiles = [
            mtop[0, ih].astype(F32) if k == TOP - 1 else top[k, ih]
            for k in range(TOP)
            for ih in range(2)
        ]
        for n, x in enumerate(squeeze(tiles)):
            m_out[pl.ds(8 * n, 8), :] = x

    by_side(True, body)


def pack_chip(f_ref, i_ref, v_ref, s_ref, m_ref, f4, a_out, stage, mstage, st, sc, sems):
    stage_in((f_ref, i_ref, v_ref, s_ref, m_ref), stage, mstage, sems)
    by_side(False, lambda side: pack_side(a_out, f4, st, sc, stage, mstage, side, side))


def first_interior(stage, mstage, f4, st, sc, tmp1, tmp2, strip):
    for c in range(C):
        put_column(
            st, sc, rows(c), {name: staged_column(stage, mstage, name, c) for name in FIELDS}
        )
    for k in range(TOP):
        for ih in range(2):
            strip[k, pl.ds(8 + 8 * ih, 8), :] = top_tile(stage, mstage, k, ih)
    interior(st, sc, tmp1, tmp2, f4[...])


def edge_side(r, out, st, sc, tmp1, tmp2, strip, f4, cross):
    def body(side):
        got = take(r, FIRST)
        put_column(st, sc, rows(C if side else -1), got)
        edges(st, sc, tmp1, tmp2, f4[...], **{("left", "right")[side]: next_names(got)})
        put(out, [st[k, rows(C - 1 if side else 0), :] for k in range(5)])
        put(out, outgoing(st, sc, f4[...], side), 5)
        tiles = squeeze([strip[k, pl.ds(16 if side else 8, 8), :] for k in range(2 * TOP)])
        for n, x in enumerate(tiles):
            out[pl.ds(len(SECOND) * R + 8 * n, 8), :] = x

    by_side(cross, body)


def cross_edges(*refs):
    rb, rm, f4 = refs[:3]
    st, sc, tmp1, tmp2, strip, out = refs[8:]
    flip = 7 - iotas((8, 128))[0]
    packed = [rm[pl.ds(8 * n, 8), :] for n in range(3)]
    for k in range(TOP):
        for ih in range(2):
            x = spread(packed, 2 * k + ih)
            strip[TOP + k, pl.ds(16 - 8 * ih, 8), :] = jnp.take_along_axis(x, flip, axis=0)
    edge_side(rb, out, st, sc, tmp1, tmp2, strip, f4, True)


def chip_edges(*refs):
    ra, f4 = refs[:2]
    st, sc, tmp1, tmp2, strip, out = refs[7:]
    edge_side(ra, out, st, sc, tmp1, tmp2, strip, f4, False)


def stage_out(st, sc, out, cols):
    for c in cols:
        x = [st[k, rows(c), :] for k in range(5)]
        for w, o in ((U, UO), (V, VO)):
            d = x[w] - sc[o, rows(c), :]
            x.append(0.5 * root(d * d + 0.0025) * d)
        for f, y in enumerate(x):
            for k in range(4):
                out[f, c // 8, pl.ds(8 * k + c % 8, 8, stride=40), :] = y[8 * k : 8 * k + 8]


def second_interior(*refs):
    f4, (st, sc, tmp1, tmp2, out) = refs[0], refs[5:]
    interior(st, sc, tmp1, tmp2, f4[...])
    stage_out(st, sc, out, range(4, 12))


def run_strips(strip, work, cor4):
    _, lane = iotas((R, 128))
    last = lane == 127
    f4 = jnp.broadcast_to(cor4[pl.ds(31, 1), :], (R, 128))
    for side in range(2):
        raw = {name: strip[side * TOP + k] for k, name in enumerate(FIELDS)}
        out, ice = statics(raw)
        work[5 * side + U] = raw["u"]
        work[5 * side + V] = raw["v"]
        for k, name in ((S1, "s1"), (S2, "s2"), (S12, "s12")):
            work[5 * side + k] = jnp.where(ice, raw[name], 0.0)
        for k in range(9):
            work[10 + 9 * side + k] = out[k]

    def step():
        x = [[work[5 * side + k] for k in range(5)] for side in range(2)]
        east = [lambda y: pltpu.roll(y, R - 1, 0), lambda y: pltpu.roll(y, 1, 0)]
        west = [east[1], east[0]]
        down = lambda y: pltpu.roll(y, 1, 1)
        up = lambda y, other, sign: jnp.where(last, sign * other, pltpu.roll(y, 127, 1))
        terms = []
        for side in range(2):
            e, w = east[side], west[side]
            u, v = x[side][U], x[side][V]
            ou, ov = x[1 - side][U], x[1 - side][V]
            upu, um, vp, vm = up(u, ou, -1.0), down(u), up(v, ov, -1.0), down(v)
            tt, d2, ww, dv2 = u + upu, upu - um, v + vm, vp - vm
            terms.append((tt, ww))
            k = lambda n: work[10 + 9 * side + n]
            a1, a2, a12 = stress_terms(
                u - w(u),
                v - vm,
                (d2 + w(d2)) + (e(ww) - w(ww)),
                e(tt) - w(tt),
                dv2 + e(dv2),
                (upu - u) + (e(v) - v),
                k(PR),
            )
            x[side][S1] = K29 * x[side][S1] + a1
            x[side][S2] = K29 * x[side][S2] + a2
            x[side][S12] = K29 * x[side][S12] + a12
        new = []
        for side in range(2):
            e, w = east[side], west[side]
            u, v, s1, s2, s12 = x[side]
            q1, q2 = s1 + s2, s1 - s2
            other = x[1 - side][S1] - x[1 - side][S2]
            fu = 0.5 * (e(q1) - q1) + (s12 - down(s12))
            fv = 0.5 * (up(q2, other, 1.0) - q2) + (s12 - w(s12))
            tt, ww = terms[side]
            k = lambda n: work[10 + 9 * side + n]
            ice = k(MK) == 2.0
            nu = momentum(u, k(UO), k(CU), k(MI), fu, f4 * (ww + e(ww)), ice, k(OU))
            nv = momentum(v, k(VO), k(CV), k(MI), fv, -f4 * (tt + w(tt)), ice, k(OV))
            new.append((nu, nv, s1, s2, s12))
        for side in range(2):
            for k in range(5):
                work[5 * side + k] = new[side][k]

    return step


def second_edges(*refs):
    rb, ra, f4 = refs[:3]
    vel_o, str_o, oce_o, st, sc, tmp1, tmp2, strip, out, work, sems = refs[9:]
    even = parity() == 0
    left, right = receive(rb, ra, SECOND, even)
    for k, name in enumerate(STATE):
        st[k, rows(-1), :], st[k, rows(C), :] = left[name], right[name]
    edges(st, sc, tmp1, tmp2, f4[...], next_names(left), next_names(right))
    whole = out.reshape(7, 2, 8, 40, 128)
    copies = []

    def start(ih, at):
        for dst, f in ((vel_o, 0), (str_o, 2), (oce_o, 5)):
            src = whole.at[pl.ds(f, dst.shape[0]), ih, at, pl.ds(0, 32), :]
            sem = sems.at[len(copies)]
            copies.append(pltpu.make_async_copy(src, dst.at[:, ih, at], sem))
            copies[-1].start()

    for ih, cols in enumerate((range(4), range(12, 16))):
        stage_out(st, sc, out, cols)
        start(ih, pl.ds(0, 7))
    base = len(SECOND) * R
    pb = [rb[pl.ds(base + 8 * n, 8), :] for n in range(3)]
    pa = [ra[pl.ds(base + 8 * n, 8), :] for n in range(3)]
    low = [jnp.where(even, b, a) for b, a in zip(pb, pa)]
    high = [jnp.where(even, a, b) for b, a in zip(pb, pa)]
    for k in range(2 * TOP):
        strip[k, pl.ds(0, 8), :] = spread(low, k)
        strip[k, pl.ds(24, 8), :] = spread(high, k)
    step = run_strips(strip, work, f4)
    for _ in range(4):
        step()
    top = iotas((8, 128))[1] >= 120
    for ih in range(2):
        mine = pl.ds(8 + 8 * ih, 8)
        x = [work[k, mine, :] for k in range(5)]
        for w, o in ((U, UO), (V, VO)):
            d = x[w] - work[10 + o, mine, :]
            x.append(0.5 * root(d * d + 0.0025) * d)
        tile = pl.ds(7 * 40 + 24, 8)
        for f, y in enumerate(x):
            out[f, ih, tile, :] = jnp.where(top, y, out[f, ih, tile, :])
        start(ih, pl.ds(7, 1))
    for c in copies:
        c.wait()


HBM = pl.BlockSpec(memory_space=pltpu.HBM)
VM = pl.BlockSpec(memory_space=pltpu.VMEM)


def shape(*dims):
    return jax.ShapeDtypeStruct(dims, F32)


def permuted(x, pairs):
    return lax.ppermute(x, AXES, pairs)


N = 128
CROSS = [(d, (d + 1) % N if d % 2 else (d - 1) % N) for d in range(N)]
CHIP = [(d, d ^ 1) for d in range(N)]
MIRROR = [(d, N - 1 - d) for d in range(N)]


def coriolis():
    b = 4 * np.arange(8)[None, :] + np.arange(4)[:, None]
    j = b.reshape(32, 1) * 128 + np.arange(128)[None, :]
    return (0.125 * np.sin(math.pi * ((j + 0.5) / 4096 - 0.5))).astype(np.float32)


def edge_scratch():
    return [pltpu.VMEM((5, NC * R, 128), F32), pltpu.VMEM((9, NC * R, 128), F32)]


def call(kernel, out, ins, specs, scratch, alias=None, outs=None, cost=None):
    return pl.pallas_call(
        kernel,
        out_shape=out,
        in_specs=specs,
        out_specs=outs or [VM] * len(out),
        scratch_shapes=scratch,
        input_output_aliases=alias or {},
        compiler_params=pltpu.CompilerParams(vmem_limit_bytes=20 << 20),
        cost_estimate=cost,
    )(*ins)


def on_device(forcing, ice_state, velocity, stress, ice_mask):
    raw = [
        pltpu.with_memory_space_constraint(view(x), pltpu.HBM)
        for x in (forcing, ice_state, velocity, stress, ice_mask[None])
    ]
    vel, strs, ocean = window(raw)
    return unview(vel), unview(strs), unview(ocean)


def window(raw):
    n1, n2 = len(FIRST) * R, len(SECOND) * R + 24
    cor = pltpu.with_memory_space_constraint(jnp.asarray(coriolis()), pltpu.HBM)
    cost = pl.CostEstimate(flops=20_000_000, bytes_accessed=4_000_000, transcendentals=500_000)
    b, m, f4 = call(
        pack_cross,
        [shape(n1, 128), shape(24, 128), shape(R, 128)],
        [*raw, cor],
        [HBM] * 6,
        [
            *edge_scratch(),
            pltpu.VMEM((11, 1, *STAGE[1:]), F32),
            pltpu.VMEM((1, 1, *STAGE[1:]), jnp.int32),
            pltpu.VMEM((11, 2, 8, 128), F32),
            pltpu.VMEM((1, 2, 8, 128), jnp.int32),
            pltpu.SemaphoreType.DMA((11,)),
        ],
    )
    rb = permuted(b, CROSS)
    rm = permuted(m, MIRROR)
    a, stage, mstage = call(
        pack_chip,
        [
            shape(n1, 128),
            shape(11, *STAGE),
            jax.ShapeDtypeStruct((1, *STAGE), jnp.int32),
        ],
        [*raw, f4],
        [HBM] * 5 + [VM],
        [*edge_scratch(), pltpu.SemaphoreType.DMA((5,))],
        cost=cost,
    )
    ra = permuted(a, CHIP)
    main = [shape(5, NC * R, 128), shape(9, NC * R, 128), *[shape(6, NC * R, 128)] * 2]
    strips = shape(2 * TOP, R, 128)
    *state, strip = call(
        first_interior, [*main, strips], [stage, mstage, f4], [VM] * 3, [], cost=cost
    )
    *state, strip, b = call(
        cross_edges,
        [*main, strips, shape(n2, 128)],
        [rb, rm, f4, *state, strip],
        [VM] * 8,
        [],
        alias={3 + k: k for k in range(5)},
    )
    rb = permuted(b, CROSS)
    *state, strip, a = call(
        chip_edges,
        [*main, strips, shape(n2, 128)],
        [ra, f4, *state, strip],
        [VM] * 7,
        [],
        alias={2 + k: k for k in range(5)},
        cost=cost,
    )
    ra = permuted(a, CHIP)
    *state, out = call(
        second_interior,
        [*main, shape(7, *STAGE)],
        [f4, *state],
        [VM] * 5,
        [],
        alias={1 + k: k for k in range(4)},
        cost=cost,
    )
    vel, strs, ocean, *_ = call(
        second_edges,
        [*[shape(n, 2, 8, 32, 128) for n in (2, 3, 2)], *main, strips, shape(7, *STAGE)],
        [rb, ra, f4, *state, strip, out],
        [VM] * 9,
        [pltpu.VMEM((28, R, 128), F32), pltpu.SemaphoreType.DMA((12,))],
        alias={3 + k: 3 + k for k in range(6)},
        outs=[HBM] * 3 + [VM] * 6,
    )
    return vel, strs, ocean


def solution(mesh):
    slab = P(None, AXES, None)
    return jax.shard_map(
        on_device,
        mesh=mesh,
        in_specs=(slab, slab, slab, slab, P(AXES, None)),
        out_specs=(slab, slab, slab),
        check_vma=False,
    )
```

```python
import math

import jax
import jax.numpy as jnp
import numpy as np
from jax import lax
from jax.experimental import pallas as pl
from jax.experimental.pallas import tpu as pltpu
from jax.sharding import PartitionSpec as P


F32 = jnp.float32
AXES = ("gx", "gy")
C = 16
R = 32
H = 3
NC = C + 2 * H
FIELDS = ("uo", "vo", "tx", "ty", "a", "h", "u", "v", "s1", "s2", "s12", "mask")
WHERE = {n: k for k, n in enumerate(FIELDS)}
STATE = ("u", "v", "s1", "s2", "s12")
NEXT = ("u", "v", "z", "alpha", "beta")
U, V, S1, S2, S12 = range(5)
PR, MI, UO, CU, VO, CV, MK, OU, OV = range(9)
T, D2, W, DV2, E1, UP = range(6)
K29 = 29.0 / 30.0
STAGE = (2, 8 * 40, 128)
TOP = len(FIELDS)


def view(x):
    c = x.shape[0]
    return x.reshape(c, 2, 8, 8, 4, 128).transpose(0, 1, 3, 4, 2, 5).reshape(c, 2, 8, 32, 128)


def unview(y):
    c = y.shape[0]
    return y.reshape(c, 2, 8, 4, 8, 128).transpose(0, 1, 4, 2, 3, 5).reshape(c, C, 4096)


def iotas(shape):
    return lax.broadcasted_iota(jnp.int32, shape, 0), lax.broadcasted_iota(jnp.int32, shape, 1)


def root(x):
    return x * lax.rsqrt(jnp.maximum(x, 1e-30))


def below(x, masks):
    lane0, _, sub0, _ = masks
    r = pltpu.roll(x, 1, 1)
    q = jnp.where(sub0, 0.0, pltpu.roll(r[24:32], 1, 0))
    return jnp.where(lane0, jnp.concatenate([q, r[0:24]], 0), r)


def above(x, masks):
    _, lane127, _, _ = masks
    r = pltpu.roll(x, 127, 1)
    q = pltpu.roll(r[0:8], 7, 0)
    return jnp.where(lane127, jnp.concatenate([r[8:32], q], 0), r)


def make_masks():
    _, lane = iotas((R, 128))
    sub, _ = iotas((8, 128))
    return lane == 0, lane == 127, sub == 0, sub == 7


def rows(c):
    return pl.ds(pl.multiple_of((c + H) * R, R), R)


def each_column(span, body):
    if isinstance(span, tuple):
        lo, hi, chunk = span

        def step(t, carry):
            for q in range(chunk):
                body(lo + t * chunk + q)
            return carry

        lax.fori_loop(0, (hi - lo) // chunk, step, 0)
    else:
        for c in span:
            body(c)


def stress_terms(x1, e1, sc4, x, y, s, p):
    d = x1 + e1
    e = x1 - e1
    delta = root(d * d + 0.25 * (e * e) + (1.0 / 64.0) * (sc4 * sc4))
    r = p / (delta + 0.05)
    dk = x + y
    ek = x - y
    dk2 = root((1.0 / 16.0) * (dk * dk) + (1.0 / 64.0) * (ek * ek) + 0.25 * (s * s))
    rk = p / (dk2 + 0.05)
    return r * (d - delta), r * (0.25 * e), rk * (0.125 * s)


def momentum(w, o, c, mi, force, cor, ice, open_o):
    g = 0.5 * root((o - w) * (o - w) + 0.0025) * mi
    new = (30.0 * w + c + force * mi + g * o + cor) / (31.0 + g)
    return jnp.where(ice, new, open_o)


def subcycle(st, sc, tmp, f4, masks, vel, stress, mom):
    def shift(c):
        u, v = st[U, rows(c), :], st[V, rows(c), :]
        up, um = above(u, masks), below(u, masks)
        vp, vm = above(v, masks), below(v, masks)
        tmp[T, rows(c), :] = u + up
        tmp[D2, rows(c), :] = up - um
        tmp[UP, rows(c), :] = up - u
        tmp[W, rows(c), :] = v + vm
        tmp[E1, rows(c), :] = v - vm
        tmp[DV2, rows(c), :] = vp - vm

    each_column(vel, shift)

    def strain(c):
        ld = lambda k, d=0: tmp[k, rows(c + d), :]
        us = lambda d: st[U, rows(c + d), :]
        vs = lambda d: st[V, rows(c + d), :]
        a1, a2, a12 = stress_terms(
            us(0) - us(-1),
            ld(E1),
            (ld(D2) + ld(D2, -1)) + (ld(W, 1) - ld(W, -1)),
            ld(T, 1) - ld(T, -1),
            ld(DV2) + ld(DV2, 1),
            ld(UP) + (vs(1) - vs(0)),
            sc[PR, rows(c), :],
        )
        st[S1, rows(c), :] = K29 * st[S1, rows(c), :] + a1
        st[S2, rows(c), :] = K29 * st[S2, rows(c), :] + a2
        st[S12, rows(c), :] = K29 * st[S12, rows(c), :] + a12

    each_column(stress, strain)

    def move(c):
        ss = lambda k, d=0: st[k, rows(c + d), :]
        q1 = ss(S1) + ss(S2)
        q1n = ss(S1, 1) + ss(S2, 1)
        q2 = ss(S1) - ss(S2)
        s12 = ss(S12)
        fu = 0.5 * (q1n - q1) + (s12 - below(s12, masks))
        fv = 0.5 * (above(q2, masks) - q2) + (s12 - ss(S12, -1))
        cu = f4 * (tmp[W, rows(c), :] + tmp[W, rows(c + 1), :])
        cv = f4 * (tmp[T, rows(c), :] + tmp[T, rows(c - 1), :])
        k = lambda n: sc[n, rows(c), :]
        ice = k(MK) == 2.0
        mi = k(MI)
        st[U, rows(c), :] = momentum(ss(U), k(UO), k(CU), mi, fu, cu, ice, k(OU))
        st[V, rows(c), :] = momentum(ss(V), k(VO), k(CV), mi, fv, -cv, ice, k(OV))

    each_column(mom, move)


def interior(st, sc, tmp1, tmp2, f4):
    masks = make_masks()
    subcycle(st, sc, tmp1, f4, masks, (0, 16, 8), (1, 15, 7), (2, 14, 6))
    subcycle(st, sc, tmp2, f4, masks, (2, 14, 6), (3, 13, 5), (4, 12, 4))


def edges(st, sc, tmp1, tmp2, f4, left=None, right=None):
    masks = make_masks()

    def near(a, b, c, d):
        return [*(range(a, b) if left else ()), *(range(c, d) if right else ())]

    if left:
        st[U, rows(-2), :], st[V, rows(-2), :] = left["u"], left["v"]
        st[S12, rows(-2), :] = left["z"]
    if right:
        st[U, rows(17), :], st[V, rows(17), :] = right["u"], right["v"]
        st[S1, rows(17), :] = right["z"]
        st[S2, rows(17), :] = jnp.zeros((R, 128), F32)
    subcycle(
        st, sc, tmp1, f4, masks, near(-2, 0, 16, 18), near(-1, 1, 15, 17), near(-1, 2, 14, 17)
    )
    if left:
        n11 = 0.5 * (st[S1, rows(-1), :] + st[S2, rows(-1), :])
        st[U, rows(-2), :] = left["alpha"] + left["beta"] * n11
    if right:
        st[V, rows(17), :] = right["alpha"] - right["beta"] * st[S12, rows(16), :]
    subcycle(
        st, sc, tmp2, f4, masks, near(-2, 2, 14, 18), near(-1, 3, 13, 17), near(0, 4, 12, 16)
    )


def outgoing(st, sc, f4, side):
    masks = make_masks()

    def around(c):
        s = lambda k, d=0: st[k, rows(c + d), :]
        f = lambda k: sc[k, rows(c), :]
        t, d2, w, dv2 = [], [], [], []
        for d in (-1, 0, 1):
            u, v = s(U, d), s(V, d)
            up, um, vp, vm = above(u, masks), below(u, masks), above(v, masks), below(v, masks)
            t.append(u + up)
            d2.append(up - um)
            w.append(v + vm)
            dv2.append(vp - vm)
            if d == 0:
                e1, rise = v - vm, up - u
        a1, a2, a12 = stress_terms(
            s(U) - s(U, -1),
            e1,
            (d2[1] + d2[0]) + (w[2] - w[0]),
            t[2] - t[0],
            dv2[1] + dv2[2],
            rise + (s(V, 1) - s(V)),
            f(PR),
        )
        s1, s2, s12 = K29 * s(S1) + a1, K29 * s(S2) + a2, K29 * s(S12) + a12
        return s, f, t, w, s1 + s2, s1 - s2, s12

    def numbers(x, o, c, mi, force, cor, ice, open_o):
        g = 0.5 * root((o - x) * (o - x) + 0.0025) * mi
        b = 1.0 / (31.0 + g)
        a = (30.0 * x + c + force * mi + g * o + cor) * b
        return jnp.where(ice, a, open_o), jnp.where(ice, mi * b, 0.0)

    if side == 0:
        s, f, t, w, q1, q2, s12 = around(1)
        force = 0.5 * (above(q2, masks) - q2) + s12
        cor = -f4 * (t[1] + t[0])
        ice = f(MK) == 2.0
        return s(U), s(V), q1, *numbers(s(V), f(VO), f(CV), f(MI), force, cor, ice, f(OV))
    s, f, t, w, q1, q2, s12 = around(C - 2)
    force = (s12 - below(s12, masks)) - 0.5 * q1
    cor = f4 * (w[1] + w[2])
    ice = f(MK) == 2.0
    return s(U), s(V), s12, *numbers(s(U), f(UO), f(CU), f(MI), force, cor, ice, f(OU))


def put(out, xs, n=0):
    for x in xs:
        out[pl.ds(n * R, R), :] = x
        n += 1


def take(ref, names):
    return {name: ref[pl.ds(n * R, R), :] for n, name in enumerate(names)}


def receive(rb, ra, names, even):
    b, a = take(rb, names), take(ra, names)
    left = {n: jnp.where(even, b[n], a[n]) for n in names}
    right = {n: jnp.where(even, a[n], b[n]) for n in names}
    return left, right


def next_names(x):
    return {n: x[n + "1"] for n in NEXT}


FIRST = (*FIELDS, *[n + "1" for n in NEXT])
SECOND = (*STATE, *[n + "1" for n in NEXT])


def statics(raw):
    a, h, mask = raw["a"], raw["h"], raw["mask"]
    ice = mask == 2.0
    opened = mask == 1.0
    mi = 1.0 / (a * h)
    out = {
        PR: jnp.where(ice, h * jnp.exp(-20.0 * (1.0 - a)) * (1.0 / 30.0), 0.0),
        MI: mi,
        UO: raw["uo"],
        CU: raw["u"] + raw["tx"] * mi,
        VO: raw["vo"],
        CV: raw["v"] + raw["ty"] * mi,
        MK: mask,
        OU: jnp.where(opened, raw["uo"], 0.0),
        OV: jnp.where(opened, raw["vo"], 0.0),
    }
    return out, ice


def put_column(st, sc, at, raw):
    out, ice = statics(raw)
    for k, x in out.items():
        sc[k, at, :] = x
    st[U, at, :] = raw["u"]
    st[V, at, :] = raw["v"]
    st[S1, at, :] = jnp.where(ice, raw["s1"], 0.0)
    st[S2, at, :] = jnp.where(ice, raw["s2"], 0.0)
    st[S12, at, :] = jnp.where(ice, raw["s12"], 0.0)


def stage_in(srcs, stage, mstage, sems):
    copies = []
    at = 0
    for k, src in enumerate(srcs):
        n = src.shape[0]
        if k < 4:
            dst = stage.reshape(11, 2, 8, 40, 128).at[pl.ds(at, n), :, :, pl.ds(0, 32), :]
        else:
            dst = mstage.reshape(1, 2, 8, 40, 128).at[:, :, :, pl.ds(0, 32), :]
        copies.append(pltpu.make_async_copy(src, dst, sems.at[k]))
        at += n
    for c in copies:
        c.start()
    for c in copies:
        c.wait()


def staged_column(stage, mstage, name, c):
    ref, f = (mstage, 0) if name == "mask" else (stage, WHERE[name])
    parts = [ref[f, c // 8, pl.ds(8 * k + c % 8, 8, stride=40), :] for k in range(4)]
    return jnp.concatenate(parts, 0).astype(F32)


def parity():
    return lax.rem(lax.axis_index("gy"), 2)


def squeeze(tiles):
    _, lane = iotas((8, 128))
    out = []
    for t in range(0, len(tiles), 8):
        x = tiles[t + 7]
        for g in range(7):
            x = jnp.where(lane // 16 == g, pltpu.roll(tiles[t + g], 16 * (g + 1), 1), x)
        out.append(x)
    return out


def spread(packed, n):
    x = packed[n // 8]
    g = n % 8
    return x if g == 7 else pltpu.roll(x, 128 - 16 * (g + 1), 1)


def top_tile(stage, mstage, k, ih):
    ref, f = (mstage, 0) if k == TOP - 1 else (stage, k)
    return ref[f, ih, pl.ds(7 * 40 + 24, 8), :].astype(F32)


def by_side(cross, body):
    even = parity() == 0
    here = even if cross else jnp.logical_not(even)

    @pl.when(here)
    def _():
        body(0)

    @pl.when(jnp.logical_not(here))
    def _():
        body(1)


def pack_side(out, f4, st, sc, stage, mstage, side, half):
    def column(name, m):
        ref, f = (mstage, 0) if name == "mask" else (stage, WHERE[name])
        il = 7 - m if side else m
        parts = [ref[f, half, pl.ds(8 * k + il, 8, stride=40), :] for k in range(4)]
        return jnp.concatenate(parts, 0).astype(F32)

    at = lambda m: rows(C - 1 - m if side else m)
    put_column(st, sc, at(1), {name: column(name, 1) for name in FIELDS})
    for m in (0, 2):
        st[U, at(m), :], st[V, at(m), :] = column("u", m), column("v", m)
    put(out, [column(name, 0) for name in FIELDS])
    put(out, outgoing(st, sc, f4[...], side), TOP)


def pack_cross(
    f_ref, i_ref, v_ref, s_ref, m_ref, cor, b_out, m_out, f4, st, sc, stage, mstage, top, mtop, sems
):
    srcs = (f_ref, i_ref, v_ref, s_ref, m_ref)

    def body(side):
        main = [pltpu.make_async_copy(cor, f4, sems.at[5])]
        tops = []
        il = pl.ds(5 if side else 0, 3)
        at = 0
        for k, src in enumerate(srcs):
            n = src.shape[0]
            if k < 4:
                dst = stage.reshape(11, 8, 5, 8, 128).at[pl.ds(at, n), :, pl.ds(0, 4), il, :]
            else:
                dst = mstage.reshape(1, 8, 5, 8, 128).at[:, :, pl.ds(0, 4), il, :]
            part = src.reshape(n, 2, 8, 4, 8, 128).at[:, side, :, :, il, :]
            main.append(pltpu.make_async_copy(part, dst, sems.at[k]))
            dst = top.at[pl.ds(at, n)] if k < 4 else mtop
            tile = src.at[:, :, 7, pl.ds(24, 8), :]
            tops.append(pltpu.make_async_copy(tile, dst, sems.at[6 + k]))
            at += n
        for c in main + tops:
            c.start()
        for c in main:
            c.wait()
        pack_side(b_out, f4, st, sc, stage, mstage, side, 0)
        for c in tops:
            c.wait()
        tiles = [
            mtop[0, ih].astype(F32) if k == TOP - 1 else top[k, ih]
            for k in range(TOP)
            for ih in range(2)
        ]
        for n, x in enumerate(squeeze(tiles)):
            m_out[pl.ds(8 * n, 8), :] = x
            b_out[pl.ds(len(FIRST) * R + 8 * n, 8), :] = x

    by_side(True, body)


def pack_chip(f_ref, i_ref, v_ref, s_ref, m_ref, f4, a_out, stage, mstage, st, sc, sems):
    stage_in((f_ref, i_ref, v_ref, s_ref, m_ref), stage, mstage, sems)
    by_side(False, lambda side: pack_side(a_out, f4, st, sc, stage, mstage, side, side))


def first_interior(stage, mstage, f4, st, sc, tmp1, tmp2, strip):
    for c in range(C):
        put_column(
            st, sc, rows(c), {name: staged_column(stage, mstage, name, c) for name in FIELDS}
        )
    for k in range(TOP):
        for ih in range(2):
            strip[k, pl.ds(8 + 8 * ih, 8), :] = top_tile(stage, mstage, k, ih)
    interior(st, sc, tmp1, tmp2, f4[...])


def edge_side(r, out, st, sc, tmp1, tmp2, strip, f4, cross):
    def body(side):
        got = take(r, FIRST)
        put_column(st, sc, rows(C if side else -1), got)
        edges(st, sc, tmp1, tmp2, f4[...], **{("left", "right")[side]: next_names(got)})
        put(out, [st[k, rows(C - 1 if side else 0), :] for k in range(5)])
        put(out, outgoing(st, sc, f4[...], side), 5)
        tiles = squeeze([strip[k, pl.ds(16 if side else 8, 8), :] for k in range(2 * TOP)])
        for n, x in enumerate(tiles):
            out[pl.ds(len(SECOND) * R + 8 * n, 8), :] = x

    by_side(cross, body)


def cross_edges(*refs):
    rb, rm, f4 = refs[:3]
    st, sc, tmp1, tmp2, strip, out = refs[8:]
    flip = 7 - iotas((8, 128))[0]
    slab = lax.axis_index("gx") * lax.axis_size("gy") + lax.axis_index("gy")
    paired = (slab == 0) | (slab == N - 1) | (slab == N // 2 - 1) | (slab == N // 2)
    packed = [
        jnp.where(paired, rb[pl.ds(len(FIRST) * R + 8 * n, 8), :], rm[pl.ds(8 * n, 8), :])
        for n in range(3)
    ]
    for k in range(TOP):
        for ih in range(2):
            x = spread(packed, 2 * k + ih)
            strip[TOP + k, pl.ds(16 - 8 * ih, 8), :] = jnp.take_along_axis(x, flip, axis=0)
    edge_side(rb, out, st, sc, tmp1, tmp2, strip, f4, True)


def chip_edges(*refs):
    ra, f4 = refs[:2]
    st, sc, tmp1, tmp2, strip, out = refs[7:]
    edge_side(ra, out, st, sc, tmp1, tmp2, strip, f4, False)


def stage_out(st, sc, out, cols):
    for c in cols:
        x = [st[k, rows(c), :] for k in range(5)]
        for w, o in ((U, UO), (V, VO)):
            d = x[w] - sc[o, rows(c), :]
            x.append(0.5 * root(d * d + 0.0025) * d)
        for f, y in enumerate(x):
            for k in range(4):
                out[f, c // 8, pl.ds(8 * k + c % 8, 8, stride=40), :] = y[8 * k : 8 * k + 8]


def second_interior(*refs):
    f4, (st, sc, tmp1, tmp2, out) = refs[0], refs[5:]
    interior(st, sc, tmp1, tmp2, f4[...])
    stage_out(st, sc, out, range(4, 12))


def run_strips(strip, work, cor4):
    _, lane = iotas((R, 128))
    last = lane == 127
    f4 = jnp.broadcast_to(cor4[pl.ds(31, 1), :], (R, 128))
    for side in range(2):
        raw = {name: strip[side * TOP + k] for k, name in enumerate(FIELDS)}
        out, ice = statics(raw)
        work[5 * side + U] = raw["u"]
        work[5 * side + V] = raw["v"]
        for k, name in ((S1, "s1"), (S2, "s2"), (S12, "s12")):
            work[5 * side + k] = jnp.where(ice, raw[name], 0.0)
        for k in range(9):
            work[10 + 9 * side + k] = out[k]

    def step():
        x = [[work[5 * side + k] for k in range(5)] for side in range(2)]
        east = [lambda y: pltpu.roll(y, R - 1, 0), lambda y: pltpu.roll(y, 1, 0)]
        west = [east[1], east[0]]
        down = lambda y: pltpu.roll(y, 1, 1)
        up = lambda y, other, sign: jnp.where(last, sign * other, pltpu.roll(y, 127, 1))
        terms = []
        for side in range(2):
            e, w = east[side], west[side]
            u, v = x[side][U], x[side][V]
            ou, ov = x[1 - side][U], x[1 - side][V]
            upu, um, vp, vm = up(u, ou, -1.0), down(u), up(v, ov, -1.0), down(v)
            tt, d2, ww, dv2 = u + upu, upu - um, v + vm, vp - vm
            terms.append((tt, ww))
            k = lambda n: work[10 + 9 * side + n]
            a1, a2, a12 = stress_terms(
                u - w(u),
                v - vm,
                (d2 + w(d2)) + (e(ww) - w(ww)),
                e(tt) - w(tt),
                dv2 + e(dv2),
                (upu - u) + (e(v) - v),
                k(PR),
            )
            x[side][S1] = K29 * x[side][S1] + a1
            x[side][S2] = K29 * x[side][S2] + a2
            x[side][S12] = K29 * x[side][S12] + a12
        new = []
        for side in range(2):
            e, w = east[side], west[side]
            u, v, s1, s2, s12 = x[side]
            q1, q2 = s1 + s2, s1 - s2
            other = x[1 - side][S1] - x[1 - side][S2]
            fu = 0.5 * (e(q1) - q1) + (s12 - down(s12))
            fv = 0.5 * (up(q2, other, 1.0) - q2) + (s12 - w(s12))
            tt, ww = terms[side]
            k = lambda n: work[10 + 9 * side + n]
            ice = k(MK) == 2.0
            nu = momentum(u, k(UO), k(CU), k(MI), fu, f4 * (ww + e(ww)), ice, k(OU))
            nv = momentum(v, k(VO), k(CV), k(MI), fv, -f4 * (tt + w(tt)), ice, k(OV))
            new.append((nu, nv, s1, s2, s12))
        for side in range(2):
            for k in range(5):
                work[5 * side + k] = new[side][k]

    return step


def second_edges(*refs):
    rb, ra, f4 = refs[:3]
    vel_o, str_o, oce_o, st, sc, tmp1, tmp2, strip, out, work, sems = refs[9:]
    even = parity() == 0
    left, right = receive(rb, ra, SECOND, even)
    for k, name in enumerate(STATE):
        st[k, rows(-1), :], st[k, rows(C), :] = left[name], right[name]
    edges(st, sc, tmp1, tmp2, f4[...], next_names(left), next_names(right))
    whole = out.reshape(7, 2, 8, 40, 128)
    copies = []

    def start(ih, at):
        for dst, f in ((vel_o, 0), (str_o, 2), (oce_o, 5)):
            src = whole.at[pl.ds(f, dst.shape[0]), ih, at, pl.ds(0, 32), :]
            sem = sems.at[len(copies)]
            copies.append(pltpu.make_async_copy(src, dst.at[:, ih, at], sem))
            copies[-1].start()

    for ih, cols in enumerate((range(4), range(12, 16))):
        stage_out(st, sc, out, cols)
        start(ih, pl.ds(0, 7))
    base = len(SECOND) * R
    pb = [rb[pl.ds(base + 8 * n, 8), :] for n in range(3)]
    pa = [ra[pl.ds(base + 8 * n, 8), :] for n in range(3)]
    low = [jnp.where(even, b, a) for b, a in zip(pb, pa)]
    high = [jnp.where(even, a, b) for b, a in zip(pb, pa)]
    for k in range(2 * TOP):
        strip[k, pl.ds(0, 8), :] = spread(low, k)
        strip[k, pl.ds(24, 8), :] = spread(high, k)
    step = run_strips(strip, work, f4)
    for _ in range(4):
        step()
    top = iotas((8, 128))[1] >= 120
    for ih in range(2):
        mine = pl.ds(8 + 8 * ih, 8)
        x = [work[k, mine, :] for k in range(5)]
        for w, o in ((U, UO), (V, VO)):
            d = x[w] - work[10 + o, mine, :]
            x.append(0.5 * root(d * d + 0.0025) * d)
        tile = pl.ds(7 * 40 + 24, 8)
        for f, y in enumerate(x):
            out[f, ih, tile, :] = jnp.where(top, y, out[f, ih, tile, :])
        start(ih, pl.ds(7, 1))
    for c in copies:
        c.wait()


HBM = pl.BlockSpec(memory_space=pltpu.HBM)
VM = pl.BlockSpec(memory_space=pltpu.VMEM)


def shape(*dims):
    return jax.ShapeDtypeStruct(dims, F32)


def permuted(x, pairs):
    return lax.ppermute(x, AXES, pairs)


N = 128
CROSS = [(d, (d + 1) % N if d % 2 else (d - 1) % N) for d in range(N)]
CHIP = [(d, d ^ 1) for d in range(N)]
MIRROR = [(d, (d + N // 2) % N if (d, N - 1 - d) in CROSS else N - 1 - d) for d in range(N)]


def coriolis():
    b = 4 * np.arange(8)[None, :] + np.arange(4)[:, None]
    j = b.reshape(32, 1) * 128 + np.arange(128)[None, :]
    return (0.125 * np.sin(math.pi * ((j + 0.5) / 4096 - 0.5))).astype(np.float32)


def edge_scratch():
    return [pltpu.VMEM((5, NC * R, 128), F32), pltpu.VMEM((9, NC * R, 128), F32)]


def call(kernel, out, ins, specs, scratch, alias=None, outs=None, cost=None):
    return pl.pallas_call(
        kernel,
        out_shape=out,
        in_specs=specs,
        out_specs=outs or [VM] * len(out),
        scratch_shapes=scratch,
        input_output_aliases=alias or {},
        compiler_params=pltpu.CompilerParams(vmem_limit_bytes=20 << 20),
        cost_estimate=cost,
    )(*ins)


def on_device(forcing, ice_state, velocity, stress, ice_mask):
    raw = [
        pltpu.with_memory_space_constraint(view(x), pltpu.HBM)
        for x in (forcing, ice_state, velocity, stress, ice_mask[None])
    ]
    vel, strs, ocean = window(raw)
    return unview(vel), unview(strs), unview(ocean)


def window(raw):
    n1, n2 = len(FIRST) * R, len(SECOND) * R + 24
    cor = pltpu.with_memory_space_constraint(jnp.asarray(coriolis()), pltpu.HBM)
    cost = pl.CostEstimate(flops=20_000_000, bytes_accessed=4_000_000, transcendentals=500_000)
    b, m, f4 = call(
        pack_cross,
        [shape(n1 + 24, 128), shape(24, 128), shape(R, 128)],
        [*raw, cor],
        [HBM] * 6,
        [
            *edge_scratch(),
            pltpu.VMEM((11, 1, *STAGE[1:]), F32),
            pltpu.VMEM((1, 1, *STAGE[1:]), jnp.int32),
            pltpu.VMEM((11, 2, 8, 128), F32),
            pltpu.VMEM((1, 2, 8, 128), jnp.int32),
            pltpu.SemaphoreType.DMA((11,)),
        ],
    )
    rb = permuted(b, CROSS)
    rm = permuted(m, MIRROR)
    a, stage, mstage = call(
        pack_chip,
        [
            shape(n1, 128),
            shape(11, *STAGE),
            jax.ShapeDtypeStruct((1, *STAGE), jnp.int32),
        ],
        [*raw, f4],
        [HBM] * 5 + [VM],
        [*edge_scratch(), pltpu.SemaphoreType.DMA((5,))],
        cost=cost,
    )
    ra = permuted(a, CHIP)
    main = [shape(5, NC * R, 128), shape(9, NC * R, 128), *[shape(6, NC * R, 128)] * 2]
    strips = shape(2 * TOP, R, 128)
    *state, strip = call(
        first_interior, [*main, strips], [stage, mstage, f4], [VM] * 3, [], cost=cost
    )
    *state, strip, b = call(
        cross_edges,
        [*main, strips, shape(n2, 128)],
        [rb, rm, f4, *state, strip],
        [VM] * 8,
        [],
        alias={3 + k: k for k in range(5)},
    )
    rb = permuted(b, CROSS)
    *state, strip, a = call(
        chip_edges,
        [*main, strips, shape(n2, 128)],
        [ra, f4, *state, strip],
        [VM] * 7,
        [],
        alias={2 + k: k for k in range(5)},
        cost=cost,
    )
    ra = permuted(a, CHIP)
    *state, out = call(
        second_interior,
        [*main, shape(7, *STAGE)],
        [f4, *state],
        [VM] * 5,
        [],
        alias={1 + k: k for k in range(4)},
        cost=cost,
    )
    vel, strs, ocean, *_ = call(
        second_edges,
        [*[shape(n, 2, 8, 32, 128) for n in (2, 3, 2)], *main, strips, shape(7, *STAGE)],
        [rb, ra, f4, *state, strip, out],
        [VM] * 9,
        [pltpu.VMEM((28, R, 128), F32), pltpu.SemaphoreType.DMA((12,))],
        alias={3 + k: 3 + k for k in range(6)},
        outs=[HBM] * 3 + [VM] * 6,
    )
    return vel, strs, ocean


def solution(mesh):
    slab = P(None, AXES, None)
    return jax.shard_map(
        on_device,
        mesh=mesh,
        in_specs=(slab, slab, slab, slab, P(AXES, None)),
        out_specs=(slab, slab, slab),
        check_vma=False,
    )
```

```python
import math

import jax
import jax.numpy as jnp
import numpy as np
from jax import lax
from jax.experimental import pallas as pl
from jax.experimental.pallas import tpu as pltpu
from jax.sharding import PartitionSpec as P


F32 = jnp.float32
AXES = ("gx", "gy")
C = 16
R = 32
H = 3
NC = C + 2 * H
FIELDS = ("uo", "vo", "tx", "ty", "a", "h", "u", "v", "s1", "s2", "s12", "mask")
WHERE = {n: k for k, n in enumerate(FIELDS)}
STATE = ("u", "v", "s1", "s2", "s12")
NEXT = ("u", "v", "z", "alpha", "beta")
U, V, S1, S2, S12 = range(5)
PR, MI, UO, CU, VO, CV, MK, OU, OV = range(9)
T, D2, W, DV2, E1, UP = range(6)
K29 = 29.0 / 30.0
STAGE = (2, 8 * 40, 128)
TOP = len(FIELDS)


def view(x):
    c = x.shape[0]
    return x.reshape(c, 2, 8, 8, 4, 128).transpose(0, 1, 3, 4, 2, 5).reshape(c, 2, 8, 32, 128)


def unview(y):
    c = y.shape[0]
    return y.reshape(c, 2, 8, 4, 8, 128).transpose(0, 1, 4, 2, 3, 5).reshape(c, C, 4096)


def iotas(shape):
    return lax.broadcasted_iota(jnp.int32, shape, 0), lax.broadcasted_iota(jnp.int32, shape, 1)


def root(x):
    return x * lax.rsqrt(jnp.maximum(x, 1e-30))


def below(x, masks):
    lane0, _, sub0, _ = masks
    r = pltpu.roll(x, 1, 1)
    q = jnp.where(sub0, 0.0, pltpu.roll(r[24:32], 1, 0))
    return jnp.where(lane0, jnp.concatenate([q, r[0:24]], 0), r)


def above(x, masks):
    _, lane127, _, _ = masks
    r = pltpu.roll(x, 127, 1)
    q = pltpu.roll(r[0:8], 7, 0)
    return jnp.where(lane127, jnp.concatenate([r[8:32], q], 0), r)


def make_masks():
    _, lane = iotas((R, 128))
    sub, _ = iotas((8, 128))
    return lane == 0, lane == 127, sub == 0, sub == 7


def rows(c):
    return pl.ds(pl.multiple_of((c + H) * R, R), R)


def each_column(span, body):
    if isinstance(span, tuple):
        lo, hi, chunk = span

        def step(t, carry):
            for q in range(chunk):
                body(lo + t * chunk + q)
            return carry

        lax.fori_loop(0, (hi - lo) // chunk, step, 0)
    else:
        for c in span:
            body(c)


def stress_terms(x1, e1, sc4, x, y, s, p):
    d = x1 + e1
    e = x1 - e1
    delta = root(d * d + 0.25 * (e * e) + (1.0 / 64.0) * (sc4 * sc4))
    r = p / (delta + 0.05)
    dk = x + y
    ek = x - y
    dk2 = root((1.0 / 16.0) * (dk * dk) + (1.0 / 64.0) * (ek * ek) + 0.25 * (s * s))
    rk = p / (dk2 + 0.05)
    return r * (d - delta), r * (0.25 * e), rk * (0.125 * s)


def momentum(w, o, c, mi, force, cor, ice, open_o):
    g = 0.5 * root((o - w) * (o - w) + 0.0025) * mi
    new = (30.0 * w + c + force * mi + g * o + cor) / (31.0 + g)
    return jnp.where(ice, new, open_o)


def subcycle(st, sc, tmp, f4, masks, vel, stress, mom, also=None):
    def shift(c):
        u, v = st[U, rows(c), :], st[V, rows(c), :]
        up, um = above(u, masks), below(u, masks)
        vp, vm = above(v, masks), below(v, masks)
        tmp[T, rows(c), :] = u + up
        tmp[D2, rows(c), :] = up - um
        tmp[UP, rows(c), :] = up - u
        tmp[W, rows(c), :] = v + vm
        tmp[E1, rows(c), :] = v - vm
        tmp[DV2, rows(c), :] = vp - vm

    each_column(vel, shift)

    def strain(c):
        ld = lambda k, d=0: tmp[k, rows(c + d), :]
        us = lambda d: st[U, rows(c + d), :]
        vs = lambda d: st[V, rows(c + d), :]
        a1, a2, a12 = stress_terms(
            us(0) - us(-1),
            ld(E1),
            (ld(D2) + ld(D2, -1)) + (ld(W, 1) - ld(W, -1)),
            ld(T, 1) - ld(T, -1),
            ld(DV2) + ld(DV2, 1),
            ld(UP) + (vs(1) - vs(0)),
            sc[PR, rows(c), :],
        )
        st[S1, rows(c), :] = K29 * st[S1, rows(c), :] + a1
        st[S2, rows(c), :] = K29 * st[S2, rows(c), :] + a2
        st[S12, rows(c), :] = K29 * st[S12, rows(c), :] + a12

    if also:
        also()
    each_column(stress, strain)
    if also:
        also()

    def move(c):
        ss = lambda k, d=0: st[k, rows(c + d), :]
        q1 = ss(S1) + ss(S2)
        q1n = ss(S1, 1) + ss(S2, 1)
        q2 = ss(S1) - ss(S2)
        s12 = ss(S12)
        fu = 0.5 * (q1n - q1) + (s12 - below(s12, masks))
        fv = 0.5 * (above(q2, masks) - q2) + (s12 - ss(S12, -1))
        cu = f4 * (tmp[W, rows(c), :] + tmp[W, rows(c + 1), :])
        cv = f4 * (tmp[T, rows(c), :] + tmp[T, rows(c - 1), :])
        k = lambda n: sc[n, rows(c), :]
        ice = k(MK) == 2.0
        mi = k(MI)
        st[U, rows(c), :] = momentum(ss(U), k(UO), k(CU), mi, fu, cu, ice, k(OU))
        st[V, rows(c), :] = momentum(ss(V), k(VO), k(CV), mi, fv, -cv, ice, k(OV))

    each_column(mom, move)


def interior(st, sc, tmp1, tmp2, f4):
    masks = make_masks()
    subcycle(st, sc, tmp1, f4, masks, (0, 16, 8), (1, 15, 7), (2, 14, 6))
    subcycle(st, sc, tmp2, f4, masks, (2, 14, 6), (3, 13, 5), (4, 12, 4))


def edges(st, sc, tmp1, tmp2, f4, left=None, right=None, also=None):
    masks = make_masks()

    def near(a, b, c, d):
        return [*(range(a, b) if left else ()), *(range(c, d) if right else ())]

    if left:
        st[U, rows(-2), :], st[V, rows(-2), :] = left["u"], left["v"]
        st[S12, rows(-2), :] = left["z"]
    if right:
        st[U, rows(17), :], st[V, rows(17), :] = right["u"], right["v"]
        st[S1, rows(17), :] = right["z"]
        st[S2, rows(17), :] = jnp.zeros((R, 128), F32)
    subcycle(
        st, sc, tmp1, f4, masks, near(-2, 0, 16, 18), near(-1, 1, 15, 17), near(-1, 2, 14, 17), also
    )
    if left:
        n11 = 0.5 * (st[S1, rows(-1), :] + st[S2, rows(-1), :])
        st[U, rows(-2), :] = left["alpha"] + left["beta"] * n11
    if right:
        st[V, rows(17), :] = right["alpha"] - right["beta"] * st[S12, rows(16), :]
    subcycle(
        st, sc, tmp2, f4, masks, near(-2, 2, 14, 18), near(-1, 3, 13, 17), near(0, 4, 12, 16), also
    )


def outgoing(st, sc, f4, side):
    masks = make_masks()

    def around(c):
        s = lambda k, d=0: st[k, rows(c + d), :]
        f = lambda k: sc[k, rows(c), :]
        t, d2, w, dv2 = [], [], [], []
        for d in (-1, 0, 1):
            u, v = s(U, d), s(V, d)
            up, um, vp, vm = above(u, masks), below(u, masks), above(v, masks), below(v, masks)
            t.append(u + up)
            d2.append(up - um)
            w.append(v + vm)
            dv2.append(vp - vm)
            if d == 0:
                e1, rise = v - vm, up - u
        a1, a2, a12 = stress_terms(
            s(U) - s(U, -1),
            e1,
            (d2[1] + d2[0]) + (w[2] - w[0]),
            t[2] - t[0],
            dv2[1] + dv2[2],
            rise + (s(V, 1) - s(V)),
            f(PR),
        )
        s1, s2, s12 = K29 * s(S1) + a1, K29 * s(S2) + a2, K29 * s(S12) + a12
        return s, f, t, w, s1 + s2, s1 - s2, s12

    def numbers(x, o, c, mi, force, cor, ice, open_o):
        g = 0.5 * root((o - x) * (o - x) + 0.0025) * mi
        b = 1.0 / (31.0 + g)
        a = (30.0 * x + c + force * mi + g * o + cor) * b
        return jnp.where(ice, a, open_o), jnp.where(ice, mi * b, 0.0)

    if side == 0:
        s, f, t, w, q1, q2, s12 = around(1)
        force = 0.5 * (above(q2, masks) - q2) + s12
        cor = -f4 * (t[1] + t[0])
        ice = f(MK) == 2.0
        return s(U), s(V), q1, *numbers(s(V), f(VO), f(CV), f(MI), force, cor, ice, f(OV))
    s, f, t, w, q1, q2, s12 = around(C - 2)
    force = (s12 - below(s12, masks)) - 0.5 * q1
    cor = f4 * (w[1] + w[2])
    ice = f(MK) == 2.0
    return s(U), s(V), s12, *numbers(s(U), f(UO), f(CU), f(MI), force, cor, ice, f(OU))


def put(out, xs, n=0):
    for x in xs:
        out[pl.ds(n * R, R), :] = x
        n += 1


def take(ref, names):
    return {name: ref[pl.ds(n * R, R), :] for n, name in enumerate(names)}


def receive(rb, ra, names, even):
    b, a = take(rb, names), take(ra, names)
    left = {n: jnp.where(even, b[n], a[n]) for n in names}
    right = {n: jnp.where(even, a[n], b[n]) for n in names}
    return left, right


def next_names(x):
    return {n: x[n + "1"] for n in NEXT}


FIRST = (*FIELDS, *[n + "1" for n in NEXT])
SECOND = (*STATE, *[n + "1" for n in NEXT])


def statics(raw):
    a, h, mask = raw["a"], raw["h"], raw["mask"]
    ice = mask == 2.0
    opened = mask == 1.0
    mi = 1.0 / (a * h)
    out = {
        PR: jnp.where(ice, h * jnp.exp(-20.0 * (1.0 - a)) * (1.0 / 30.0), 0.0),
        MI: mi,
        UO: raw["uo"],
        CU: raw["u"] + raw["tx"] * mi,
        VO: raw["vo"],
        CV: raw["v"] + raw["ty"] * mi,
        MK: mask,
        OU: jnp.where(opened, raw["uo"], 0.0),
        OV: jnp.where(opened, raw["vo"], 0.0),
    }
    return out, ice


def put_column(st, sc, at, raw):
    out, ice = statics(raw)
    for k, x in out.items():
        sc[k, at, :] = x
    st[U, at, :] = raw["u"]
    st[V, at, :] = raw["v"]
    st[S1, at, :] = jnp.where(ice, raw["s1"], 0.0)
    st[S2, at, :] = jnp.where(ice, raw["s2"], 0.0)
    st[S12, at, :] = jnp.where(ice, raw["s12"], 0.0)


def stage_in(srcs, stage, mstage, sems):
    copies = []
    at = 0
    for k, src in enumerate(srcs):
        n = src.shape[0]
        if k < 4:
            dst = stage.reshape(11, 2, 8, 40, 128).at[pl.ds(at, n), :, :, pl.ds(0, 32), :]
        else:
            dst = mstage.reshape(1, 2, 8, 40, 128).at[:, :, :, pl.ds(0, 32), :]
        copies.append(pltpu.make_async_copy(src, dst, sems.at[k]))
        at += n
    for c in copies:
        c.start()
    for c in copies:
        c.wait()


def staged_column(stage, mstage, name, c):
    ref, f = (mstage, 0) if name == "mask" else (stage, WHERE[name])
    parts = [ref[f, c // 8, pl.ds(8 * k + c % 8, 8, stride=40), :] for k in range(4)]
    return jnp.concatenate(parts, 0).astype(F32)


def parity():
    return lax.rem(lax.axis_index("gy"), 2)


def turned(x, by):
    return pltpu.roll(x, by % 128, 1) if by % 128 else x


def squeeze(tiles):
    _, lane = iotas((8, 128))
    out = []
    for t in range(0, len(tiles), 8):
        for g in range(8):
            tile, first = tiles[t + g]
            y = turned(tile, 16 * g - first)
            x = y if g == 0 else jnp.where(lane // 16 >= g, y, x)
        out.append(x)
    return out


def spread(packed, n, first):
    return turned(packed[n // 8], first - 16 * (n % 8))


OWN, OTHER = 112, 48


def top_tile(stage, mstage, k, ih):
    ref, f = (mstage, 0) if k == TOP - 1 else (stage, k)
    return ref[f, ih, pl.ds(7 * 40 + 24, 8), :].astype(F32)


def by_side(cross, body):
    even = parity() == 0
    here = even if cross else jnp.logical_not(even)

    @pl.when(here)
    def _():
        body(0)

    @pl.when(jnp.logical_not(here))
    def _():
        body(1)


def pack_side(out, f4, st, sc, stage, mstage, side, half):
    def column(name, m):
        ref, f = (mstage, 0) if name == "mask" else (stage, WHERE[name])
        il = 7 - m if side else m
        parts = [ref[f, half, pl.ds(8 * k + il, 8, stride=40), :] for k in range(4)]
        return jnp.concatenate(parts, 0).astype(F32)

    at = lambda m: rows(C - 1 - m if side else m)
    put_column(st, sc, at(1), {name: column(name, 1) for name in FIELDS})
    for m in (0, 2):
        st[U, at(m), :], st[V, at(m), :] = column("u", m), column("v", m)
    put(out, [column(name, 0) for name in FIELDS])
    put(out, outgoing(st, sc, f4[...], side), TOP)


def pack_cross(
    f_ref, i_ref, v_ref, s_ref, m_ref, cor, b_out, m_out, f4, st, sc, stage, mstage, top, mtop, sems
):
    srcs = (f_ref, i_ref, v_ref, s_ref, m_ref)

    def body(side):
        main = [pltpu.make_async_copy(cor, f4, sems.at[5])]
        tops = []
        il = pl.ds(5 if side else 0, 3)
        at = 0
        for k, src in enumerate(srcs):
            n = src.shape[0]
            if k < 4:
                dst = stage.reshape(11, 8, 5, 8, 128).at[pl.ds(at, n), :, pl.ds(0, 4), il, :]
            else:
                dst = mstage.reshape(1, 8, 5, 8, 128).at[:, :, pl.ds(0, 4), il, :]
            part = src.reshape(n, 2, 8, 4, 8, 128).at[:, side, :, :, il, :]
            main.append(pltpu.make_async_copy(part, dst, sems.at[k]))
            dst = top.at[pl.ds(at, n)] if k < 4 else mtop
            tile = src.at[:, :, 7, pl.ds(24, 8), :]
            tops.append(pltpu.make_async_copy(tile, dst, sems.at[6 + k]))
            at += n
        for c in main + tops:
            c.start()
        for c in main:
            c.wait()
        pack_side(b_out, f4, st, sc, stage, mstage, side, 0)
        for c in tops:
            c.wait()
        tiles = [
            mtop[0, ih].astype(F32) if k == TOP - 1 else top[k, ih]
            for k in range(TOP)
            for ih in range(2)
        ]
        for n, x in enumerate(squeeze([(x, OWN) for x in tiles])):
            m_out[pl.ds(8 * n, 8), :] = x
            b_out[pl.ds(len(FIRST) * R + 8 * n, 8), :] = x

    by_side(True, body)


def pack_chip(f_ref, i_ref, v_ref, s_ref, m_ref, f4, a_out, stage, mstage, st, sc, sems):
    stage_in((f_ref, i_ref, v_ref, s_ref, m_ref), stage, mstage, sems)
    by_side(False, lambda side: pack_side(a_out, f4, st, sc, stage, mstage, side, side))


def first_interior(stage, mstage, f4, st, sc, tmp1, tmp2, strip):
    for c in range(C):
        put_column(
            st, sc, rows(c), {name: staged_column(stage, mstage, name, c) for name in FIELDS}
        )
    for k in range(TOP):
        for ih in range(2):
            strip[k, pl.ds(8 + 8 * ih, 8), :] = top_tile(stage, mstage, k, ih)
    interior(st, sc, tmp1, tmp2, f4[...])


def edge_side(r, out, st, sc, tmp1, tmp2, strip, f4, cross):
    def body(side):
        got = take(r, FIRST)
        put_column(st, sc, rows(C if side else -1), got)
        edges(st, sc, tmp1, tmp2, f4[...], **{("left", "right")[side]: next_names(got)})
        put(out, [st[k, rows(C - 1 if side else 0), :] for k in range(5)])
        put(out, outgoing(st, sc, f4[...], side), 5)
        at = pl.ds(16 if side else 8, 8)
        tiles = squeeze([(strip[k, at, :], first) for first in (OWN, OTHER) for k in range(TOP)])
        for n, x in enumerate(tiles):
            out[pl.ds(len(SECOND) * R + 8 * n, 8), :] = x

    by_side(cross, body)


def cross_edges(*refs):
    rb, rm, f4 = refs[:3]
    st, sc, tmp1, tmp2, strip, out = refs[8:]
    row, lane = iotas((8, 128))
    flip = 7 - row
    own = lane >= 64
    slab = lax.axis_index("gx") * lax.axis_size("gy") + lax.axis_index("gy")
    paired = (slab == 0) | (slab == N - 1) | (slab == N // 2 - 1) | (slab == N // 2)
    packed = [
        jnp.where(paired, rb[pl.ds(len(FIRST) * R + 8 * n, 8), :], rm[pl.ds(8 * n, 8), :])
        for n in range(3)
    ]
    for k in range(TOP):
        for ih in range(2):
            x = jnp.take_along_axis(spread(packed, 2 * k + ih, OTHER), flip, axis=0)
            at = pl.ds(16 - 8 * ih, 8)
            strip[k, at, :] = jnp.where(own, strip[k, at, :], x)
    edge_side(rb, out, st, sc, tmp1, tmp2, strip, f4, True)


def chip_edges(*refs):
    ra, f4 = refs[:2]
    st, sc, tmp1, tmp2, strip, out = refs[7:]
    edge_side(ra, out, st, sc, tmp1, tmp2, strip, f4, False)


def stage_out(st, sc, out, cols):
    for c in cols:
        x = [st[k, rows(c), :] for k in range(5)]
        for w, o in ((U, UO), (V, VO)):
            d = x[w] - sc[o, rows(c), :]
            x.append(0.5 * root(d * d + 0.0025) * d)
        for f, y in enumerate(x):
            for k in range(4):
                out[f, c // 8, pl.ds(8 * k + c % 8, 8, stride=40), :] = y[8 * k : 8 * k + 8]


def rows_out(out, dsts, sems, copies, ih, s, il):
    f = 0
    for dst in dsts:
        n = dst.shape[0]
        src = out.reshape(7, 2, 8, 5, 8, 128).at[pl.ds(f, n), ih, s, pl.ds(0, 4), il, :]
        to = dst.reshape(n, 2, 8, 4, 8, 128).at[:, ih, s, :, il, :]
        copies.append(pltpu.make_async_copy(src, to, sems.at[len(copies)]))
        copies[-1].start()
        f += n


FREE, TIED = pl.ds(0, 7), pl.ds(7, 1)


def second_interior(*refs):
    f4, (st, sc, tmp1, tmp2, out, vel_o, str_o, oce_o, sems) = refs[0], refs[5:]
    interior(st, sc, tmp1, tmp2, f4[...])
    copies = []
    for ih in range(2):
        stage_out(st, sc, out, range(8, 12) if ih else range(4, 8))
        il = pl.ds(0 if ih else 4, 4)
        rows_out(out, (vel_o, str_o, oce_o), sems, copies, ih, FREE, il)
    for c in copies:
        c.wait()


def run_strips(strip, work, cor4):
    _, lane = iotas((R, 128))
    last = lane % 64 == 63
    own = lane >= 64
    f4 = jnp.broadcast_to(cor4[pl.ds(31, 1), :], (R, 128))
    f4 = jnp.where(own, f4, pltpu.roll(f4, 64, 1))
    raw = {name: strip[k] for k, name in enumerate(FIELDS)}
    out, ice = statics(raw)
    work[U] = raw["u"]
    work[V] = raw["v"]
    for k, name in ((S1, "s1"), (S2, "s2"), (S12, "s12")):
        work[k] = jnp.where(ice, raw[name], 0.0)
    for k in range(9):
        work[5 + k] = out[k]
    ice = out[MK] == 2.0

    def west_east(y):
        plus, minus = pltpu.roll(y, R - 1, 0), pltpu.roll(y, 1, 0)
        return jnp.where(own, minus, plus), jnp.where(own, plus, minus)

    def down(y):
        return pltpu.roll(y, 1, 1)

    def up(y, sign):
        return jnp.where(last, sign * pltpu.roll(y, 64, 1), pltpu.roll(y, 127, 1))

    def step():
        u, v, s1, s2, s12 = [work[k] for k in range(5)]
        k = lambda n: work[5 + n]
        upu, um, vp, vm = up(u, -1.0), down(u), up(v, -1.0), down(v)
        tt, d2, ww, dv2 = u + upu, upu - um, v + vm, vp - vm
        w_ww, e_ww = west_east(ww)
        w_tt, e_tt = west_east(tt)
        a1, a2, a12 = stress_terms(
            u - west_east(u)[0],
            v - vm,
            (d2 + west_east(d2)[0]) + (e_ww - w_ww),
            e_tt - w_tt,
            dv2 + west_east(dv2)[1],
            (upu - u) + (west_east(v)[1] - v),
            k(PR),
        )
        s1, s2, s12 = K29 * s1 + a1, K29 * s2 + a2, K29 * s12 + a12
        q1, q2 = s1 + s2, s1 - s2
        fu = 0.5 * (west_east(q1)[1] - q1) + (s12 - down(s12))
        fv = 0.5 * (up(q2, 1.0) - q2) + (s12 - west_east(s12)[0])
        work[U] = momentum(u, k(UO), k(CU), k(MI), fu, f4 * (ww + e_ww), ice, k(OU))
        work[V] = momentum(v, k(VO), k(CV), k(MI), fv, -f4 * (tt + w_tt), ice, k(OV))
        work[S1], work[S2], work[S12] = s1, s2, s12

    return step


def second_edges(*refs):
    rb, ra, f4 = refs[:3]
    vel_o, str_o, oce_o, st, sc, tmp1, tmp2, strip, out, work, sems = refs[12:]
    even = parity() == 0
    left, right = receive(rb, ra, SECOND, even)
    for k, name in enumerate(STATE):
        st[k, rows(-1), :], st[k, rows(C), :] = left[name], right[name]
    base = len(SECOND) * R
    pb = [rb[pl.ds(base + 8 * n, 8), :] for n in range(3)]
    pa = [ra[pl.ds(base + 8 * n, 8), :] for n in range(3)]
    low = [jnp.where(even, b, a) for b, a in zip(pb, pa)]
    high = [jnp.where(even, a, b) for b, a in zip(pb, pa)]
    own = iotas((8, 128))[1] >= 64
    for k in range(TOP):
        for at, x in ((0, low), (24, high)):
            strip[k, pl.ds(at, 8), :] = jnp.where(
                own, spread(x, k, OWN), spread(x, TOP + k, OTHER)
            )
    step = run_strips(strip, work, f4)
    edges(st, sc, tmp1, tmp2, f4[...], next_names(left), next_names(right), step)
    copies = []
    outs = (vel_o, str_o, oce_o)
    top = iotas((8, 128))[1] >= 120
    tile = pl.ds(7 * 40 + 24, 8)
    for ih in range(2):
        stage_out(st, sc, out, range(12, 16) if ih else range(4))
        rows_out(out, outs, sems, copies, ih, FREE, pl.ds(4 if ih else 0, 4))
        mine = pl.ds(8 + 8 * ih, 8)
        x = [work[k, mine, :] for k in range(5)]
        for w, o in ((U, UO), (V, VO)):
            d = x[w] - work[5 + o, mine, :]
            x.append(0.5 * root(d * d + 0.0025) * d)
        for f, y in enumerate(x):
            out[f, ih, tile, :] = jnp.where(top, y, out[f, ih, tile, :])
        rows_out(out, outs, sems, copies, ih, TIED, pl.ds(0, 8))
    for c in copies:
        c.wait()


HBM = pl.BlockSpec(memory_space=pltpu.HBM)
VM = pl.BlockSpec(memory_space=pltpu.VMEM)


def shape(*dims):
    return jax.ShapeDtypeStruct(dims, F32)


def permuted(x, pairs):
    return lax.ppermute(x, AXES, pairs)


N = 128
CROSS = [(d, (d + 1) % N if d % 2 else (d - 1) % N) for d in range(N)]
CHIP = [(d, d ^ 1) for d in range(N)]
MIRROR = [(d, (d + N // 2) % N if (d, N - 1 - d) in CROSS else N - 1 - d) for d in range(N)]


def coriolis():
    b = 4 * np.arange(8)[None, :] + np.arange(4)[:, None]
    j = b.reshape(32, 1) * 128 + np.arange(128)[None, :]
    return (0.125 * np.sin(math.pi * ((j + 0.5) / 4096 - 0.5))).astype(np.float32)


def edge_scratch():
    return [pltpu.VMEM((5, NC * R, 128), F32), pltpu.VMEM((9, NC * R, 128), F32)]


def call(kernel, out, ins, specs, scratch, alias=None, outs=None, cost=None):
    return pl.pallas_call(
        kernel,
        out_shape=out,
        in_specs=specs,
        out_specs=outs or [VM] * len(out),
        scratch_shapes=scratch,
        input_output_aliases=alias or {},
        compiler_params=pltpu.CompilerParams(vmem_limit_bytes=20 << 20),
        cost_estimate=cost,
    )(*ins)


def on_device(forcing, ice_state, velocity, stress, ice_mask):
    raw = [
        pltpu.with_memory_space_constraint(view(x), pltpu.HBM)
        for x in (forcing, ice_state, velocity, stress, ice_mask[None])
    ]
    vel, strs, ocean = window(raw)
    return unview(vel), unview(strs), unview(ocean)


def window(raw):
    n1, n2 = len(FIRST) * R, len(SECOND) * R + 24
    cor = pltpu.with_memory_space_constraint(jnp.asarray(coriolis()), pltpu.HBM)
    cost = pl.CostEstimate(flops=20_000_000, bytes_accessed=4_000_000, transcendentals=500_000)
    b, m, f4 = call(
        pack_cross,
        [shape(n1 + 24, 128), shape(24, 128), shape(R, 128)],
        [*raw, cor],
        [HBM] * 6,
        [
            *edge_scratch(),
            pltpu.VMEM((11, 1, *STAGE[1:]), F32),
            pltpu.VMEM((1, 1, *STAGE[1:]), jnp.int32),
            pltpu.VMEM((11, 2, 8, 128), F32),
            pltpu.VMEM((1, 2, 8, 128), jnp.int32),
            pltpu.SemaphoreType.DMA((11,)),
        ],
    )
    rb = permuted(b, CROSS)
    rm = permuted(m, MIRROR)
    a, stage, mstage = call(
        pack_chip,
        [
            shape(n1, 128),
            shape(11, *STAGE),
            jax.ShapeDtypeStruct((1, *STAGE), jnp.int32),
        ],
        [*raw, f4],
        [HBM] * 5 + [VM],
        [*edge_scratch(), pltpu.SemaphoreType.DMA((5,))],
        cost=cost,
    )
    ra = permuted(a, CHIP)
    main = [shape(5, NC * R, 128), shape(9, NC * R, 128), *[shape(6, NC * R, 128)] * 2]
    strips = shape(TOP, R, 128)
    *state, strip = call(
        first_interior, [*main, strips], [stage, mstage, f4], [VM] * 3, [], cost=cost
    )
    *state, strip, b = call(
        cross_edges,
        [*main, strips, shape(n2, 128)],
        [rb, rm, f4, *state, strip],
        [VM] * 8,
        [],
        alias={3 + k: k for k in range(5)},
    )
    rb = permuted(b, CROSS)
    *state, strip, a = call(
        chip_edges,
        [*main, strips, shape(n2, 128)],
        [ra, f4, *state, strip],
        [VM] * 7,
        [],
        alias={2 + k: k for k in range(5)},
        cost=cost,
    )
    ra = permuted(a, CHIP)
    results = [shape(n, 2, 8, 32, 128) for n in (2, 3, 2)]
    *state, out, vel, strs, ocean = call(
        second_interior,
        [*main, shape(7, *STAGE), *results],
        [f4, *state],
        [VM] * 5,
        [pltpu.SemaphoreType.DMA((6,))],
        alias={1 + k: k for k in range(4)},
        outs=[VM] * 5 + [HBM] * 3,
        cost=cost,
    )
    vel, strs, ocean, *_ = call(
        second_edges,
        [*results, *main, strips, shape(7, *STAGE)],
        [rb, ra, f4, vel, strs, ocean, *state, strip, out],
        [VM] * 3 + [HBM] * 3 + [VM] * 6,
        [pltpu.VMEM((14, R, 128), F32), pltpu.SemaphoreType.DMA((12,))],
        alias={3 + k: k for k in range(9)},
        outs=[HBM] * 3 + [VM] * 6,
    )
    return vel, strs, ocean


def solution(mesh):
    slab = P(None, AXES, None)
    return jax.shard_map(
        on_device,
        mesh=mesh,
        in_specs=(slab, slab, slab, slab, P(AXES, None)),
        out_specs=(slab, slab, slab),
        check_vma=False,
    )
```

```python
import math

import jax
import jax.numpy as jnp
import numpy as np
from jax import lax
from jax.experimental import pallas as pl
from jax.experimental.pallas import tpu as pltpu
from jax.sharding import PartitionSpec as P


F32 = jnp.float32
AXES = ("gx", "gy")
C = 16
R = 32
H = 3
NC = C + 2 * H
FIELDS = ("uo", "vo", "tx", "ty", "a", "h", "u", "v", "s1", "s2", "s12", "mask")
WHERE = {n: k for k, n in enumerate(FIELDS)}
STATE = ("u", "v", "s1", "s2", "s12")
NEXT = ("u", "v", "z", "alpha", "beta")
U, V, S1, S2, S12 = range(5)
PR, MI, UO, CU, VO, CV, MK, OU, OV = range(9)
T, D2, W, DV2, E1, UP = range(6)
K29 = 29.0 / 30.0
STAGE = (2, 8 * 40, 128)
TOP = len(FIELDS)


def view(x):
    c = x.shape[0]
    return x.reshape(c, 2, 8, 8, 4, 128).transpose(0, 1, 3, 4, 2, 5).reshape(c, 2, 8, 32, 128)


def unview(y):
    c = y.shape[0]
    return y.reshape(c, 2, 8, 4, 8, 128).transpose(0, 1, 4, 2, 3, 5).reshape(c, C, 4096)


def iotas(shape):
    return lax.broadcasted_iota(jnp.int32, shape, 0), lax.broadcasted_iota(jnp.int32, shape, 1)


def root(x):
    return x * lax.rsqrt(jnp.maximum(x, 1e-30))


def below(x, masks):
    lane0, _, sub0, _ = masks
    r = pltpu.roll(x, 1, 1)
    q = jnp.where(sub0, 0.0, pltpu.roll(r[24:32], 1, 0))
    return jnp.where(lane0, jnp.concatenate([q, r[0:24]], 0), r)


def above(x, masks):
    _, lane127, _, _ = masks
    r = pltpu.roll(x, 127, 1)
    q = pltpu.roll(r[0:8], 7, 0)
    return jnp.where(lane127, jnp.concatenate([r[8:32], q], 0), r)


def make_masks():
    _, lane = iotas((R, 128))
    sub, _ = iotas((8, 128))
    return lane == 0, lane == 127, sub == 0, sub == 7


def rows(c):
    return pl.ds(pl.multiple_of((c + H) * R, R), R)


def each_column(span, body):
    if isinstance(span, tuple):
        lo, hi, chunk = span

        def step(t, carry):
            for q in range(chunk):
                body(lo + t * chunk + q)
            return carry

        lax.fori_loop(0, (hi - lo) // chunk, step, 0)
    else:
        for c in span:
            body(c)


def stress_terms(x1, e1, sc4, x, y, s, p):
    d = x1 + e1
    e = x1 - e1
    delta = root(d * d + 0.25 * (e * e) + (1.0 / 64.0) * (sc4 * sc4))
    r = p / (delta + 0.05)
    dk = x + y
    ek = x - y
    dk2 = root((1.0 / 16.0) * (dk * dk) + (1.0 / 64.0) * (ek * ek) + 0.25 * (s * s))
    rk = p / (dk2 + 0.05)
    return r * (d - delta), r * (0.25 * e), rk * (0.125 * s)


def momentum(w, o, c, mi, force, cor, ice, open_o):
    g = 0.5 * root((o - w) * (o - w) + 0.0025) * mi
    new = (30.0 * w + c + force * mi + g * o + cor) / (31.0 + g)
    return jnp.where(ice, new, open_o)


def subcycle(st, sc, tmp, f4, masks, vel, stress, mom, also=None):
    def shift(c):
        u, v = st[U, rows(c), :], st[V, rows(c), :]
        up, um = above(u, masks), below(u, masks)
        vp, vm = above(v, masks), below(v, masks)
        tmp[T, rows(c), :] = u + up
        tmp[D2, rows(c), :] = up - um
        tmp[UP, rows(c), :] = up - u
        tmp[W, rows(c), :] = v + vm
        tmp[E1, rows(c), :] = v - vm
        tmp[DV2, rows(c), :] = vp - vm

    each_column(vel, shift)

    def strain(c):
        ld = lambda k, d=0: tmp[k, rows(c + d), :]
        us = lambda d: st[U, rows(c + d), :]
        vs = lambda d: st[V, rows(c + d), :]
        a1, a2, a12 = stress_terms(
            us(0) - us(-1),
            ld(E1),
            (ld(D2) + ld(D2, -1)) + (ld(W, 1) - ld(W, -1)),
            ld(T, 1) - ld(T, -1),
            ld(DV2) + ld(DV2, 1),
            ld(UP) + (vs(1) - vs(0)),
            sc[PR, rows(c), :],
        )
        st[S1, rows(c), :] = K29 * st[S1, rows(c), :] + a1
        st[S2, rows(c), :] = K29 * st[S2, rows(c), :] + a2
        st[S12, rows(c), :] = K29 * st[S12, rows(c), :] + a12

    if also:
        also()
    each_column(stress, strain)
    if also:
        also()

    def move(c):
        ss = lambda k, d=0: st[k, rows(c + d), :]
        q1 = ss(S1) + ss(S2)
        q1n = ss(S1, 1) + ss(S2, 1)
        q2 = ss(S1) - ss(S2)
        s12 = ss(S12)
        fu = 0.5 * (q1n - q1) + (s12 - below(s12, masks))
        fv = 0.5 * (above(q2, masks) - q2) + (s12 - ss(S12, -1))
        cu = f4 * (tmp[W, rows(c), :] + tmp[W, rows(c + 1), :])
        cv = f4 * (tmp[T, rows(c), :] + tmp[T, rows(c - 1), :])
        k = lambda n: sc[n, rows(c), :]
        ice = k(MK) == 2.0
        mi = k(MI)
        st[U, rows(c), :] = momentum(ss(U), k(UO), k(CU), mi, fu, cu, ice, k(OU))
        st[V, rows(c), :] = momentum(ss(V), k(VO), k(CV), mi, fv, -cv, ice, k(OV))

    each_column(mom, move)


def interior(st, sc, tmp1, tmp2, f4):
    masks = make_masks()
    subcycle(st, sc, tmp1, f4, masks, (0, 16, 8), (1, 15, 7), (2, 14, 6))
    subcycle(st, sc, tmp2, f4, masks, (2, 14, 6), (3, 13, 5), (4, 12, 4))


def edges(st, sc, tmp1, tmp2, f4, left=None, right=None, also=None):
    masks = make_masks()

    def near(a, b, c, d):
        return [*(range(a, b) if left else ()), *(range(c, d) if right else ())]

    if left:
        st[U, rows(-2), :], st[V, rows(-2), :] = left["u"], left["v"]
        st[S12, rows(-2), :] = left["z"]
    if right:
        st[U, rows(17), :], st[V, rows(17), :] = right["u"], right["v"]
        st[S1, rows(17), :] = right["z"]
        st[S2, rows(17), :] = jnp.zeros((R, 128), F32)
    subcycle(
        st, sc, tmp1, f4, masks, near(-2, 0, 16, 18), near(-1, 1, 15, 17), near(-1, 2, 14, 17), also
    )
    if left:
        n11 = 0.5 * (st[S1, rows(-1), :] + st[S2, rows(-1), :])
        st[U, rows(-2), :] = left["alpha"] + left["beta"] * n11
    if right:
        st[V, rows(17), :] = right["alpha"] - right["beta"] * st[S12, rows(16), :]
    subcycle(
        st, sc, tmp2, f4, masks, near(-2, 2, 14, 18), near(-1, 3, 13, 17), near(0, 4, 12, 16), also
    )


def outgoing(st, sc, f4, side):
    masks = make_masks()

    def around(c):
        s = lambda k, d=0: st[k, rows(c + d), :]
        f = lambda k: sc[k, rows(c), :]
        t, d2, w, dv2 = [], [], [], []
        for d in (-1, 0, 1):
            u, v = s(U, d), s(V, d)
            up, um, vp, vm = above(u, masks), below(u, masks), above(v, masks), below(v, masks)
            t.append(u + up)
            d2.append(up - um)
            w.append(v + vm)
            dv2.append(vp - vm)
            if d == 0:
                e1, rise = v - vm, up - u
        a1, a2, a12 = stress_terms(
            s(U) - s(U, -1),
            e1,
            (d2[1] + d2[0]) + (w[2] - w[0]),
            t[2] - t[0],
            dv2[1] + dv2[2],
            rise + (s(V, 1) - s(V)),
            f(PR),
        )
        s1, s2, s12 = K29 * s(S1) + a1, K29 * s(S2) + a2, K29 * s(S12) + a12
        return s, f, t, w, s1 + s2, s1 - s2, s12

    def numbers(x, o, c, mi, force, cor, ice, open_o):
        g = 0.5 * root((o - x) * (o - x) + 0.0025) * mi
        b = 1.0 / (31.0 + g)
        a = (30.0 * x + c + force * mi + g * o + cor) * b
        return jnp.where(ice, a, open_o), jnp.where(ice, mi * b, 0.0)

    if side == 0:
        s, f, t, w, q1, q2, s12 = around(1)
        force = 0.5 * (above(q2, masks) - q2) + s12
        cor = -f4 * (t[1] + t[0])
        ice = f(MK) == 2.0
        return s(U), s(V), q1, *numbers(s(V), f(VO), f(CV), f(MI), force, cor, ice, f(OV))
    s, f, t, w, q1, q2, s12 = around(C - 2)
    force = (s12 - below(s12, masks)) - 0.5 * q1
    cor = f4 * (w[1] + w[2])
    ice = f(MK) == 2.0
    return s(U), s(V), s12, *numbers(s(U), f(UO), f(CU), f(MI), force, cor, ice, f(OU))


def put(out, xs, n=0):
    for x in xs:
        out[pl.ds(n * R, R), :] = x
        n += 1


def take(ref, names):
    return {name: ref[pl.ds(n * R, R), :] for n, name in enumerate(names)}


def receive(rb, ra, names, even):
    b, a = take(rb, names), take(ra, names)
    left = {n: jnp.where(even, b[n], a[n]) for n in names}
    right = {n: jnp.where(even, a[n], b[n]) for n in names}
    return left, right


def next_names(x):
    return {n: x[n + "1"] for n in NEXT}


FIRST = (*FIELDS, *[n + "1" for n in NEXT])
SECOND = (*STATE, *[n + "1" for n in NEXT])


def statics(raw):
    a, h, mask = raw["a"], raw["h"], raw["mask"]
    ice = mask == 2.0
    opened = mask == 1.0
    mi = 1.0 / (a * h)
    out = {
        PR: jnp.where(ice, h * jnp.exp(-20.0 * (1.0 - a)) * (1.0 / 30.0), 0.0),
        MI: mi,
        UO: raw["uo"],
        CU: raw["u"] + raw["tx"] * mi,
        VO: raw["vo"],
        CV: raw["v"] + raw["ty"] * mi,
        MK: mask,
        OU: jnp.where(opened, raw["uo"], 0.0),
        OV: jnp.where(opened, raw["vo"], 0.0),
    }
    return out, ice


def put_column(st, sc, at, raw):
    out, ice = statics(raw)
    for k, x in out.items():
        sc[k, at, :] = x
    st[U, at, :] = raw["u"]
    st[V, at, :] = raw["v"]
    st[S1, at, :] = jnp.where(ice, raw["s1"], 0.0)
    st[S2, at, :] = jnp.where(ice, raw["s2"], 0.0)
    st[S12, at, :] = jnp.where(ice, raw["s12"], 0.0)


def stage_in(srcs, stage, mstage, sems):
    copies = []
    at = 0
    for k, src in enumerate(srcs):
        n = src.shape[0]
        if k < 4:
            dst = stage.reshape(11, 2, 8, 40, 128).at[pl.ds(at, n), :, :, pl.ds(0, 32), :]
        else:
            dst = mstage.reshape(1, 2, 8, 40, 128).at[:, :, :, pl.ds(0, 32), :]
        copies.append(pltpu.make_async_copy(src, dst, sems.at[k]))
        at += n
    for c in copies:
        c.start()
    for c in copies:
        c.wait()


def staged_column(stage, mstage, name, c):
    ref, f = (mstage, 0) if name == "mask" else (stage, WHERE[name])
    parts = [ref[f, c // 8, pl.ds(8 * k + c % 8, 8, stride=40), :] for k in range(4)]
    return jnp.concatenate(parts, 0).astype(F32)


def parity():
    return lax.rem(lax.axis_index("gy"), 2)


def turned(x, by):
    return pltpu.roll(x, by % 128, 1) if by % 128 else x


def squeeze(tiles):
    _, lane = iotas((8, 128))
    out = []
    for t in range(0, len(tiles), 8):
        for g in range(8):
            tile, first = tiles[t + g]
            y = turned(tile, 16 * g - first)
            x = y if g == 0 else jnp.where(lane // 16 >= g, y, x)
        out.append(x)
    return out


def spread(packed, n, first):
    return turned(packed[n // 8], first - 16 * (n % 8))


OWN, OTHER = 112, 48


def top_tile(stage, mstage, k, ih):
    ref, f = (mstage, 0) if k == TOP - 1 else (stage, k)
    return ref[f, ih, pl.ds(7 * 40 + 24, 8), :].astype(F32)


def by_side(cross, body):
    even = parity() == 0
    here = even if cross else jnp.logical_not(even)

    @pl.when(here)
    def _():
        body(0)

    @pl.when(jnp.logical_not(here))
    def _():
        body(1)


def pack_side(out, f4, st, sc, stage, mstage, side, half):
    def column(name, m):
        ref, f = (mstage, 0) if name == "mask" else (stage, WHERE[name])
        il = 7 - m if side else m
        parts = [ref[f, half, pl.ds(8 * k + il, 8, stride=40), :] for k in range(4)]
        return jnp.concatenate(parts, 0).astype(F32)

    at = lambda m: rows(C - 1 - m if side else m)
    put_column(st, sc, at(1), {name: column(name, 1) for name in FIELDS})
    for m in (0, 2):
        st[U, at(m), :], st[V, at(m), :] = column("u", m), column("v", m)
    put(out, [column(name, 0) for name in FIELDS])
    put(out, outgoing(st, sc, f4[...], side), TOP)


def pack_cross(
    f_ref, i_ref, v_ref, s_ref, m_ref, cor, b_out, m_out, f4, st, sc, stage, mstage, top, mtop, sems
):
    srcs = (f_ref, i_ref, v_ref, s_ref, m_ref)

    def body(side):
        main = [pltpu.make_async_copy(cor, f4, sems.at[5])]
        tops = []
        il = pl.ds(5 if side else 0, 3)
        at = 0
        for k, src in enumerate(srcs):
            n = src.shape[0]
            if k < 4:
                dst = stage.reshape(11, 8, 5, 8, 128).at[pl.ds(at, n), :, pl.ds(0, 4), il, :]
            else:
                dst = mstage.reshape(1, 8, 5, 8, 128).at[:, :, pl.ds(0, 4), il, :]
            part = src.reshape(n, 2, 8, 4, 8, 128).at[:, side, :, :, il, :]
            main.append(pltpu.make_async_copy(part, dst, sems.at[k]))
            dst = top.at[pl.ds(at, n)] if k < 4 else mtop
            tile = src.at[:, :, 7, pl.ds(24, 8), :]
            tops.append(pltpu.make_async_copy(tile, dst, sems.at[6 + k]))
            at += n
        for c in main + tops:
            c.start()
        for c in main:
            c.wait()
        pack_side(b_out, f4, st, sc, stage, mstage, side, 0)
        for c in tops:
            c.wait()
        tiles = [
            mtop[0, ih].astype(F32) if k == TOP - 1 else top[k, ih]
            for k in range(TOP)
            for ih in range(2)
        ]
        for n, x in enumerate(squeeze([(x, OWN) for x in tiles])):
            m_out[pl.ds(8 * n, 8), :] = x
            b_out[pl.ds(len(FIRST) * R + 8 * n, 8), :] = x

    by_side(True, body)


def pack_chip(f_ref, i_ref, v_ref, s_ref, m_ref, f4, a_out, stage, mstage, st, sc, sems):
    stage_in((f_ref, i_ref, v_ref, s_ref, m_ref), stage, mstage, sems)
    by_side(False, lambda side: pack_side(a_out, f4, st, sc, stage, mstage, side, side))


def first_interior(stage, mstage, f4, st, sc, tmp1, tmp2, strip):
    for c in range(C):
        put_column(
            st, sc, rows(c), {name: staged_column(stage, mstage, name, c) for name in FIELDS}
        )
    for k in range(TOP):
        for ih in range(2):
            strip[k, pl.ds(8 + 8 * ih, 8), :] = top_tile(stage, mstage, k, ih)
    interior(st, sc, tmp1, tmp2, f4[...])


def edge_side(r, out, st, sc, tmp1, tmp2, strip, f4, cross, first=None):
    def body(side):
        if first:
            first()
        got = take(r, FIRST)
        put_column(st, sc, rows(C if side else -1), got)
        edges(st, sc, tmp1, tmp2, f4[...], **{("left", "right")[side]: next_names(got)})
        put(out, [st[k, rows(C - 1 if side else 0), :] for k in range(5)])
        put(out, outgoing(st, sc, f4[...], side), 5)
        at = pl.ds(16 if side else 8, 8)
        tiles = squeeze([(strip[k, at, :], first) for first in (OWN, OTHER) for k in range(TOP)])
        for n, x in enumerate(tiles):
            out[pl.ds(len(SECOND) * R + 8 * n, 8), :] = x

    by_side(cross, body)


def cross_edges(*refs):
    rb, rm, f4 = refs[:3]
    st, sc, tmp1, tmp2, strip, out = refs[8:]
    row, lane = iotas((8, 128))
    flip = 7 - row
    own = lane >= 64
    slab = lax.axis_index("gx") * lax.axis_size("gy") + lax.axis_index("gy")
    paired = (slab == 0) | (slab == N - 1) | (slab == N // 2 - 1) | (slab == N // 2)
    packed = [
        jnp.where(paired, rb[pl.ds(len(FIRST) * R + 8 * n, 8), :], rm[pl.ds(8 * n, 8), :])
        for n in range(3)
    ]

    def mirrored():
        for k in range(TOP):
            for ih in range(2):
                x = jnp.take_along_axis(spread(packed, 2 * k + ih, OTHER), flip, axis=0)
                at = pl.ds(16 - 8 * ih, 8)
                strip[k, at, :] = jnp.where(own, strip[k, at, :], x)

    edge_side(rb, out, st, sc, tmp1, tmp2, strip, f4, True, mirrored)


def chip_edges(*refs):
    ra, f4 = refs[:2]
    st, sc, tmp1, tmp2, strip, out = refs[7:]
    edge_side(ra, out, st, sc, tmp1, tmp2, strip, f4, False)


def stage_out(st, sc, out, cols):
    for c in cols:
        x = [st[k, rows(c), :] for k in range(5)]
        for w, o in ((U, UO), (V, VO)):
            d = x[w] - sc[o, rows(c), :]
            x.append(0.5 * root(d * d + 0.0025) * d)
        for f, y in enumerate(x):
            for k in range(4):
                out[f, c // 8, pl.ds(8 * k + c % 8, 8, stride=40), :] = y[8 * k : 8 * k + 8]


def rows_out(out, dsts, sems, copies, ih, s, il):
    f = 0
    for dst in dsts:
        n = dst.shape[0]
        src = out.reshape(7, 2, 8, 5, 8, 128).at[pl.ds(f, n), ih, s, pl.ds(0, 4), il, :]
        to = dst.reshape(n, 2, 8, 4, 8, 128).at[:, ih, s, :, il, :]
        copies.append(pltpu.make_async_copy(src, to, sems.at[len(copies)]))
        copies[-1].start()
        f += n


FREE, TIED = pl.ds(0, 7), pl.ds(7, 1)


def second_interior(*refs):
    f4, (st, sc, tmp1, tmp2, out, vel_o, str_o, oce_o, sems) = refs[0], refs[5:]
    interior(st, sc, tmp1, tmp2, f4[...])
    copies = []
    for ih in range(2):
        stage_out(st, sc, out, range(8, 12) if ih else range(4, 8))
        il = pl.ds(0 if ih else 4, 4)
        rows_out(out, (vel_o, str_o, oce_o), sems, copies, ih, FREE, il)
    for c in copies:
        c.wait()


def run_strips(strip, work, cor4):
    _, lane = iotas((R, 128))
    last = lane % 64 == 63
    own = lane >= 64
    f4 = jnp.broadcast_to(cor4[pl.ds(31, 1), :], (R, 128))
    f4 = jnp.where(own, f4, pltpu.roll(f4, 64, 1))
    raw = {name: strip[k] for k, name in enumerate(FIELDS)}
    out, ice = statics(raw)
    work[U] = raw["u"]
    work[V] = raw["v"]
    for k, name in ((S1, "s1"), (S2, "s2"), (S12, "s12")):
        work[k] = jnp.where(ice, raw[name], 0.0)
    for k in range(9):
        work[5 + k] = out[k]
    ice = out[MK] == 2.0

    def west_east(y):
        plus, minus = pltpu.roll(y, R - 1, 0), pltpu.roll(y, 1, 0)
        return jnp.where(own, minus, plus), jnp.where(own, plus, minus)

    def down(y):
        return pltpu.roll(y, 1, 1)

    def up(y, sign):
        return jnp.where(last, sign * pltpu.roll(y, 64, 1), pltpu.roll(y, 127, 1))

    def step():
        u, v, s1, s2, s12 = [work[k] for k in range(5)]
        k = lambda n: work[5 + n]
        upu, um, vp, vm = up(u, -1.0), down(u), up(v, -1.0), down(v)
        tt, d2, ww, dv2 = u + upu, upu - um, v + vm, vp - vm
        w_ww, e_ww = west_east(ww)
        w_tt, e_tt = west_east(tt)
        a1, a2, a12 = stress_terms(
            u - west_east(u)[0],
            v - vm,
            (d2 + west_east(d2)[0]) + (e_ww - w_ww),
            e_tt - w_tt,
            dv2 + west_east(dv2)[1],
            (upu - u) + (west_east(v)[1] - v),
            k(PR),
        )
        s1, s2, s12 = K29 * s1 + a1, K29 * s2 + a2, K29 * s12 + a12
        q1, q2 = s1 + s2, s1 - s2
        fu = 0.5 * (west_east(q1)[1] - q1) + (s12 - down(s12))
        fv = 0.5 * (up(q2, 1.0) - q2) + (s12 - west_east(s12)[0])
        work[U] = momentum(u, k(UO), k(CU), k(MI), fu, f4 * (ww + e_ww), ice, k(OU))
        work[V] = momentum(v, k(VO), k(CV), k(MI), fv, -f4 * (tt + w_tt), ice, k(OV))
        work[S1], work[S2], work[S12] = s1, s2, s12

    return step


def second_edges(*refs):
    rb, ra, f4 = refs[:3]
    vel_o, str_o, oce_o, st, sc, tmp1, tmp2, strip, out, work, sems = refs[12:]
    even = parity() == 0
    left, right = receive(rb, ra, SECOND, even)
    for k, name in enumerate(STATE):
        st[k, rows(-1), :], st[k, rows(C), :] = left[name], right[name]
    base = len(SECOND) * R
    pb = [rb[pl.ds(base + 8 * n, 8), :] for n in range(3)]
    pa = [ra[pl.ds(base + 8 * n, 8), :] for n in range(3)]
    low = [jnp.where(even, b, a) for b, a in zip(pb, pa)]
    high = [jnp.where(even, a, b) for b, a in zip(pb, pa)]
    own = iotas((8, 128))[1] >= 64
    for k in range(TOP):
        for at, x in ((0, low), (24, high)):
            strip[k, pl.ds(at, 8), :] = jnp.where(
                own, spread(x, k, OWN), spread(x, TOP + k, OTHER)
            )
    step = run_strips(strip, work, f4)
    edges(st, sc, tmp1, tmp2, f4[...], next_names(left), next_names(right), step)
    copies = []
    outs = (vel_o, str_o, oce_o)
    top = iotas((8, 128))[1] >= 120
    tile = pl.ds(7 * 40 + 24, 8)
    for ih in range(2):
        stage_out(st, sc, out, range(12, 16) if ih else range(4))
        rows_out(out, outs, sems, copies, ih, FREE, pl.ds(4 if ih else 0, 4))
        mine = pl.ds(8 + 8 * ih, 8)
        x = [work[k, mine, :] for k in range(5)]
        for w, o in ((U, UO), (V, VO)):
            d = x[w] - work[5 + o, mine, :]
            x.append(0.5 * root(d * d + 0.0025) * d)
        for f, y in enumerate(x):
            out[f, ih, tile, :] = jnp.where(top, y, out[f, ih, tile, :])
        rows_out(out, outs, sems, copies, ih, TIED, pl.ds(0, 8))
    for c in copies:
        c.wait()


HBM = pl.BlockSpec(memory_space=pltpu.HBM)
VM = pl.BlockSpec(memory_space=pltpu.VMEM)


def shape(*dims):
    return jax.ShapeDtypeStruct(dims, F32)


def permuted(x, pairs):
    return lax.ppermute(x, AXES, pairs)


N = 128
CROSS = [(d, (d + 1) % N if d % 2 else (d - 1) % N) for d in range(N)]
CHIP = [(d, d ^ 1) for d in range(N)]
MIRROR = [(d, (d + N // 2) % N if (d, N - 1 - d) in CROSS else N - 1 - d) for d in range(N)]


def coriolis():
    b = 4 * np.arange(8)[None, :] + np.arange(4)[:, None]
    j = b.reshape(32, 1) * 128 + np.arange(128)[None, :]
    return (0.125 * np.sin(math.pi * ((j + 0.5) / 4096 - 0.5))).astype(np.float32)


def edge_scratch():
    return [pltpu.VMEM((5, NC * R, 128), F32), pltpu.VMEM((9, NC * R, 128), F32)]


def call(kernel, out, ins, specs, scratch, alias=None, outs=None, cost=None):
    return pl.pallas_call(
        kernel,
        out_shape=out,
        in_specs=specs,
        out_specs=outs or [VM] * len(out),
        scratch_shapes=scratch,
        input_output_aliases=alias or {},
        compiler_params=pltpu.CompilerParams(vmem_limit_bytes=20 << 20),
        cost_estimate=cost,
    )(*ins)


def on_device(forcing, ice_state, velocity, stress, ice_mask):
    raw = [
        pltpu.with_memory_space_constraint(view(x), pltpu.HBM)
        for x in (forcing, ice_state, velocity, stress, ice_mask[None])
    ]
    vel, strs, ocean = window(raw)
    return unview(vel), unview(strs), unview(ocean)


def window(raw):
    n1, n2 = len(FIRST) * R, len(SECOND) * R + 24
    cor = pltpu.with_memory_space_constraint(jnp.asarray(coriolis()), pltpu.HBM)
    cost = pl.CostEstimate(flops=20_000_000, bytes_accessed=4_000_000, transcendentals=500_000)
    b, m, f4 = call(
        pack_cross,
        [shape(n1 + 24, 128), shape(24, 128), shape(R, 128)],
        [*raw, cor],
        [HBM] * 6,
        [
            *edge_scratch(),
            pltpu.VMEM((11, 1, *STAGE[1:]), F32),
            pltpu.VMEM((1, 1, *STAGE[1:]), jnp.int32),
            pltpu.VMEM((11, 2, 8, 128), F32),
            pltpu.VMEM((1, 2, 8, 128), jnp.int32),
            pltpu.SemaphoreType.DMA((11,)),
        ],
    )
    rb = permuted(b, CROSS)
    rm = permuted(m, MIRROR)
    a, stage, mstage = call(
        pack_chip,
        [
            shape(n1, 128),
            shape(11, *STAGE),
            jax.ShapeDtypeStruct((1, *STAGE), jnp.int32),
        ],
        [*raw, f4],
        [HBM] * 5 + [VM],
        [*edge_scratch(), pltpu.SemaphoreType.DMA((5,))],
        cost=cost,
    )
    ra = permuted(a, CHIP)
    main = [shape(5, NC * R, 128), shape(9, NC * R, 128), *[shape(6, NC * R, 128)] * 2]
    strips = shape(TOP, R, 128)
    *state, strip = call(
        first_interior, [*main, strips], [stage, mstage, f4], [VM] * 3, [], cost=cost
    )
    *state, strip, b = call(
        cross_edges,
        [*main, strips, shape(n2, 128)],
        [rb, rm, f4, *state, strip],
        [VM] * 8,
        [],
        alias={3 + k: k for k in range(5)},
    )
    rb = permuted(b, CROSS)
    *state, strip, a = call(
        chip_edges,
        [*main, strips, shape(n2, 128)],
        [ra, f4, *state, strip],
        [VM] * 7,
        [],
        alias={2 + k: k for k in range(5)},
        cost=cost,
    )
    ra = permuted(a, CHIP)
    results = [shape(n, 2, 8, 32, 128) for n in (2, 3, 2)]
    *state, out, vel, strs, ocean = call(
        second_interior,
        [*main, shape(7, *STAGE), *results],
        [f4, *state],
        [VM] * 5,
        [pltpu.SemaphoreType.DMA((6,))],
        alias={1 + k: k for k in range(4)},
        outs=[VM] * 5 + [HBM] * 3,
        cost=cost,
    )
    vel, strs, ocean, *_ = call(
        second_edges,
        [*results, *main, strips, shape(7, *STAGE)],
        [rb, ra, f4, vel, strs, ocean, *state, strip, out],
        [VM] * 3 + [HBM] * 3 + [VM] * 6,
        [pltpu.VMEM((14, R, 128), F32), pltpu.SemaphoreType.DMA((12,))],
        alias={3 + k: k for k in range(9)},
        outs=[HBM] * 3 + [VM] * 6,
    )
    return vel, strs, ocean


def solution(mesh):
    slab = P(None, AXES, None)
    return jax.shard_map(
        on_device,
        mesh=mesh,
        in_specs=(slab, slab, slab, slab, P(AXES, None)),
        out_specs=(slab, slab, slab),
        check_vma=False,
    )
```
